32 devices in a mesh: row: 8 (over z, y), col: 4 (over x, core).
Axes of the slice: x: 2, y: 2, z: 4, core: 2. Of those that a mesh axis runs over, the one named last changes fastest.
Arguments:
- object_slab: float32 [2, 2560, 1280], P(None, 'row', 'col'), may hold values from -5 to 5
- probe_field: float32 [2, 512, 512], replicated, may hold values from -5 to 5
- offsets: int32 [8, 4, 1, 2], P('row', 'col'), may hold values from 0 to 64
- counts: int32 [8, 4, 1, 512, 512], P('row', 'col'), may hold values from 0 to 399
Outputs:
- updated: float32 [2, 2560, 1280], P(None, 'row', 'col')
The draws below stay inside these ranges and needn't reach their ends.
Inputs may be any that keep to these rules, and one draw needn't show every extreme that they name: Window offsets inside the widened tile of 576 cells a side; the window never leaves it.
All inputs are finite; a program needn't handle non-finite values.
Results may differ from the reference program's by a relative error of at most 0.0003.
Values sent between devices are 32-bit elements; how exact they have to be, the bound alone decides.
No kernel may reach another device: no remote copies, remote signals or barrier semaphores. Data moves between devices by JAX's collectives and lax.ppermute only.
A program may use at most 128 MiB of HBM per device.

```python
import math
import jax
import jax.numpy as jnp
from jax import lax

TILE = 448
OVL = 128
WIN = 512
POS_DEV = 1
TILES_R = 8
TILES_C = 4
SLAB_R = 2560
SLAB_C = 1280


def with_ends(result, stream_key, least, high):
    spot = [jax.random.randint(jax.random.fold_in(stream_key, axis), (), 0, length) for axis, length in enumerate(result.shape)]
    longest = result.shape.index(max(result.shape))
    neighbour = spot[:longest] + [(spot[longest] + 1) % result.shape[longest]] + spot[longest + 1:]
    return result.at[tuple(spot)].set(least).at[tuple(neighbour)].set(high)


def levels(rng, shape, pieces, smallest, top_value):
    def one(dim, blocks):
        heights = jax.random.uniform(jax.random.fold_in(jax.random.fold_in(rng, 6), dim), (blocks,), jnp.float32, smallest / len(pieces), top_value / len(pieces))
        return jnp.repeat(jnp.exp(heights), shape[dim] // blocks).reshape((-1,) + (1,) * (len(shape) - dim - 1))

    gain = one(*pieces[0])
    for cut in pieces[1:]:
        gain = gain * one(*cut)
    return gain


def bell_draw(key, shape, scale, most, pieces=(), held_as=jnp.bfloat16):
    entries = scale * jax.random.normal(key, shape, jnp.float32)
    if pieces:
        entries = entries * levels(key, shape, pieces, -0.22, 0.18)
    return jnp.clip(entries, -most, most).astype(held_as)


def setup_inputs(seed: int = 0) -> dict:
    key_of = jax.random.split(jax.random.key(seed), 5)
    return {
        "object_slab": bell_draw(key_of[0], (2, SLAB_R, SLAB_C), 0.7, 5.0, ((1, 8), (2, 4)), jnp.float32),
        "probe_field": bell_draw(key_of[1], (2, WIN, WIN), 1.0, 5.0, (), jnp.float32),
        "offsets": with_ends(jax.random.randint(key_of[2], (TILES_R, TILES_C, POS_DEV, 2), 0, TILE + OVL - WIN + 1), jax.random.fold_in(key_of[2], 1), 0, TILE + OVL - WIN).astype(jnp.int32),
        "counts": with_ends(jax.random.randint(key_of[3], (TILES_R, TILES_C, POS_DEV, WIN, WIN), 0, 400), jax.random.fold_in(key_of[3], 1), 0, 399).astype(jnp.int32),
    }


EPSILON = 0.01
PHOTON_SCALE = 0.01
STEP_SIZE = 0.5
REGULAR = 1.0

def matmul(left, right):
    return jnp.dot(left, right, precision=lax.Precision.HIGH, preferred_element_type=jnp.float32)

def dft_tables(length):
    indices = jnp.arange(length, dtype=jnp.int32)
    products = indices[:, None] * indices[None, :] % length
    angles = products.astype(jnp.float32) * (2.0 * math.pi / length)
    norm_factor = 1.0 / math.sqrt(length)
    return (jnp.cos(angles) * norm_factor, jnp.sin(angles) * norm_factor)

def forward(real_part, imag_part, cosine_table, sine_table):
    left_real = matmul(cosine_table, real_part) + matmul(sine_table, imag_part)
    left_imag = matmul(cosine_table, imag_part) - matmul(sine_table, real_part)
    return (matmul(left_real, cosine_table) + matmul(left_imag, sine_table), matmul(left_imag, cosine_table) - matmul(left_real, sine_table))

def inverse(real_part, imag_part, cosine_table, sine_table):
    left_real = matmul(cosine_table, real_part) - matmul(sine_table, imag_part)
    left_imag = matmul(cosine_table, imag_part) + matmul(sine_table, real_part)
    return (matmul(left_real, cosine_table) - matmul(left_imag, sine_table), matmul(left_imag, cosine_table) + matmul(left_real, sine_table))

def tile_terms(widened, probe_field, tile_counts, tile_offsets, cosine_table, sine_table):
    window = probe_field.shape[-1]
    totals = jnp.zeros((3,) + widened.shape[1:], jnp.float32)
    lighting = probe_field[0] * probe_field[0] + probe_field[1] * probe_field[1]
    for position in range(tile_counts.shape[0]):
        row_start = tile_offsets[position, 0]
        col_start = tile_offsets[position, 1]
        corner_at = (jnp.int32(0), row_start, col_start)
        patch = lax.dynamic_slice(widened, corner_at, (2, window, window))
        exit_real = probe_field[0] * patch[0] - probe_field[1] * patch[1]
        exit_imag = probe_field[0] * patch[1] + probe_field[1] * patch[0]
        far_real, far_imag = forward(exit_real, exit_imag, cosine_table, sine_table)
        modulus = jnp.sqrt(far_real * far_real + far_imag * far_imag + EPSILON)
        measured = jnp.sqrt(tile_counts[position].astype(jnp.float32) * PHOTON_SCALE)
        factor = 1.0 - measured / modulus
        back_real, back_imag = inverse(factor * far_real, factor * far_imag, cosine_table, sine_table)
        grad_real = probe_field[0] * back_real + probe_field[1] * back_imag
        grad_imag = probe_field[0] * back_imag - probe_field[1] * back_real
        contrib = jnp.stack([grad_real, grad_imag, lighting])
        current = lax.dynamic_slice(totals, corner_at, contrib.shape)
        totals = lax.dynamic_update_slice(totals, current + contrib, corner_at)
    return totals

def reference(object_slab, probe_field, offsets, counts):
    cosine_table, sine_table = dft_tables(WIN)
    block_cells = TILE - OVL
    extent = block_cells + 2 * OVL
    padded = jnp.pad(object_slab, ((0, 0), (OVL, OVL), (OVL, OVL)))
    tile_rows = offsets.shape[0]
    tile_cols = offsets.shape[1]
    flat_offsets = offsets.reshape(tile_rows * tile_cols, offsets.shape[2], 2)
    flat_counts = counts.reshape(tile_rows * tile_cols, counts.shape[2], WIN, WIN)
    numbers = jnp.arange(tile_rows * tile_cols, dtype=jnp.int32)

    def visit_tile(running, inputs):
        number, tile_offsets, tile_counts = inputs
        corner_at = (jnp.int32(0), number // tile_cols * block_cells, number % tile_cols * block_cells)
        widened = lax.dynamic_slice(padded, corner_at, (2, extent, extent))
        contrib = tile_terms(widened, probe_field, tile_counts, tile_offsets, cosine_table, sine_table)
        current = lax.dynamic_slice(running, corner_at, (3, extent, extent))
        return (lax.dynamic_update_slice(running, current + contrib, corner_at), None)
    initial = jnp.zeros((3, padded.shape[1], padded.shape[2]), jnp.float32)
    totals, unused = lax.scan(visit_tile, initial, (numbers, flat_offsets, flat_counts))
    owned = totals[:, OVL:OVL + object_slab.shape[1], OVL:OVL + object_slab.shape[2]]
    return object_slab - STEP_SIZE * owned[:2] / (owned[2] + REGULAR)
```

```python
import functools
import math

import jax
import jax.numpy as jnp
import ml_dtypes
import numpy as np
from jax import lax
from jax.experimental import pallas as pl
from jax.experimental.pallas import tpu as pltpu
from jax.sharding import PartitionSpec as P

OVL = 128
HALF = 64
LANES = 128

EPSILON = 0.01
PHOTON_SCALE = 0.01
STEP_SIZE = 0.5
REGULAR = 1.0

F32 = jnp.float32
BF16 = jnp.bfloat16


def call(kernel, name, out_shapes, n_smem, args, scratch=(), flops=0):
    specs = [
        pl.BlockSpec(memory_space=pltpu.SMEM if i < n_smem else pltpu.VMEM)
        for i in range(len(args))
    ]
    return pl.pallas_call(
        kernel,
        name=name,
        out_shape=[jax.ShapeDtypeStruct(s, d) for s, d in out_shapes],
        in_specs=specs,
        out_specs=[pl.BlockSpec(memory_space=pltpu.VMEM) for _ in out_shapes],
        scratch_shapes=list(scratch),
        compiler_params=pltpu.CompilerParams(vmem_limit_bytes=56 * 1024 * 1024),
        cost_estimate=pl.CostEstimate(flops=flops, bytes_accessed=0, transcendentals=0)
        if flops
        else None,
    )(*args)


@functools.lru_cache(maxsize=None)
def tables(length):
    quarter = length // 4
    n = np.arange(quarter)[:, None]
    k = np.arange(quarter)[None, :]
    blocks = []
    for p in range(4):
        angle = 2.0 * np.pi * ((n * (4 * k + p)) % length) / length
        c = np.cos(angle) / math.sqrt(length)
        s = np.sin(angle) / math.sqrt(length)
        blocks.append(np.block([[c, -s], [s, c]]))
    blocks += [b.T for b in blocks]
    full = np.stack(blocks)
    high = full.astype(np.float32).astype(ml_dtypes.bfloat16)
    low = (full - high.astype(np.float64)).astype(np.float32).astype(ml_dtypes.bfloat16)
    return high, low


def split(x):
    high = x.astype(BF16)
    return high, (x - high.astype(F32)).astype(BF16)


def dot(a, b):
    return lax.dot_general(a, b, (((1,), (0,)), ((), ())), preferred_element_type=F32)


def mix_forward(x):
    (x0r, x0i), (x1r, x1i), (x2r, x2i), (x3r, x3i) = x
    ar, ai, br, bi = x0r + x2r, x0i + x2i, x0r - x2r, x0i - x2i
    cr, ci, dr, di = x1r + x3r, x1i + x3i, x1r - x3r, x1i - x3i
    return [(ar + cr, ai + ci), (br + di, bi - dr), (ar - cr, ai - ci), (br - di, bi + dr)]


def mix_inverse(x):
    (x0r, x0i), (x1r, x1i), (x2r, x2i), (x3r, x3i) = x
    ar, ai, br, bi = x0r + x2r, x0i + x2i, x0r - x2r, x0i - x2i
    cr, ci, dr, di = x1r + x3r, x1i + x3i, x1r - x3r, x1i - x3i
    return [(ar + cr, ai + ci), (br - di, bi + dr), (ar - cr, ai - ci), (br + di, bi - dr)]


def lane_iota(shape):
    return lax.broadcasted_iota(jnp.int32, shape, len(shape) - 1)


def row_iota(shape):
    return lax.broadcasted_iota(jnp.int32, shape, len(shape) - 2)


def turn(x):
    return pltpu.roll(x, HALF, len(x.shape) - 1)


def pack_kernel(obj, north, south, west, east):
    rows, cols = obj.shape[1:]
    first = lane_iota((OVL, LANES)) < HALF
    for out, base in ((north, 0), (south, rows - OVL)):
        for c in range(2):
            out[:, c * 256 : c * 256 + 256] = obj[c, base : base + OVL, 0:256]
        out[:, 512 + 0 : 512 + HALF] = obj[0, base : base + OVL, 256:cols]
        out[:, 512 + HALF : 640] = obj[1, base : base + OVL, 256:cols]
    for c in range(2):
        west[c] = turn(obj[c, :, 0:128])
        east[c] = obj[c, :, cols - OVL : cols]


def corner_kernel(north, south, west, east):
    for base, halo in ((0, north), (OVL, south)):
        for c in range(2):
            west[c, base : base + OVL, :] = turn(halo[:, c * 256 : c * 256 + 128])
            tail = halo[:, 512 + c * HALF : 512 + c * HALF + HALF]
            east[c, base : base + OVL, 0:HALF] = halo[:, c * 256 + 192 : c * 256 + 256]
            east[c, base : base + OVL, HALF:128] = tail


def ready_kernel(offs, probe, counts, rolled, measured, wide):
    size = probe.shape[-1]
    quarter = size // 4
    u = offs[0]
    v = offs[1]
    for c in range(2):
        for t in range(4):
            cols = slice(t * quarter, (t + 1) * quarter)
            wide[c, t, 0:HALF, :] = probe[c, size - HALF : size, cols]
            wide[c, t, HALF : HALF + size, :] = probe[c, :, cols]
        for base in range(0, size, HALF):
            rows = pl.ds(HALF - u + base, HALF)
            piece = jnp.concatenate([wide[c, t, rows, :] for t in range(4)], axis=1)
            rolled[c, base : base + HALF, :] = pltpu.roll(piece, v, 1)
    r = row_iota((size, size))
    k = lane_iota((size, size))
    order = jnp.where(r == 4 * (k % quarter) + k // quarter, 1.0, 0.0).astype(BF16)
    for t in range(4):
        wide[0, t, 0:size, :] = counts[:, t * quarter : (t + 1) * quarter].astype(F32)
    for p in range(4):
        rows = jnp.concatenate([wide[0, t, pl.ds(p, quarter, stride=4), :] for t in range(4)], axis=1)
        high = jnp.floor(rows * (1.0 / 256.0))
        low = rows - 256.0 * high
        moved = 256.0 * dot(high.astype(BF16), order) + dot(low.astype(BF16), order)
        measured[p * quarter : (p + 1) * quarter, :] = jnp.sqrt(moved * PHOTON_SCALE)


def main_kernel(
    offs, obj, north, south, west, east, wcorner, ecorner, rolled, measured, high, low,
    own, nblock, sblock, wedge, eedge, wcorn, ecorn, fr, fi,
):
    size = rolled.shape[-1]
    quarter = size // 4
    cells = obj.shape[1]
    u = offs[0]
    v = offs[1]

    def pieces(c, part, base, count):
        lane = lane_iota((count, LANES))
        if part == "own":
            tiles = [obj[c, base : base + count, 0:128], obj[c, base : base + count, 128:256]]
            last = obj[c, base : base + count, 256:cells]
            last = jnp.concatenate([last, last], axis=1)
            w = west[c, base : base + count, :]
            e = east[c, base : base + count, :]
        else:
            ref, start = (north, base) if part == "n" else (south, base)
            tiles = [ref[start : start + count, c * 256 + 128 * t : c * 256 + 128 * t + 128] for t in range(2)]
            last = ref[start : start + count, 512:640]
            if c == 1:
                last = turn(last)
            start = start + (0 if part == "n" else OVL)
            w = wcorner[c, start : start + count, :]
            e = ecorner[c, start : start + count, :]
        return [jnp.where(lane < v, e, w), tiles[0], tiles[1], jnp.where(lane < HALF, last, e)]

    def patch(c, slot, count):
        if slot < HALF:
            row = row_iota((count, LANES)) + slot
            a = pieces(c, "n", slot, count)
            b = pieces(c, "s", slot + HALF, count)
            return [jnp.where(row < u, y, x) for x, y in zip(a, b)]
        if slot < OVL:
            return pieces(c, "n", slot, count)
        if slot < OVL + cells:
            return pieces(c, "own", slot - OVL, count)
        return pieces(c, "s", slot - OVL - cells, count)

    step = 64
    for base in range(0, size, step):
        rows = slice(base, base + step)
        orr, oi = patch(0, base, step), patch(1, base, step)
        exits = []
        for q in range(4):
            cols = slice(q * quarter, (q + 1) * quarter)
            pr, pi = rolled[0, rows, cols], rolled[1, rows, cols]
            exits.append((pr * orr[q] - pi * oi[q], pr * oi[q] + pi * orr[q]))
        for p, (yr, yi) in enumerate(mix_forward(exits)):
            a, b = split(jnp.concatenate([yr, yi], axis=1))
            z = dot(a, high[p]) + dot(a, low[p]) + dot(b, high[p])
            cols = slice(p * quarter, (p + 1) * quarter)
            fr[rows, cols] = z[:, :quarter]
            fi[rows, cols] = z[:, quarter:]

    for cb in range(4):
        cols = slice(cb * quarter, (cb + 1) * quarter)
        quads = [
            (fr[q * quarter : (q + 1) * quarter, cols], fi[q * quarter : (q + 1) * quarter, cols])
            for q in range(4)
        ]
        backs = []
        for p, (yr, yi) in enumerate(mix_forward(quads)):
            a, b = split(jnp.concatenate([yr, yi], axis=0))
            z = dot(high[4 + p], a) + dot(low[4 + p], a) + dot(high[4 + p], b)
            zr, zi = z[:quarter], z[quarter:]
            m = measured[p * quarter : (p + 1) * quarter, cols]
            factor = 1.0 - m * lax.rsqrt(zr * zr + zi * zi + EPSILON)
            a, b = split(jnp.concatenate([factor * zr, factor * zi], axis=0))
            z = dot(high[p], a) + dot(low[p], a) + dot(high[p], b)
            backs.append((z[:quarter], z[quarter:]))
        for q, (xr, xi) in enumerate(mix_inverse(backs)):
            fr[q * quarter : (q + 1) * quarter, cols] = xr
            fi[q * quarter : (q + 1) * quarter, cols] = xi

    for base in range(0, size, step):
        rows = slice(base, base + step)
        outs = []
        for p in range(4):
            cols = slice(p * quarter, (p + 1) * quarter)
            a, b = split(jnp.concatenate([fr[rows, cols], fi[rows, cols]], axis=1))
            z = dot(a, high[4 + p]) + dot(a, low[4 + p]) + dot(b, high[4 + p])
            outs.append((z[:, :quarter], z[:, quarter:]))
        grads = ([], [])
        for q, (br, bi) in enumerate(mix_inverse(outs)):
            cols = slice(q * quarter, (q + 1) * quarter)
            pr, pi = rolled[0, rows, cols], rolled[1, rows, cols]
            grads[0].append(pr * br + pi * bi)
            grads[1].append(pr * bi - pi * br)
        lane = lane_iota((step, LANES))
        for c in range(2):
            g = grads[c]
            wout = turn(jnp.where(lane >= v, g[0], 0.0))
            eout = turn(jnp.where(lane < HALF, jnp.where(lane < v, g[0], 0.0), g[3]))
            if OVL <= base < OVL + cells:
                o = base - OVL
                own[c, o : o + step, 0:128] = g[1]
                own[c, o : o + step, 128:256] = g[2]
                own[c, o : o + step, 256:cells] = g[3][:, : cells - 256]
                wedge[c, o : o + step, :] = wout
                eedge[c, o : o + step, :] = eout
                continue
            row = row_iota((step, LANES)) + base
            sends = []
            if base < OVL:
                sends.append((nblock, 0, base, row >= u if base < HALF else None))
            if base < HALF:
                sends.append((sblock, OVL, base + HALF, row < u))
            if base >= OVL + cells:
                sends.append((sblock, OVL, base - OVL - cells, None))
            for block, off, o, keep in sends:
                put = (lambda x: x) if keep is None else (lambda x: jnp.where(keep, x, 0.0))
                block[c, o : o + step, 0:128] = put(g[1])
                block[c, o : o + step, 128:256] = put(g[2])
                block[c, o : o + step, 256:384] = put(g[3])
                wcorn[c, off + o : off + o + step, :] = put(wout)
                ecorn[c, off + o : off + o + step, :] = put(eout)


def send_kernel(nblock, sblock, fromw, frome, north, south):
    first = lane_iota((OVL, LANES)) < HALF
    for base, block, out in ((0, nblock, north), (OVL, sblock, south)):
        last = []
        for c in range(2):
            fw = fromw[c, base : base + OVL, :]
            fe = frome[c, base : base + OVL, :]
            out[:, c * 256 : c * 256 + 128] = block[c, :, 0:128] + fw
            out[:, c * 256 + 128 : c * 256 + 256] = block[c, :, 128:256] + jnp.where(first, 0.0, fe)
            last.append(block[c, :, 256:384] + fe)
        out[:, 512:640] = jnp.where(first, last[0], turn(last[1]))


def light_kernel(info, probe, obj, own, fromw, frome, total, weight, pad, acc):
    size = probe.shape[-1]
    cells = own.shape[1]
    pad[...] = jnp.zeros(pad.shape, F32)
    for t in range(4):
        cols = slice(t * LANES, (t + 1) * LANES)
        x = probe[0, :, cols]
        y = probe[1, :, cols]
        pad[1 + t, OVL : OVL + size, :] = x * x + y * y
    acc[...] = jnp.zeros(acc.shape, F32)
    first = lane_iota((HALF, LANES)) < HALF
    for di in (0, -1, 1):
        for dj in (0, -1, 1):
            at = (di + 1) * 3 + (dj + 1)
            there = info[at, 2]
            u = info[at, 0]
            v = info[at, 1]
            start, count, put = {
                0: (2 * OVL - u, cells, 0),
                1: (OVL - u, OVL, cells - OVL),
                -1: (size + HALF - u, OVL, 0),
            }[di]
            seen = there.astype(F32)
            for r in range(0, count, HALF):
                rows = pl.ds(start + r, HALF)
                to = slice(put + r, put + r + HALF)
                lo, hi, shift = {0: (1, 5, 384 + v), -1: (4, 6, lax.rem(192 + v, 256)), 1: (0, 2, 128 + v)}[dj]
                x = pltpu.roll(jnp.concatenate([pad[t, rows, :] for t in range(lo, hi)], axis=1), shift, 1)
                if dj == 0:
                    x = x[:, 0:384]
                    acc[to, :] += x * seen
                    continue
                if dj == -1:
                    x = x[:, 0:128]
                    acc[to, 0:128] += x * seen
                    continue
                x = turn(x[:, 0:128]) * seen
                acc[to, 128:256] += jnp.where(first, 0.0, x)
                acc[to, 256:384] += x
    for r in range(0, cells, HALF):
        rows = slice(r, r + HALF)
        for c in range(2):
            fe = frome[c, rows, :]
            total[c, rows, 0:128] = own[c, rows, 0:128] + fromw[c, rows, :]
            total[c, rows, 128:256] = own[c, rows, 128:256] + jnp.where(first, 0.0, fe)
            total[c, rows, 256:cells] = own[c, rows, 256:cells] + fe[:, : cells - 256]
        weight[rows, :] = STEP_SIZE / (acc[rows, 0:cells] + REGULAR)


def final_kernel(obj, total, weight, fromn, froms, updated):
    cells = obj.shape[1]
    for r in range(0, cells, HALF):
        rows = slice(r, r + HALF)
        for c in range(2):
            g = [total[c, rows, 0:128], total[c, rows, 128:256], total[c, rows, 256:cells]]
            adds = []
            if r < OVL:
                adds.append((fromn, r))
            if r >= cells - OVL:
                adds.append((froms, r - cells + OVL))
            for ref, o in adds:
                src = slice(o, o + HALF)
                g[0] = g[0] + ref[src, c * 256 : c * 256 + 128]
                g[1] = g[1] + ref[src, c * 256 + 128 : c * 256 + 256]
                g[2] = g[2] + ref[src, 512 + c * HALF : 512 + c * HALF + HALF]
            for t, x in enumerate(g):
                cols = slice(128 * t, min(128 * t + 128, cells))
                updated[c, rows, cols] = obj[c, rows, cols] - x * weight[rows, cols]


def routes(axis):
    count = lax.axis_size(axis)
    up = [(i, i - 1) for i in range(1, count)]
    down = [(i, i + 1) for i in range(count - 1)]
    return up, down


def local(object_slab, probe_field, offsets, counts):
    cells = object_slab.shape[1]
    size = probe_field.shape[-1]
    up, down = routes("row")
    left, right = routes("col")
    offs = offsets.reshape(2)
    table_high, table_low = tables(size)
    high, low = jnp.asarray(table_high), jnp.asarray(table_low)

    north, south, west, east = call(
        pack_kernel,
        "pack",
        [((OVL, 640), F32), ((OVL, 640), F32), ((2, cells, OVL), F32), ((2, cells, OVL), F32)],
        0,
        [object_slab],
    )
    from_south = lax.ppermute(north, "row", up)
    from_north = lax.ppermute(south, "row", down)
    from_east = lax.ppermute(west, "col", left)
    from_west = lax.ppermute(east, "col", right)

    mine = jnp.concatenate([offs, jnp.ones((1,), jnp.int32)])
    above = lax.ppermute(mine, "row", down)
    below = lax.ppermute(mine, "row", up)
    column = jnp.stack([above, mine, below])
    lefts = lax.ppermute(column, "col", right)
    rights = lax.ppermute(column, "col", left)
    info = jnp.stack([lefts, column, rights], axis=1).reshape(9, 3)

    rolled, measured = call(
        ready_kernel,
        "ready",
        [((2, size, size), F32), ((size, size), F32)],
        1,
        [offs, probe_field, counts.reshape(size, size)],
        scratch=[pltpu.VMEM((2, 4, size + HALF, LANES), F32)],
        flops=20_000_000_000,
    )
    wcorner_out, ecorner_out = call(
        corner_kernel,
        "corner",
        [((2, 2 * OVL, OVL), F32), ((2, 2 * OVL, OVL), F32)],
        0,
        [from_north, from_south],
    )
    ecorner = lax.ppermute(wcorner_out, "col", left)
    wcorner = lax.ppermute(ecorner_out, "col", right)

    own, nblock, sblock, wedge, eedge, wcorn, ecorn = call(
        main_kernel,
        "main",
        [
            ((2, cells, cells), F32),
            ((2, OVL, 384), F32),
            ((2, OVL, 384), F32),
            ((2, cells, OVL), F32),
            ((2, cells, OVL), F32),
            ((2, 2 * OVL, OVL), F32),
            ((2, 2 * OVL, OVL), F32),
        ],
        1,
        [
            offs,
            object_slab,
            from_north,
            from_south,
            from_west,
            from_east,
            wcorner,
            ecorner,
            rolled,
            measured,
            high,
            low,
        ],
        scratch=[pltpu.VMEM((size, size), F32), pltpu.VMEM((size, size), F32)],
        flops=5_000_000_000,
    )
    corner_e = lax.ppermute(wcorn, "col", left)
    corner_w = lax.ppermute(ecorn, "col", right)
    edge_e = lax.ppermute(wedge, "col", left)
    edge_w = lax.ppermute(eedge, "col", right)
    nsend, ssend = call(
        send_kernel,
        "send",
        [((OVL, 640), F32), ((OVL, 640), F32)],
        0,
        [nblock, sblock, corner_w, corner_e],
    )
    grad_s = lax.ppermute(nsend, "row", up)
    grad_n = lax.ppermute(ssend, "row", down)
    total, weight = call(
        light_kernel,
        "light",
        [((2, cells, cells), F32), ((cells, cells), F32)],
        1,
        [info, probe_field, object_slab, own, edge_w, edge_e],
        scratch=[pltpu.VMEM((6, size + 2 * OVL, LANES), F32), pltpu.VMEM((cells, 384), F32)],
        flops=10_000_000_000,
    )
    (updated,) = call(
        final_kernel,
        "final",
        [((2, cells, cells), F32)],
        0,
        [object_slab, total, weight, grad_n, grad_s],
    )
    return updated


def solution(mesh):
    return jax.shard_map(
        local,
        mesh=mesh,
        in_specs=(
            P(None, "row", "col"),
            P(),
            P("row", "col", None, None),
            P("row", "col", None, None, None),
        ),
        out_specs=P(None, "row", "col"),
        check_vma=False,
    )
```

```python
import functools
import math

import jax
import jax.numpy as jnp
import ml_dtypes
import numpy as np
from jax import lax
from jax.experimental import pallas as pl
from jax.experimental.pallas import tpu as pltpu
from jax.sharding import PartitionSpec as P

OVL = 128
HALF = 64
LANES = 128

EPSILON = 0.01
PHOTON_SCALE = 0.01
STEP_SIZE = 0.5
REGULAR = 1.0

F32 = jnp.float32
BF16 = jnp.bfloat16


def call(kernel, out_shapes, args, smem=(), hbm_out=False, scratch=(), flops=0, limit=16):
    specs = [
        pl.BlockSpec(memory_space=pltpu.SMEM if i in smem else pltpu.VMEM) for i in range(len(args))
    ]
    args = [
        x if i in smem else pltpu.with_memory_space_constraint(x, pltpu.VMEM)
        for i, x in enumerate(args)
    ]
    return pl.pallas_call(
        kernel,
        out_shape=[
            jax.ShapeDtypeStruct(s, F32) if hbm_out else pltpu.VMEM(s, F32) for s in out_shapes
        ],
        in_specs=specs,
        out_specs=[pl.BlockSpec(memory_space=pltpu.VMEM) for _ in out_shapes],
        scratch_shapes=list(scratch),
        compiler_params=pltpu.CompilerParams(vmem_limit_bytes=limit * 1024 * 1024),
        cost_estimate=pl.CostEstimate(flops=flops, bytes_accessed=0, transcendentals=0)
        if flops
        else None,
    )(*args)


@functools.lru_cache(maxsize=None)
def tables(length):
    quarter = length // 4
    n = np.arange(quarter)[:, None]
    k = np.arange(quarter)[None, :]
    blocks = []
    for p in range(4):
        angle = 2.0 * np.pi * ((n * (4 * k + p)) % length) / length
        c = np.cos(angle) / math.sqrt(length)
        s = np.sin(angle) / math.sqrt(length)
        blocks.append(np.block([[c, -s], [s, c]]))
    blocks += [b.T for b in blocks]
    full = np.stack(blocks)
    high = full.astype(np.float32).astype(ml_dtypes.bfloat16)
    low = (full - high.astype(np.float64)).astype(np.float32).astype(ml_dtypes.bfloat16)
    return high, low


def split(x):
    high = x.astype(BF16)
    return high, (x - high.astype(F32)).astype(BF16)


def dot(a, b):
    return lax.dot_general(a, b, (((1,), (0,)), ((), ())), preferred_element_type=F32)


def mix_forward(x):
    (x0r, x0i), (x1r, x1i), (x2r, x2i), (x3r, x3i) = x
    ar, ai, br, bi = x0r + x2r, x0i + x2i, x0r - x2r, x0i - x2i
    cr, ci, dr, di = x1r + x3r, x1i + x3i, x1r - x3r, x1i - x3i
    return [(ar + cr, ai + ci), (br + di, bi - dr), (ar - cr, ai - ci), (br - di, bi + dr)]


def mix_inverse(x):
    (x0r, x0i), (x1r, x1i), (x2r, x2i), (x3r, x3i) = x
    ar, ai, br, bi = x0r + x2r, x0i + x2i, x0r - x2r, x0i - x2i
    cr, ci, dr, di = x1r + x3r, x1i + x3i, x1r - x3r, x1i - x3i
    return [(ar + cr, ai + ci), (br - di, bi + dr), (ar - cr, ai - ci), (br + di, bi - dr)]


def lane_iota(shape):
    return lax.broadcasted_iota(jnp.int32, shape, len(shape) - 1)


def row_iota(shape):
    return lax.broadcasted_iota(jnp.int32, shape, len(shape) - 2)


def turn(x):
    return pltpu.roll(x, HALF, len(x.shape) - 1)


def pack_kernel(offs, obj, north, south, west, east, mine):
    rows, cols = obj.shape[1:]
    lane = lane_iota((8, LANES))
    info = jnp.where(lane == 0, offs[0], jnp.where(lane == 1, offs[1], 1))
    mine[...] = info.astype(F32)
    for out, base in ((north, 0), (south, rows - OVL)):
        for c in range(2):
            out[:, c * 256 : c * 256 + 256] = obj[c, base : base + OVL, 0:256]
        out[:, 512 + 0 : 512 + HALF] = obj[0, base : base + OVL, 256:cols]
        out[:, 512 + HALF : 640] = obj[1, base : base + OVL, 256:cols]
    for c in range(2):
        west[c] = turn(obj[c, :, 0:128])
        east[c] = obj[c, :, cols - OVL : cols]


def corner_kernel(north, south, above, mine, below, token, west, east):
    for part, halo in ((0, north), (1, south)):
        for c in range(2):
            rows = slice((2 * c + part) * OVL, (2 * c + part) * OVL + OVL)
            west[rows, :] = turn(halo[:, c * 256 : c * 256 + 128])
            east[rows, 0:HALF] = halo[:, c * 256 + 192 : c * 256 + 256]
            east[rows, HALF:128] = halo[:, 512 + c * HALF : 512 + c * HALF + HALF]
    for out in (west, east):
        for t, ref in enumerate((above, mine, below)):
            out[4 * OVL + 8 * t : 4 * OVL + 8 * t + 8, :] = ref[...]


def ready_kernel(offs, probe, counts, rolled, measured, token, wide):
    size = probe.shape[-1]
    quarter = size // 4
    u = offs[0]
    v = offs[1]
    for c in range(2):
        for t in range(4):
            cols = slice(t * quarter, (t + 1) * quarter)
            wide[c, t, 0:HALF, :] = probe[c, size - HALF : size, cols]
            wide[c, t, HALF : HALF + size, :] = probe[c, :, cols]
        for base in range(0, size, HALF):
            rows = pl.ds(HALF - u + base, HALF)
            piece = jnp.concatenate([wide[c, t, rows, :] for t in range(4)], axis=1)
            rolled[c, base : base + HALF, :] = pltpu.roll(piece, v, 1)
    token[...] = jnp.zeros(token.shape, F32)
    r = row_iota((size, size))
    k = lane_iota((size, size))
    order = jnp.where(r == 4 * (k % quarter) + k // quarter, 1.0, 0.0).astype(BF16)
    for t in range(4):
        wide[0, t, 0:size, :] = counts[:, t * quarter : (t + 1) * quarter].astype(F32)
    for p in range(4):
        rows = jnp.concatenate([wide[0, t, pl.ds(p, quarter, stride=4), :] for t in range(4)], axis=1)
        high = jnp.floor(rows * (1.0 / 256.0))
        low = rows - 256.0 * high
        moved = 256.0 * dot(high.astype(BF16), order) + dot(low.astype(BF16), order)
        measured[p * quarter : (p + 1) * quarter, :] = jnp.sqrt(moved * PHOTON_SCALE)


def main_kernel(
    offs, obj, north, south, west, east, wcorner, ecorner, rolled, measured, high, low,
    own, nblock, sblock, wedge, eedge, wcorn, ecorn, fr, fi,
):
    size = rolled.shape[-1]
    quarter = size // 4
    cells = obj.shape[1]
    u = offs[0]
    v = offs[1]

    def pieces(c, part, base, count):
        lane = lane_iota((count, LANES))
        if part == "own":
            tiles = [obj[c, base : base + count, 0:128], obj[c, base : base + count, 128:256]]
            last = obj[c, base : base + count, 256:cells]
            last = jnp.concatenate([last, last], axis=1)
            w = west[c, base : base + count, :]
            e = east[c, base : base + count, :]
        else:
            ref, start = (north, base) if part == "n" else (south, base)
            tiles = [ref[start : start + count, c * 256 + 128 * t : c * 256 + 128 * t + 128] for t in range(2)]
            last = ref[start : start + count, 512:640]
            if c == 1:
                last = turn(last)
            start = start + (2 * c + (part == "s")) * OVL
            w = wcorner[start : start + count, :]
            e = ecorner[start : start + count, :]
        return [jnp.where(lane < v, e, w), tiles[0], tiles[1], jnp.where(lane < HALF, last, e)]

    def patch(c, slot, count):
        if slot < HALF:
            row = row_iota((count, LANES)) + slot
            a = pieces(c, "n", slot, count)
            b = pieces(c, "s", slot + HALF, count)
            return [jnp.where(row < u, y, x) for x, y in zip(a, b)]
        if slot < OVL:
            return pieces(c, "n", slot, count)
        if slot < OVL + cells:
            return pieces(c, "own", slot - OVL, count)
        return pieces(c, "s", slot - OVL - cells, count)

    step = 64
    for base in range(0, size, step):
        rows = slice(base, base + step)
        orr, oi = patch(0, base, step), patch(1, base, step)
        exits = []
        for q in range(4):
            cols = slice(q * quarter, (q + 1) * quarter)
            pr, pi = rolled[0, rows, cols], rolled[1, rows, cols]
            exits.append((pr * orr[q] - pi * oi[q], pr * oi[q] + pi * orr[q]))
        for p, (yr, yi) in enumerate(mix_forward(exits)):
            a, b = split(jnp.concatenate([yr, yi], axis=1))
            z = dot(a, high[p]) + dot(a, low[p]) + dot(b, high[p])
            cols = slice(p * quarter, (p + 1) * quarter)
            fr[rows, cols] = z[:, :quarter]
            fi[rows, cols] = z[:, quarter:]

    for cb in range(4):
        cols = slice(cb * quarter, (cb + 1) * quarter)
        quads = [
            (fr[q * quarter : (q + 1) * quarter, cols], fi[q * quarter : (q + 1) * quarter, cols])
            for q in range(4)
        ]
        backs = []
        for p, (yr, yi) in enumerate(mix_forward(quads)):
            a, b = split(jnp.concatenate([yr, yi], axis=0))
            z = dot(high[4 + p], a) + dot(low[4 + p], a) + dot(high[4 + p], b)
            zr, zi = z[:quarter], z[quarter:]
            m = measured[p * quarter : (p + 1) * quarter, cols]
            factor = 1.0 - m * lax.rsqrt(zr * zr + zi * zi + EPSILON)
            a, b = split(jnp.concatenate([factor * zr, factor * zi], axis=0))
            z = dot(high[p], a) + dot(low[p], a) + dot(high[p], b)
            backs.append((z[:quarter], z[quarter:]))
        for q, (xr, xi) in enumerate(mix_inverse(backs)):
            fr[q * quarter : (q + 1) * quarter, cols] = xr
            fi[q * quarter : (q + 1) * quarter, cols] = xi

    for base in range(0, size, step):
        rows = slice(base, base + step)
        outs = []
        for p in range(4):
            cols = slice(p * quarter, (p + 1) * quarter)
            a, b = split(jnp.concatenate([fr[rows, cols], fi[rows, cols]], axis=1))
            z = dot(a, high[4 + p]) + dot(a, low[4 + p]) + dot(b, high[4 + p])
            outs.append((z[:, :quarter], z[:, quarter:]))
        grads = ([], [])
        for q, (br, bi) in enumerate(mix_inverse(outs)):
            cols = slice(q * quarter, (q + 1) * quarter)
            pr, pi = rolled[0, rows, cols], rolled[1, rows, cols]
            grads[0].append(pr * br + pi * bi)
            grads[1].append(pr * bi - pi * br)
        lane = lane_iota((step, LANES))
        for c in range(2):
            g = grads[c]
            wout = turn(jnp.where(lane >= v, g[0], 0.0))
            eout = turn(jnp.where(lane < HALF, jnp.where(lane < v, g[0], 0.0), g[3]))
            if OVL <= base < OVL + cells:
                o = base - OVL
                own[c, o : o + step, 0:128] = g[1]
                own[c, o : o + step, 128:256] = g[2]
                own[c, o : o + step, 256:cells] = g[3][:, : cells - 256]
                wedge[c, o : o + step, :] = wout
                eedge[c, o : o + step, :] = eout
                continue
            row = row_iota((step, LANES)) + base
            sends = []
            if base < OVL:
                sends.append((nblock, 0, base, row >= u if base < HALF else None))
            if base < HALF:
                sends.append((sblock, OVL, base + HALF, row < u))
            if base >= OVL + cells:
                sends.append((sblock, OVL, base - OVL - cells, None))
            for block, off, o, keep in sends:
                put = (lambda x: x) if keep is None else (lambda x: jnp.where(keep, x, 0.0))
                block[c, o : o + step, 0:128] = put(g[1])
                block[c, o : o + step, 128:256] = put(g[2])
                block[c, o : o + step, 256:384] = put(g[3])
                wcorn[c, off + o : off + o + step, :] = put(wout)
                ecorn[c, off + o : off + o + step, :] = put(eout)


def send_kernel(nblock, sblock, fromw, frome, north, south):
    first = lane_iota((OVL, LANES)) < HALF
    for base, block, out in ((0, nblock, north), (OVL, sblock, south)):
        last = []
        for c in range(2):
            fw = fromw[c, base : base + OVL, :]
            fe = frome[c, base : base + OVL, :]
            out[:, c * 256 : c * 256 + 128] = block[c, :, 0:128] + fw
            out[:, c * 256 + 128 : c * 256 + 256] = block[c, :, 128:256] + jnp.where(first, 0.0, fe)
            last.append(block[c, :, 256:384] + fe)
        out[:, 512:640] = jnp.where(first, last[0], turn(last[1]))


def light_kernel(
    wcorner, ecorner, above, mine, below, probe, own, fromw, frome, total, weight, pad, acc
):
    size = probe.shape[-1]
    cells = own.shape[1]
    pad[...] = jnp.zeros(pad.shape, F32)
    for t in range(4):
        cols = slice(t * LANES, (t + 1) * LANES)
        x = probe[0, :, cols]
        y = probe[1, :, cols]
        pad[1 + t, OVL : OVL + size, :] = x * x + y * y
    acc[...] = jnp.zeros(acc.shape, F32)
    first = lane_iota((HALF, LANES)) < HALF
    unit = row_iota((8, LANES)) == 0
    lane = lane_iota((8, LANES))
    for di in (0, -1, 1):
        for dj in (0, -1, 1):
            if dj == 0:
                tile = (above, mine, below)[di + 1][...]
            else:
                tile = (wcorner if dj < 0 else ecorner)[4 * OVL + 8 * (di + 1) : 4 * OVL + 8 * (di + 2), :]
            u, v, there = [jnp.sum(jnp.where(unit & (lane == i), tile, 0.0)) for i in range(3)]
            u, v = u.astype(jnp.int32), v.astype(jnp.int32)
            start, count, put = {
                0: (2 * OVL - u, cells, 0),
                1: (OVL - u, OVL, cells - OVL),
                -1: (size + HALF - u, OVL, 0),
            }[di]
            seen = there
            for r in range(0, count, HALF):
                rows = pl.ds(start + r, HALF)
                to = slice(put + r, put + r + HALF)
                lo, hi, shift = {0: (1, 5, 384 + v), -1: (4, 6, lax.rem(192 + v, 256)), 1: (0, 2, 128 + v)}[dj]
                x = pltpu.roll(jnp.concatenate([pad[t, rows, :] for t in range(lo, hi)], axis=1), shift, 1)
                if dj == 0:
                    x = x[:, 0:384]
                    acc[to, :] += x * seen
                    continue
                if dj == -1:
                    x = x[:, 0:128]
                    acc[to, 0:128] += x * seen
                    continue
                x = turn(x[:, 0:128]) * seen
                acc[to, 128:256] += jnp.where(first, 0.0, x)
                acc[to, 256:384] += x
    for r in range(0, cells, HALF):
        rows = slice(r, r + HALF)
        for c in range(2):
            fe = frome[c, rows, :]
            total[c, rows, 0:128] = own[c, rows, 0:128] + fromw[c, rows, :]
            total[c, rows, 128:256] = own[c, rows, 128:256] + jnp.where(first, 0.0, fe)
            total[c, rows, 256:cells] = own[c, rows, 256:cells] + fe[:, : cells - 256]
        weight[rows, :] = STEP_SIZE / (acc[rows, 0:cells] + REGULAR)


def final_kernel(obj, total, weight, fromn, froms, updated):
    cells = obj.shape[1]
    for r in range(0, cells, HALF):
        rows = slice(r, r + HALF)
        for c in range(2):
            g = [total[c, rows, 0:128], total[c, rows, 128:256], total[c, rows, 256:cells]]
            adds = []
            if r < OVL:
                adds.append((fromn, r))
            if r >= cells - OVL:
                adds.append((froms, r - cells + OVL))
            for ref, o in adds:
                src = slice(o, o + HALF)
                g[0] = g[0] + ref[src, c * 256 : c * 256 + 128]
                g[1] = g[1] + ref[src, c * 256 + 128 : c * 256 + 256]
                g[2] = g[2] + ref[src, 512 + c * HALF : 512 + c * HALF + HALF]
            for t, x in enumerate(g):
                cols = slice(128 * t, min(128 * t + 128, cells))
                updated[c, rows, cols] = obj[c, rows, cols] - x * weight[rows, cols]


def routes(axis):
    count = lax.axis_size(axis)
    up = [(i, i - 1) for i in range(1, count)]
    down = [(i, i + 1) for i in range(count - 1)]
    return up, down


def local(object_slab, probe_field, offsets, counts):
    cells = object_slab.shape[1]
    size = probe_field.shape[-1]
    up, down = routes("row")
    left, right = routes("col")
    offs = offsets.reshape(2)
    table_high, table_low = tables(size)
    high, low = jnp.asarray(table_high), jnp.asarray(table_low)

    north, south, west, east, mine = call(
        pack_kernel,
        [(OVL, 640), (OVL, 640), (2, cells, OVL), (2, cells, OVL), (8, LANES)],
        [offs, object_slab],
        smem=(0,),
    )
    from_south = lax.ppermute(north, "row", up)
    from_north = lax.ppermute(south, "row", down)
    from_east = lax.ppermute(west, "col", left)
    from_west = lax.ppermute(east, "col", right)
    above = lax.ppermute(mine, "row", down)
    below = lax.ppermute(mine, "row", up)

    rolled, measured, token = call(
        ready_kernel,
        [(2, size, size), (size, size), (8, LANES)],
        [offs, probe_field, counts.reshape(size, size)],
        smem=(0,),
        scratch=[pltpu.VMEM((2, 4, size + HALF, LANES), F32)],
        flops=20_000_000_000,
    )
    wcorner_out, ecorner_out = call(
        corner_kernel,
        [(4 * OVL + 24, OVL), (4 * OVL + 24, OVL)],
        [from_north, from_south, above, mine, below, token],
    )
    ecorner = lax.ppermute(wcorner_out, "col", left)
    wcorner = lax.ppermute(ecorner_out, "col", right)

    own, nblock, sblock, wedge, eedge, wcorn, ecorn = call(
        main_kernel,
        [
            (2, cells, cells),
            (2, OVL, 384),
            (2, OVL, 384),
            (2, cells, OVL),
            (2, cells, OVL),
            (2, 2 * OVL, OVL),
            (2, 2 * OVL, OVL),
        ],
        [
            offs,
            object_slab,
            from_north,
            from_south,
            from_west,
            from_east,
            wcorner,
            ecorner,
            rolled,
            measured,
            high,
            low,
        ],
        smem=(0,),
        scratch=[pltpu.VMEM((size, size), F32), pltpu.VMEM((size, size), F32)],
        flops=5_000_000_000,
    )
    corner_e = lax.ppermute(wcorn, "col", left)
    corner_w = lax.ppermute(ecorn, "col", right)
    nsend, ssend = call(send_kernel, [(OVL, 640), (OVL, 640)], [nblock, sblock, corner_w, corner_e])
    grad_s = lax.ppermute(nsend, "row", up)
    grad_n = lax.ppermute(ssend, "row", down)
    edge_e = lax.ppermute(wedge, "col", left)
    edge_w = lax.ppermute(eedge, "col", right)
    total, weight = call(
        light_kernel,
        [(2, cells, cells), (cells, cells)],
        [wcorner, ecorner, above, mine, below, probe_field, own, edge_w, edge_e],
        scratch=[pltpu.VMEM((6, size + 2 * OVL, LANES), F32), pltpu.VMEM((cells, 384), F32)],
        flops=10_000_000_000,
    )
    (updated,) = call(
        final_kernel,
        [(2, cells, cells)],
        [object_slab, total, weight, grad_n, grad_s],
        hbm_out=True,
    )
    return updated


def solution(mesh):
    return jax.shard_map(
        local,
        mesh=mesh,
        in_specs=(
            P(None, "row", "col"),
            P(),
            P("row", "col", None, None),
            P("row", "col", None, None, None),
        ),
        out_specs=P(None, "row", "col"),
        check_vma=False,
    )
```

```python
import functools
import math

import jax
import jax.numpy as jnp
import ml_dtypes
import numpy as np
from jax import lax
from jax.experimental import pallas as pl
from jax.experimental.pallas import tpu as pltpu
from jax.sharding import PartitionSpec as P

OVL = 128
HALF = 64
LANES = 128

EPSILON = 0.01
PHOTON_SCALE = 0.01
STEP_SIZE = 0.5
REGULAR = 1.0

F32 = jnp.float32
BF16 = jnp.bfloat16


def call(kernel, out_shapes, args, smem=(), hbm_out=False, scratch=(), flops=0, limit=16):
    specs = [
        pl.BlockSpec(memory_space=pltpu.SMEM if i in smem else pltpu.VMEM) for i in range(len(args))
    ]
    args = [
        x if i in smem else pltpu.with_memory_space_constraint(x, pltpu.VMEM)
        for i, x in enumerate(args)
    ]
    return pl.pallas_call(
        kernel,
        out_shape=[
            jax.ShapeDtypeStruct(s, F32) if hbm_out else pltpu.VMEM(s, F32) for s in out_shapes
        ],
        in_specs=specs,
        out_specs=[pl.BlockSpec(memory_space=pltpu.VMEM) for _ in out_shapes],
        scratch_shapes=list(scratch),
        compiler_params=pltpu.CompilerParams(vmem_limit_bytes=limit * 1024 * 1024),
        cost_estimate=pl.CostEstimate(flops=flops, bytes_accessed=0, transcendentals=0)
        if flops
        else None,
    )(*args)


@functools.lru_cache(maxsize=None)
def tables(length):
    quarter = length // 4
    n = np.arange(quarter)[:, None]
    k = np.arange(quarter)[None, :]
    blocks = []
    for p in range(4):
        angle = 2.0 * np.pi * ((n * (4 * k + p)) % length) / length
        c = np.cos(angle) / math.sqrt(length)
        s = np.sin(angle) / math.sqrt(length)
        blocks.append(np.block([[c, -s], [s, c]]))
    blocks += [b.T for b in blocks]
    full = np.stack(blocks)
    high = full.astype(np.float32).astype(ml_dtypes.bfloat16)
    low = (full - high.astype(np.float64)).astype(np.float32).astype(ml_dtypes.bfloat16)
    return high, low


def split(x):
    high = x.astype(BF16)
    return high, (x - high.astype(F32)).astype(BF16)


def dot(a, b):
    return lax.dot_general(a, b, (((1,), (0,)), ((), ())), preferred_element_type=F32)


def mix_forward(x):
    (x0r, x0i), (x1r, x1i), (x2r, x2i), (x3r, x3i) = x
    ar, ai, br, bi = x0r + x2r, x0i + x2i, x0r - x2r, x0i - x2i
    cr, ci, dr, di = x1r + x3r, x1i + x3i, x1r - x3r, x1i - x3i
    return [(ar + cr, ai + ci), (br + di, bi - dr), (ar - cr, ai - ci), (br - di, bi + dr)]


def mix_inverse(x):
    (x0r, x0i), (x1r, x1i), (x2r, x2i), (x3r, x3i) = x
    ar, ai, br, bi = x0r + x2r, x0i + x2i, x0r - x2r, x0i - x2i
    cr, ci, dr, di = x1r + x3r, x1i + x3i, x1r - x3r, x1i - x3i
    return [(ar + cr, ai + ci), (br - di, bi + dr), (ar - cr, ai - ci), (br + di, bi - dr)]


def lane_iota(shape):
    return lax.broadcasted_iota(jnp.int32, shape, len(shape) - 1)


def row_iota(shape):
    return lax.broadcasted_iota(jnp.int32, shape, len(shape) - 2)


def turn(x):
    return pltpu.roll(x, HALF, len(x.shape) - 1)


def odd():
    return lax.axis_index("col") % 2 == 1


def pack_kernel(offs, obj, north, south, xside, dside):
    rows, cols = obj.shape[1:]
    lane = lane_iota((8, LANES))
    info = jnp.where(lane == 0, offs[0], jnp.where(lane == 1, offs[1], 1)).astype(F32)
    for out, base in ((north, 0), (south, rows - OVL)):
        for c in range(2):
            out[0:OVL, c * 256 : c * 256 + 256] = obj[c, base : base + OVL, 0:256]
            out[0:OVL, 512 + c * HALF : 512 + c * HALF + HALF] = obj[c, base : base + OVL, 256:cols]
        out[OVL : OVL + 8, 0:128] = info
        out[OVL : OVL + 8, 128:640] = jnp.zeros((8, 512), F32)
    right = odd()
    for c in range(2):
        west = turn(obj[c, :, 0:128])
        east = obj[c, :, cols - OVL : cols]
        xside[c] = jnp.where(right, east, west)
        dside[c] = jnp.where(right, west, east)


def corner_kernel(offs, north, south, token, xside, dside):
    right = odd()
    for part, halo in ((0, north), (1, south)):
        for c in range(2):
            rows = slice((2 * c + part) * OVL, (2 * c + part) * OVL + OVL)
            west = turn(halo[0:OVL, c * 256 : c * 256 + 128])
            lane = lane_iota((OVL, LANES))
            tail = halo[0:OVL, 512:640]
            if c == 0:
                tail = turn(tail)
            east = jnp.where(lane < HALF, turn(halo[0:OVL, c * 256 + 128 : c * 256 + 256]), tail)
            xside[rows, :] = jnp.where(right, east, west)
            dside[rows, :] = jnp.where(right, west, east)
    lane = lane_iota((8, LANES))
    info = jnp.where(lane == 0, offs[0], jnp.where(lane == 1, offs[1], 1)).astype(F32)
    for out in (xside, dside):
        out[4 * OVL : 4 * OVL + 8, :] = north[OVL : OVL + 8, 0:128]
        out[4 * OVL + 8 : 4 * OVL + 16, :] = info
        out[4 * OVL + 16 : 4 * OVL + 24, :] = south[OVL : OVL + 8, 0:128]


def ready_kernel(offs, probe, counts, rolled, measured, token, wide):
    size = probe.shape[-1]
    quarter = size // 4
    u = offs[0]
    v = offs[1]
    for c in range(2):
        for t in range(4):
            cols = slice(t * quarter, (t + 1) * quarter)
            wide[c, t, 0:HALF, :] = probe[c, size - HALF : size, cols]
            wide[c, t, HALF : HALF + size, :] = probe[c, :, cols]
        for base in range(0, size, HALF):
            rows = pl.ds(HALF - u + base, HALF)
            piece = jnp.concatenate([wide[c, t, rows, :] for t in range(4)], axis=1)
            rolled[c, base : base + HALF, :] = pltpu.roll(piece, v, 1)
    token[...] = jnp.zeros(token.shape, F32)
    r = row_iota((size, size))
    k = lane_iota((size, size))
    order = jnp.where(r == 4 * (k % quarter) + k // quarter, 1.0, 0.0).astype(BF16)
    for t in range(4):
        wide[0, t, 0:size, :] = counts[:, t * quarter : (t + 1) * quarter].astype(F32)
    for p in range(4):
        rows = jnp.concatenate([wide[0, t, pl.ds(p, quarter, stride=4), :] for t in range(4)], axis=1)
        high = jnp.floor(rows * (1.0 / 256.0))
        low = rows - 256.0 * high
        moved = 256.0 * dot(high.astype(BF16), order) + dot(low.astype(BF16), order)
        measured[p * quarter : (p + 1) * quarter, :] = jnp.sqrt(moved * PHOTON_SCALE)


def main_kernel(
    offs, obj, north, south, xside, dside, xcorner, dcorner, rolled, measured, high, low,
    own, nblock, sblock, xedge, dedge, xcorn, dcorn, ah, al, bh, bl, zf, tf,
):
    size = rolled.shape[-1]
    quarter = size // 4
    cells = obj.shape[1]
    u = offs[0]
    v = offs[1]
    right = odd()

    def pieces(c, part, base, count):
        lane = lane_iota((count, LANES))
        if part == "own":
            tiles = [obj[c, base : base + count, 0:128], obj[c, base : base + count, 128:256]]
            last = obj[c, base : base + count, 256:cells]
            last = jnp.concatenate([last, last], axis=1)
            x = xside[c, base : base + count, :]
            d = dside[c, base : base + count, :]
        else:
            ref, start = (north, base) if part == "n" else (south, base)
            tiles = [ref[start : start + count, c * 256 + 128 * t : c * 256 + 128 * t + 128] for t in range(2)]
            last = ref[start : start + count, 512:640]
            if c == 1:
                last = turn(last)
            start = start + (2 * c + (part == "s")) * OVL
            x = xcorner[start : start + count, :]
            d = dcorner[start : start + count, :]
        w, e = jnp.where(right, d, x), jnp.where(right, x, d)
        return [jnp.where(lane < v, e, w), tiles[0], tiles[1], jnp.where(lane < HALF, last, e)]

    def patch(c, slot, count):
        if slot < HALF:
            row = row_iota((count, LANES)) + slot
            a = pieces(c, "n", slot, count)
            b = pieces(c, "s", slot + HALF, count)
            return [jnp.where(row < u, y, x) for x, y in zip(a, b)]
        if slot < OVL:
            return pieces(c, "n", slot, count)
        if slot < OVL + cells:
            return pieces(c, "own", slot - OVL, count)
        return pieces(c, "s", slot - OVL - cells, count)

    def keep(hi, lo, at, x):
        hi[at], lo[at] = split(x)

    step = 32
    block = 256
    re, im = slice(0, quarter), slice(quarter, 2 * quarter)

    for top in range(0, size, block):
        for base in range(top, top + block, step):
            rows = slice(base, base + step)
            pr, pi = patch(0, base, step), patch(1, base, step)
            exits = []
            for q in range(4):
                cols = slice(q * quarter, (q + 1) * quarter)
                ar, ai = rolled[0, rows, cols], rolled[1, rows, cols]
                exits.append((ar * pr[q] - ai * pi[q], ar * pi[q] + ai * pr[q]))
            for p, (yr, yi) in enumerate(mix_forward(exits)):
                keep(ah, al, (p, rows, re), yr)
                keep(ah, al, (p, rows, im), yi)
        rows = slice(top, top + block)
        for p in range(4):
            a = ah[p, rows, :]
            zf[p, rows, :] = dot(a, high[p]) + dot(al[p, rows, :], high[p]) + dot(a, low[p])

    for half in range(2):
        pair = (2 * half, 2 * half + 1)
        for t, p in enumerate(pair):
            cols = slice(t * quarter, (t + 1) * quarter)
            for r in range(0, quarter, step):
                quads = []
                for q in range(4):
                    rows = slice(q * quarter + r, q * quarter + r + step)
                    quads.append((zf[p, rows, re], zf[p, rows, im]))
                for k, (yr, yi) in enumerate(mix_forward(quads)):
                    keep(bh, bl, (half, k, slice(r, r + step), cols), yr)
                    keep(bh, bl, (half, k, slice(quarter + r, quarter + r + step), cols), yi)
        for k in range(4):
            a = bh[half, k]
            z = dot(high[4 + k], a) + dot(high[4 + k], bl[half, k]) + dot(low[4 + k], a)
            zr, zi = z[re], z[im]
            m = measured[k * quarter : (k + 1) * quarter, half * block : (half + 1) * block]
            factor = 1.0 - m * lax.rsqrt(zr * zr + zi * zi + EPSILON)
            keep(bh, bl, (half, k, re), factor * zr)
            keep(bh, bl, (half, k, im), factor * zi)
        for k in range(4):
            a = bh[half, k]
            tf[half, k] = dot(high[k], a) + dot(high[k], bl[half, k]) + dot(low[k], a)
        for t, p in enumerate(pair):
            cols = slice(t * quarter, (t + 1) * quarter)
            for r in range(0, quarter, step):
                quads = [
                    (
                        tf[half, k, r : r + step, cols],
                        tf[half, k, quarter + r : quarter + r + step, cols],
                    )
                    for k in range(4)
                ]
                for q, (yr, yi) in enumerate(mix_inverse(quads)):
                    rows = slice(q * quarter + r, q * quarter + r + step)
                    keep(ah, al, (p, rows, re), yr)
                    keep(ah, al, (p, rows, im), yi)

    for top in (0, block):
        rows = slice(top, top + block)
        for p in range(4):
            a = ah[p, rows, :]
            zf[p, rows, :] = dot(a, high[4 + p]) + dot(al[p, rows, :], high[4 + p]) + dot(a, low[4 + p])
        for base in range(top, top + block, step):
            rows = slice(base, base + step)
            quads = [(zf[p, rows, re], zf[p, rows, im]) for p in range(4)]
            grads = ([], [])
            for q, (br, bi) in enumerate(mix_inverse(quads)):
                cols = slice(q * quarter, (q + 1) * quarter)
                ar, ai = rolled[0, rows, cols], rolled[1, rows, cols]
                grads[0].append(ar * br + ai * bi)
                grads[1].append(ar * bi - ai * br)
            lane = lane_iota((step, LANES))
            for c in range(2):
                g = grads[c]
                wout = turn(jnp.where(lane >= v, g[0], 0.0))
                eout = turn(jnp.where(lane < HALF, jnp.where(lane < v, g[0], 0.0), g[3]))
                xout, dout = jnp.where(right, eout, wout), jnp.where(right, wout, eout)
                if OVL <= base < OVL + cells:
                    o = base - OVL
                    own[c, o : o + step, 0:128] = g[1]
                    own[c, o : o + step, 128:256] = g[2]
                    own[c, o : o + step, 256:cells] = g[3][:, : cells - 256]
                    xedge[c, o : o + step, :] = xout
                    dedge[c, o : o + step, :] = dout
                    continue
                row = row_iota((step, LANES)) + base
                sends = []
                if base < OVL:
                    sends.append((nblock, 0, base, row >= u if base < HALF else None))
                if base < HALF:
                    sends.append((sblock, OVL, base + HALF, row < u))
                if base >= OVL + cells:
                    sends.append((sblock, OVL, base - OVL - cells, None))
                for out, off, o, mask in sends:
                    put = (lambda x: x) if mask is None else (lambda x: jnp.where(mask, x, 0.0))
                    out[c, o : o + step, 0:128] = put(g[1])
                    out[c, o : o + step, 128:256] = put(g[2])
                    out[c, o : o + step, 256:384] = put(g[3])
                    xcorn[c, off + o : off + o + step, :] = put(xout)
                    dcorn[c, off + o : off + o + step, :] = put(dout)


def send_kernel(nblock, sblock, xcorn, dcorn, north, south):
    right = odd()
    first = lane_iota((OVL, LANES)) < HALF
    for base, block, out in ((0, nblock, north), (OVL, sblock, south)):
        last = []
        for c in range(2):
            x = xcorn[c, base : base + OVL, :]
            d = dcorn[c, base : base + OVL, :]
            fw, fe = jnp.where(right, d, x), jnp.where(right, x, d)
            out[:, c * 256 : c * 256 + 128] = block[c, :, 0:128] + fw
            out[:, c * 256 + 128 : c * 256 + 256] = block[c, :, 128:256] + jnp.where(first, 0.0, fe)
            last.append(block[c, :, 256:384] + fe)
        out[:, 512:640] = jnp.where(first, last[0], turn(last[1]))


def light_kernel(
    offs, xcorner, dcorner, north, south, probe, own, xedge, dedge, total, weight, pad, acc
):
    size = probe.shape[-1]
    cells = own.shape[1]
    pad[...] = jnp.zeros(pad.shape, F32)
    for t in range(4):
        cols = slice(t * LANES, (t + 1) * LANES)
        x = probe[0, :, cols]
        y = probe[1, :, cols]
        pad[1 + t, OVL : OVL + size, :] = x * x + y * y
    acc[...] = jnp.zeros(acc.shape, F32)
    first = lane_iota((HALF, LANES)) < HALF
    right = odd()
    unit = row_iota((8, LANES)) == 0
    lane = lane_iota((8, LANES))
    for di in (0, -1, 1):
        for dj in (0, -1, 1):
            if di == 0 and dj == 0:
                u, v, there = offs[0], offs[1], 1.0
            else:
                at = slice(4 * OVL + 8 * (di + 1), 4 * OVL + 8 * (di + 2))
                if dj == 0:
                    tile = (north if di < 0 else south)[OVL : OVL + 8, 0:128]
                elif dj < 0:
                    tile = jnp.where(right, dcorner[at, :], xcorner[at, :])
                else:
                    tile = jnp.where(right, xcorner[at, :], dcorner[at, :])
                u, v, there = [jnp.sum(jnp.where(unit & (lane == i), tile, 0.0)) for i in range(3)]
                u, v = u.astype(jnp.int32), v.astype(jnp.int32)
            start, count, put = {
                0: (2 * OVL - u, cells, 0),
                1: (OVL - u, OVL, cells - OVL),
                -1: (size + HALF - u, OVL, 0),
            }[di]
            seen = there
            for r in range(0, count, HALF):
                rows = pl.ds(start + r, HALF)
                to = slice(put + r, put + r + HALF)
                lo, hi, shift = {0: (1, 5, 384 + v), -1: (4, 6, lax.rem(192 + v, 256)), 1: (0, 2, 128 + v)}[dj]
                x = pltpu.roll(jnp.concatenate([pad[t, rows, :] for t in range(lo, hi)], axis=1), shift, 1)
                if dj == 0:
                    x = x[:, 0:384]
                    acc[to, :] += x * seen
                    continue
                if dj == -1:
                    x = x[:, 0:128]
                    acc[to, 0:128] += x * seen
                    continue
                x = turn(x[:, 0:128]) * seen
                acc[to, 128:256] += jnp.where(first, 0.0, x)
                acc[to, 256:384] += x
    for r in range(0, cells, HALF):
        rows = slice(r, r + HALF)
        for c in range(2):
            x, d = xedge[c, rows, :], dedge[c, rows, :]
            fw, fe = jnp.where(right, d, x), jnp.where(right, x, d)
            total[c, rows, 0:128] = own[c, rows, 0:128] + fw
            total[c, rows, 128:256] = own[c, rows, 128:256] + jnp.where(first, 0.0, fe)
            total[c, rows, 256:cells] = own[c, rows, 256:cells] + fe[:, : cells - 256]
        weight[rows, :] = STEP_SIZE / (acc[rows, 0:cells] + REGULAR)


def final_kernel(obj, total, weight, fromn, froms, updated):
    cells = obj.shape[1]
    for r in range(0, cells, HALF):
        rows = slice(r, r + HALF)
        for c in range(2):
            g = [total[c, rows, 0:128], total[c, rows, 128:256], total[c, rows, 256:cells]]
            adds = []
            if r < OVL:
                adds.append((fromn, r))
            if r >= cells - OVL:
                adds.append((froms, r - cells + OVL))
            for ref, o in adds:
                src = slice(o, o + HALF)
                g[0] = g[0] + ref[src, c * 256 : c * 256 + 128]
                g[1] = g[1] + ref[src, c * 256 + 128 : c * 256 + 256]
                g[2] = g[2] + ref[src, 512 + c * HALF : 512 + c * HALF + HALF]
            for t, x in enumerate(g):
                cols = slice(128 * t, min(128 * t + 128, cells))
                updated[c, rows, cols] = obj[c, rows, cols] - x * weight[rows, cols]


def routes(axis):
    count = lax.axis_size(axis)
    up = [(i, i - 1) for i in range(1, count)]
    down = [(i, i + 1) for i in range(count - 1)]
    swaps = [
        [pair for i in range(first, count - 1, 2) for pair in ((i, i + 1), (i + 1, i))]
        for first in (1, 0)
    ]
    return up, down, *swaps


def local(object_slab, probe_field, offsets, counts):
    cells = object_slab.shape[1]
    size = probe_field.shape[-1]
    up, down, _, _ = routes("row")
    _, _, cross, inner = routes("col")
    offs = offsets.reshape(2)
    table_high, table_low = tables(size)
    high, low = jnp.asarray(table_high), jnp.asarray(table_low)

    north, south, west, east = call(
        pack_kernel,
        [(OVL + 8, 640), (OVL + 8, 640), (2, cells, OVL), (2, cells, OVL)],
        [offs, object_slab],
        smem=(0,),
    )
    from_south = lax.ppermute(north, "row", up)
    from_north = lax.ppermute(south, "row", down)
    side_x = lax.ppermute(west, "col", cross)
    side_d = lax.ppermute(east, "col", inner)

    rolled, measured, token = call(
        ready_kernel,
        [(2, size, size), (size, size), (8, LANES)],
        [offs, probe_field, counts.reshape(size, size)],
        smem=(0,),
        scratch=[pltpu.VMEM((2, 4, size + HALF, LANES), F32)],
        flops=20_000_000_000,
    )
    xcorner, dcorner = call(
        corner_kernel,
        [(4 * OVL + 24, OVL), (4 * OVL + 24, OVL)],
        [offs, from_north, from_south, token],
        smem=(0,),
    )
    corner_x = lax.ppermute(xcorner, "col", cross)
    corner_d = lax.ppermute(dcorner, "col", inner)

    own, nblock, sblock, xedge, dedge, xcorn, dcorn = call(
        main_kernel,
        [
            (2, cells, cells),
            (2, OVL, 384),
            (2, OVL, 384),
            (2, cells, OVL),
            (2, cells, OVL),
            (2, 2 * OVL, OVL),
            (2, 2 * OVL, OVL),
        ],
        [
            offs,
            object_slab,
            from_north,
            from_south,
            side_x,
            side_d,
            corner_x,
            corner_d,
            rolled,
            measured,
            high,
            low,
        ],
        smem=(0,),
        scratch=[
            pltpu.VMEM((4, size, size // 2), BF16),
            pltpu.VMEM((4, size, size // 2), BF16),
            pltpu.VMEM((2, 4, size // 2, size // 2), BF16),
            pltpu.VMEM((2, 4, size // 2, size // 2), BF16),
            pltpu.VMEM((4, size, size // 2), F32),
            pltpu.VMEM((2, 4, size // 2, size // 2), F32),
        ],
        flops=5_000_000_000,
        limit=20,
    )
    fix_x = lax.ppermute(xcorn, "col", cross)
    fix_d = lax.ppermute(dcorn, "col", inner)
    nsend, ssend = call(send_kernel, [(OVL, 640), (OVL, 640)], [nblock, sblock, fix_x, fix_d])
    grad_s = lax.ppermute(nsend, "row", up)
    grad_n = lax.ppermute(ssend, "row", down)
    edge_x = lax.ppermute(xedge, "col", cross)
    edge_d = lax.ppermute(dedge, "col", inner)
    total, weight = call(
        light_kernel,
        [(2, cells, cells), (cells, cells)],
        [offs, corner_x, corner_d, from_north, from_south, probe_field, own, edge_x, edge_d],
        smem=(0,),
        scratch=[pltpu.VMEM((6, size + 2 * OVL, LANES), F32), pltpu.VMEM((cells, 384), F32)],
        flops=10_000_000_000,
    )
    (updated,) = call(
        final_kernel,
        [(2, cells, cells)],
        [object_slab, total, weight, grad_n, grad_s],
        hbm_out=True,
    )
    return updated


def solution(mesh):
    return jax.shard_map(
        local,
        mesh=mesh,
        in_specs=(
            P(None, "row", "col"),
            P(),
            P("row", "col", None, None),
            P("row", "col", None, None, None),
        ),
        out_specs=P(None, "row", "col"),
        check_vma=False,
    )
```

```python
import functools
import math

import jax
import jax.numpy as jnp
import ml_dtypes
import numpy as np
from jax import lax
from jax.experimental import pallas as pl
from jax.experimental.pallas import tpu as pltpu
from jax.sharding import PartitionSpec as P

OVL = 128
HALF = 64
LANES = 128

EPSILON = 0.01
PHOTON_SCALE = 0.01
STEP_SIZE = 0.5
REGULAR = 1.0

F32 = jnp.float32
BF16 = jnp.bfloat16


def call(kernel, out_shapes, args, smem=(), hbm_out=False, scratch=(), flops=0, limit=16):
    specs = [
        pl.BlockSpec(memory_space=pltpu.SMEM if i in smem else pltpu.VMEM) for i in range(len(args))
    ]
    args = [
        x if i in smem else pltpu.with_memory_space_constraint(x, pltpu.VMEM)
        for i, x in enumerate(args)
    ]
    return pl.pallas_call(
        kernel,
        out_shape=[
            jax.ShapeDtypeStruct(s, F32) if hbm_out else pltpu.VMEM(s, F32) for s in out_shapes
        ],
        in_specs=specs,
        out_specs=[pl.BlockSpec(memory_space=pltpu.VMEM) for _ in out_shapes],
        scratch_shapes=list(scratch),
        compiler_params=pltpu.CompilerParams(vmem_limit_bytes=limit * 1024 * 1024),
        cost_estimate=pl.CostEstimate(flops=flops, bytes_accessed=0, transcendentals=0)
        if flops
        else None,
    )(*args)


@functools.lru_cache(maxsize=None)
def tables(length):
    quarter = length // 4
    n = np.arange(quarter)[:, None]
    k = np.arange(quarter)[None, :]
    blocks = []
    for p in range(4):
        angle = 2.0 * np.pi * ((n * (4 * k + p)) % length) / length
        c = np.cos(angle) / math.sqrt(length)
        s = np.sin(angle) / math.sqrt(length)
        blocks.append(np.block([[c, -s], [s, c]]))
    blocks += [b.T for b in blocks]
    full = np.stack(blocks)
    high = full.astype(np.float32).astype(ml_dtypes.bfloat16)
    low = (full - high.astype(np.float64)).astype(np.float32).astype(ml_dtypes.bfloat16)
    return high, low


def split(x):
    high = x.astype(BF16)
    return high, (x - high.astype(F32)).astype(BF16)


def dot(a, b):
    return lax.dot_general(a, b, (((1,), (0,)), ((), ())), preferred_element_type=F32)


def mix_forward(x):
    (x0r, x0i), (x1r, x1i), (x2r, x2i), (x3r, x3i) = x
    ar, ai, br, bi = x0r + x2r, x0i + x2i, x0r - x2r, x0i - x2i
    cr, ci, dr, di = x1r + x3r, x1i + x3i, x1r - x3r, x1i - x3i
    return [(ar + cr, ai + ci), (br + di, bi - dr), (ar - cr, ai - ci), (br - di, bi + dr)]


def mix_inverse(x):
    (x0r, x0i), (x1r, x1i), (x2r, x2i), (x3r, x3i) = x
    ar, ai, br, bi = x0r + x2r, x0i + x2i, x0r - x2r, x0i - x2i
    cr, ci, dr, di = x1r + x3r, x1i + x3i, x1r - x3r, x1i - x3i
    return [(ar + cr, ai + ci), (br - di, bi + dr), (ar - cr, ai - ci), (br + di, bi - dr)]


def lane_iota(shape):
    return lax.broadcasted_iota(jnp.int32, shape, len(shape) - 1)


def row_iota(shape):
    return lax.broadcasted_iota(jnp.int32, shape, len(shape) - 2)


def turn(x):
    return pltpu.roll(x, HALF, len(x.shape) - 1)


def odd(axis):
    return lax.axis_index(axis) % 2 == 1


def row_kernel(offs, obj, inner, cross, held, numbers, sems):
    rows, cols = obj.shape[1:]
    far = odd("row")
    bases = jnp.where(far, 0, rows - OVL), jnp.where(far, rows - OVL, 0)
    copies = [pltpu.make_async_copy(offs, numbers, sems.at[2])]
    for t, base in enumerate(bases):
        part = obj.at[:, pl.ds(pl.multiple_of(base, 8), OVL), :]
        copies.append(pltpu.make_async_copy(part, held.at[t], sems.at[t]))
    for copy in (copies[1], copies[0], copies[2]):
        copy.start()
    copies[0].wait()
    lane = lane_iota((8, LANES))
    first, second = numbers[0, 0, 0, 0], numbers[0, 0, 0, 1]
    info = jnp.where(lane == 0, first, jnp.where(lane == 1, second, 1)).astype(F32)
    for t, out in enumerate((inner, cross)):
        out[OVL : OVL + 8, 0:128] = info
        out[OVL : OVL + 8, 128:640] = jnp.zeros((8, 512), F32)
        copies[1 + t].wait()
        for c in range(2):
            out[0:OVL, c * 256 : c * 256 + 256] = held[t, c, :, 0:256]
            out[0:OVL, 512 + c * HALF : 512 + c * HALF + HALF] = held[t, c, :, 256:cols]


def side_kernel(obj, xside, dside):
    cols = obj.shape[2]
    right = odd("col")
    for c in range(2):
        west = turn(obj[c, :, 0:128])
        east = obj[c, :, cols - OVL : cols]
        xside[c] = jnp.where(right, east, west)
        dside[c] = jnp.where(right, west, east)


def corner_kernel(offs, inner, cross, token, xside, dside):
    right = odd("col")
    far = odd("row")

    def halo(part, rows, cols):
        a, b = inner[rows, cols], cross[rows, cols]
        return jnp.where(far, a, b) if part == 0 else jnp.where(far, b, a)

    top = slice(0, OVL)
    for part in range(2):
        for c in range(2):
            rows = slice((2 * c + part) * OVL, (2 * c + part) * OVL + OVL)
            west = turn(halo(part, top, slice(c * 256, c * 256 + 128)))
            lane = lane_iota((OVL, LANES))
            tail = halo(part, top, slice(512, 640))
            if c == 0:
                tail = turn(tail)
            middle = turn(halo(part, top, slice(c * 256 + 128, c * 256 + 256)))
            east = jnp.where(lane < HALF, middle, tail)
            xside[rows, :] = jnp.where(right, east, west)
            dside[rows, :] = jnp.where(right, west, east)
    lane = lane_iota((8, LANES))
    info = jnp.where(lane == 0, offs[0], jnp.where(lane == 1, offs[1], 1)).astype(F32)
    for out in (xside, dside):
        out[4 * OVL : 4 * OVL + 8, :] = halo(0, slice(OVL, OVL + 8), slice(0, 128))
        out[4 * OVL + 8 : 4 * OVL + 16, :] = info
        out[4 * OVL + 16 : 4 * OVL + 24, :] = halo(1, slice(OVL, OVL + 8), slice(0, 128))


def ready_kernel(offs, probe, counts, rolled, measured, token, wide):
    size = probe.shape[-1]
    quarter = size // 4
    u = offs[0]
    v = offs[1]
    for c in range(2):
        for t in range(4):
            cols = slice(t * quarter, (t + 1) * quarter)
            wide[c, t, 0:HALF, :] = probe[c, size - HALF : size, cols]
            wide[c, t, HALF : HALF + size, :] = probe[c, :, cols]
        for base in range(0, size, HALF):
            rows = pl.ds(HALF - u + base, HALF)
            piece = jnp.concatenate([wide[c, t, rows, :] for t in range(4)], axis=1)
            rolled[c, base : base + HALF, :] = pltpu.roll(piece, v, 1)
    token[...] = jnp.zeros(token.shape, F32)
    r = row_iota((size, size))
    k = lane_iota((size, size))
    order = jnp.where(r == 4 * (k % quarter) + k // quarter, 1.0, 0.0).astype(BF16)
    for t in range(4):
        wide[0, t, 0:size, :] = counts[:, t * quarter : (t + 1) * quarter].astype(F32)
    for p in range(4):
        rows = jnp.concatenate([wide[0, t, pl.ds(p, quarter, stride=4), :] for t in range(4)], axis=1)
        high = jnp.floor(rows * (1.0 / 256.0))
        low = rows - 256.0 * high
        moved = 256.0 * dot(high.astype(BF16), order) + dot(low.astype(BF16), order)
        measured[p * quarter : (p + 1) * quarter, :] = jnp.sqrt(moved * PHOTON_SCALE)


def main_kernel(
    offs, obj, inner, cross, xside, dside, xcorner, dcorner, rolled, measured, high, low,
    own, nblock, sblock, xedge, dedge, xcorn, dcorn, ah, al, bh, bl, zf, tf,
):
    size = rolled.shape[-1]
    quarter = size // 4
    cells = obj.shape[1]
    u = offs[0]
    v = offs[1]
    right = odd("col")
    far = odd("row")

    def pieces(c, part, base, count):
        lane = lane_iota((count, LANES))
        if part == "own":
            tiles = [obj[c, base : base + count, 0:128], obj[c, base : base + count, 128:256]]
            last = obj[c, base : base + count, 256:cells]
            last = jnp.concatenate([last, last], axis=1)
            x = xside[c, base : base + count, :]
            d = dside[c, base : base + count, :]
        else:
            tiles = []
            for at in (c * 256, c * 256 + 128, 512):
                x = inner[base : base + count, at : at + 128]
                d = cross[base : base + count, at : at + 128]
                tiles.append(jnp.where(far, x, d) if part == "n" else jnp.where(far, d, x))
            last = turn(tiles[2]) if c == 1 else tiles[2]
            start = base + (2 * c + (part == "s")) * OVL
            x = xcorner[start : start + count, :]
            d = dcorner[start : start + count, :]
        w, e = jnp.where(right, d, x), jnp.where(right, x, d)
        return [jnp.where(lane < v, e, w), tiles[0], tiles[1], jnp.where(lane < HALF, last, e)]

    def patch(c, slot, count):
        if slot < HALF:
            row = row_iota((count, LANES)) + slot
            a = pieces(c, "n", slot, count)
            b = pieces(c, "s", slot + HALF, count)
            return [jnp.where(row < u, y, x) for x, y in zip(a, b)]
        if slot < OVL:
            return pieces(c, "n", slot, count)
        if slot < OVL + cells:
            return pieces(c, "own", slot - OVL, count)
        return pieces(c, "s", slot - OVL - cells, count)

    def keep(hi, lo, at, x):
        hi[at], lo[at] = split(x)

    step = 32
    block = 256
    re, im = slice(0, quarter), slice(quarter, 2 * quarter)

    for top in range(0, size, block):
        for base in range(top, top + block, step):
            rows = slice(base, base + step)
            pr, pi = patch(0, base, step), patch(1, base, step)
            exits = []
            for q in range(4):
                cols = slice(q * quarter, (q + 1) * quarter)
                ar, ai = rolled[0, rows, cols], rolled[1, rows, cols]
                exits.append((ar * pr[q] - ai * pi[q], ar * pi[q] + ai * pr[q]))
            for p, (yr, yi) in enumerate(mix_forward(exits)):
                keep(ah, al, (p, rows, re), yr)
                keep(ah, al, (p, rows, im), yi)
        rows = slice(top, top + block)
        for p in range(4):
            a = ah[p, rows, :]
            zf[p, rows, :] = dot(a, high[p]) + dot(al[p, rows, :], high[p]) + dot(a, low[p])

    for half in range(2):
        pair = (2 * half, 2 * half + 1)
        for t, p in enumerate(pair):
            cols = slice(t * quarter, (t + 1) * quarter)
            for r in range(0, quarter, step):
                quads = []
                for q in range(4):
                    rows = slice(q * quarter + r, q * quarter + r + step)
                    quads.append((zf[p, rows, re], zf[p, rows, im]))
                for k, (yr, yi) in enumerate(mix_forward(quads)):
                    keep(bh, bl, (half, k, slice(r, r + step), cols), yr)
                    keep(bh, bl, (half, k, slice(quarter + r, quarter + r + step), cols), yi)
        for k in range(4):
            a = bh[half, k]
            z = dot(high[4 + k], a) + dot(high[4 + k], bl[half, k]) + dot(low[4 + k], a)
            zr, zi = z[re], z[im]
            m = measured[k * quarter : (k + 1) * quarter, half * block : (half + 1) * block]
            factor = 1.0 - m * lax.rsqrt(zr * zr + zi * zi + EPSILON)
            keep(bh, bl, (half, k, re), factor * zr)
            keep(bh, bl, (half, k, im), factor * zi)
        for k in range(4):
            a = bh[half, k]
            tf[half, k] = dot(high[k], a) + dot(high[k], bl[half, k]) + dot(low[k], a)
        for t, p in enumerate(pair):
            cols = slice(t * quarter, (t + 1) * quarter)
            for r in range(0, quarter, step):
                quads = [
                    (
                        tf[half, k, r : r + step, cols],
                        tf[half, k, quarter + r : quarter + r + step, cols],
                    )
                    for k in range(4)
                ]
                for q, (yr, yi) in enumerate(mix_inverse(quads)):
                    rows = slice(q * quarter + r, q * quarter + r + step)
                    keep(ah, al, (p, rows, re), yr)
                    keep(ah, al, (p, rows, im), yi)

    for top in (0, block):
        rows = slice(top, top + block)
        for p in range(4):
            a = ah[p, rows, :]
            zf[p, rows, :] = dot(a, high[4 + p]) + dot(al[p, rows, :], high[4 + p]) + dot(a, low[4 + p])
        for base in range(top, top + block, step):
            rows = slice(base, base + step)
            quads = [(zf[p, rows, re], zf[p, rows, im]) for p in range(4)]
            grads = ([], [])
            for q, (br, bi) in enumerate(mix_inverse(quads)):
                cols = slice(q * quarter, (q + 1) * quarter)
                ar, ai = rolled[0, rows, cols], rolled[1, rows, cols]
                grads[0].append(ar * br + ai * bi)
                grads[1].append(ar * bi - ai * br)
            lane = lane_iota((step, LANES))
            for c in range(2):
                g = grads[c]
                wout = turn(jnp.where(lane >= v, g[0], 0.0))
                eout = turn(jnp.where(lane < HALF, jnp.where(lane < v, g[0], 0.0), g[3]))
                xout, dout = jnp.where(right, eout, wout), jnp.where(right, wout, eout)
                if OVL <= base < OVL + cells:
                    o = base - OVL
                    own[c, o : o + step, 0:128] = g[1]
                    own[c, o : o + step, 128:256] = g[2]
                    own[c, o : o + step, 256:cells] = g[3][:, : cells - 256]
                    xedge[c, o : o + step, :] = xout
                    dedge[c, o : o + step, :] = dout
                    continue
                row = row_iota((step, LANES)) + base
                sends = []
                if base < OVL:
                    sends.append((nblock, 0, base, row >= u if base < HALF else None))
                if base < HALF:
                    sends.append((sblock, OVL, base + HALF, row < u))
                if base >= OVL + cells:
                    sends.append((sblock, OVL, base - OVL - cells, None))
                for out, off, o, mask in sends:
                    put = (lambda x: x) if mask is None else (lambda x: jnp.where(mask, x, 0.0))
                    out[c, o : o + step, 0:128] = put(g[1])
                    out[c, o : o + step, 128:256] = put(g[2])
                    out[c, o : o + step, 256:384] = put(g[3])
                    xcorn[c, off + o : off + o + step, :] = put(xout)
                    dcorn[c, off + o : off + o + step, :] = put(dout)


def send_kernel(nblock, sblock, xcorn, dcorn, inner, cross):
    right = odd("col")
    far = odd("row")
    first = lane_iota((OVL, LANES)) < HALF
    tiles = []
    for base, block in ((0, nblock), (OVL, sblock)):
        last, part = [], []
        for c in range(2):
            x = xcorn[c, base : base + OVL, :]
            d = dcorn[c, base : base + OVL, :]
            fw, fe = jnp.where(right, d, x), jnp.where(right, x, d)
            part.append(block[c, :, 0:128] + fw)
            part.append(block[c, :, 128:256] + jnp.where(first, 0.0, fe))
            last.append(block[c, :, 256:384] + fe)
        part.append(jnp.where(first, last[0], turn(last[1])))
        tiles.append(part)
    for t, (n, s) in enumerate(zip(*tiles)):
        inner[:, t * 128 : t * 128 + 128] = jnp.where(far, n, s)
        cross[:, t * 128 : t * 128 + 128] = jnp.where(far, s, n)


def light_kernel(offs, xcorner, dcorner, inner, cross, probe, weight, pad, acc):
    size = probe.shape[-1]
    cells = weight.shape[0]
    far = odd("row")
    pad[...] = jnp.zeros(pad.shape, F32)
    for t in range(4):
        cols = slice(t * LANES, (t + 1) * LANES)
        x = probe[0, :, cols]
        y = probe[1, :, cols]
        pad[1 + t, OVL : OVL + size, :] = x * x + y * y
    acc[...] = jnp.zeros(acc.shape, F32)
    first = lane_iota((HALF, LANES)) < HALF
    right = odd("col")
    unit = row_iota((8, LANES)) == 0
    lane = lane_iota((8, LANES))
    for di in (0, -1, 1):
        for dj in (0, -1, 1):
            if di == 0 and dj == 0:
                u, v, there = offs[0], offs[1], 1.0
            else:
                at = slice(4 * OVL + 8 * (di + 1), 4 * OVL + 8 * (di + 2))
                if dj == 0:
                    a, b = inner[OVL : OVL + 8, 0:128], cross[OVL : OVL + 8, 0:128]
                    tile = jnp.where(far, a, b) if di < 0 else jnp.where(far, b, a)
                elif dj < 0:
                    tile = jnp.where(right, dcorner[at, :], xcorner[at, :])
                else:
                    tile = jnp.where(right, xcorner[at, :], dcorner[at, :])
                u, v, there = [jnp.sum(jnp.where(unit & (lane == i), tile, 0.0)) for i in range(3)]
                u, v = u.astype(jnp.int32), v.astype(jnp.int32)
            start, count, put = {
                0: (2 * OVL - u, cells, 0),
                1: (OVL - u, OVL, cells - OVL),
                -1: (size + HALF - u, OVL, 0),
            }[di]
            seen = there
            for r in range(0, count, HALF):
                rows = pl.ds(start + r, HALF)
                to = slice(put + r, put + r + HALF)
                lo, hi, shift = {0: (1, 5, 384 + v), -1: (4, 6, lax.rem(192 + v, 256)), 1: (0, 2, 128 + v)}[dj]
                x = pltpu.roll(jnp.concatenate([pad[t, rows, :] for t in range(lo, hi)], axis=1), shift, 1)
                if dj == 0:
                    x = x[:, 0:384]
                    acc[to, :] += x * seen
                    continue
                if dj == -1:
                    x = x[:, 0:128]
                    acc[to, 0:128] += x * seen
                    continue
                x = turn(x[:, 0:128]) * seen
                acc[to, 128:256] += jnp.where(first, 0.0, x)
                acc[to, 256:384] += x
    for r in range(0, cells, HALF):
        rows = slice(r, r + HALF)
        weight[rows, :] = STEP_SIZE / (acc[rows, 0:cells] + REGULAR)


def final_kernel(obj, own, weight, xedge, dedge, inner, cross, updated):
    cells = obj.shape[1]
    right = odd("col")
    far = odd("row")
    first = lane_iota((HALF, LANES)) < HALF
    for r in range(0, cells, HALF):
        rows = slice(r, r + HALF)
        for c in range(2):
            x, d = xedge[c, rows, :], dedge[c, rows, :]
            fw, fe = jnp.where(right, d, x), jnp.where(right, x, d)
            g = [
                own[c, rows, 0:128] + fw,
                own[c, rows, 128:256] + jnp.where(first, 0.0, fe),
                own[c, rows, 256:cells] + fe[:, : cells - 256],
            ]
            adds = []
            if r < OVL:
                adds.append((0, r))
            if r >= cells - OVL:
                adds.append((1, r - cells + OVL))
            for part, o in adds:
                src = slice(o, o + HALF)

                def take(cols):
                    a, b = inner[src, cols], cross[src, cols]
                    return jnp.where(far, a, b) if part == 0 else jnp.where(far, b, a)

                g[0] = g[0] + take(slice(c * 256, c * 256 + 128))
                g[1] = g[1] + take(slice(c * 256 + 128, c * 256 + 256))
                g[2] = g[2] + take(slice(512 + c * HALF, 512 + c * HALF + HALF))
            for t, x in enumerate(g):
                cols = slice(128 * t, min(128 * t + 128, cells))
                updated[c, rows, cols] = obj[c, rows, cols] - x * weight[rows, cols]


def swaps(axis):
    count = lax.axis_size(axis)
    return [
        [pair for i in range(first, count - 1, 2) for pair in ((i, i + 1), (i + 1, i))]
        for first in (1, 0)
    ]


def local(object_slab, probe_field, offsets, counts):
    cells = object_slab.shape[1]
    size = probe_field.shape[-1]
    row_cross, row_inner = swaps("row")
    col_cross, col_inner = swaps("col")
    offs = offsets.reshape(2)
    table_high, table_low = tables(size)
    high, low = jnp.asarray(table_high), jnp.asarray(table_low)

    to_inner, to_cross = pl.pallas_call(
        row_kernel,
        name="rows",
        out_shape=[pltpu.VMEM((OVL + 8, 640), F32) for _ in range(2)],
        in_specs=[pl.BlockSpec(memory_space=pltpu.HBM) for _ in range(2)],
        out_specs=[pl.BlockSpec(memory_space=pltpu.VMEM) for _ in range(2)],
        scratch_shapes=[
            pltpu.VMEM((2, 2, OVL, cells), F32),
            pltpu.SMEM((1, 1, 1, 2), jnp.int32),
            pltpu.SemaphoreType.DMA((3,)),
        ],
        compiler_params=pltpu.CompilerParams(vmem_limit_bytes=8 * 1024 * 1024),
    )(*[pltpu.with_memory_space_constraint(x, pltpu.HBM) for x in (offsets, object_slab)])
    halo_inner = lax.ppermute(to_inner, "row", row_inner)
    halo_cross = lax.ppermute(to_cross, "row", row_cross)
    xside, dside = call(
        side_kernel, [(2, cells, OVL), (2, cells, OVL)], [object_slab], flops=5_000_000_000
    )
    side_x = lax.ppermute(xside, "col", col_cross)
    side_d = lax.ppermute(dside, "col", col_inner)

    rolled, measured, token = call(
        ready_kernel,
        [(2, size, size), (size, size), (8, LANES)],
        [offs, probe_field, counts.reshape(size, size)],
        smem=(0,),
        scratch=[pltpu.VMEM((2, 4, size + HALF, LANES), F32)],
        flops=20_000_000_000,
    )
    xcorner, dcorner = call(
        corner_kernel,
        [(4 * OVL + 24, OVL), (4 * OVL + 24, OVL)],
        [offs, halo_inner, halo_cross, token],
        smem=(0,),
    )
    corner_x = lax.ppermute(xcorner, "col", col_cross)
    corner_d = lax.ppermute(dcorner, "col", col_inner)

    own, nblock, sblock, xedge, dedge, xcorn, dcorn = call(
        main_kernel,
        [
            (2, cells, cells),
            (2, OVL, 384),
            (2, OVL, 384),
            (2, cells, OVL),
            (2, cells, OVL),
            (2, 2 * OVL, OVL),
            (2, 2 * OVL, OVL),
        ],
        [
            offs,
            object_slab,
            halo_inner,
            halo_cross,
            side_x,
            side_d,
            corner_x,
            corner_d,
            rolled,
            measured,
            high,
            low,
        ],
        smem=(0,),
        scratch=[
            pltpu.VMEM((4, size, size // 2), BF16),
            pltpu.VMEM((4, size, size // 2), BF16),
            pltpu.VMEM((2, 4, size // 2, size // 2), BF16),
            pltpu.VMEM((2, 4, size // 2, size // 2), BF16),
            pltpu.VMEM((4, size, size // 2), F32),
            pltpu.VMEM((2, 4, size // 2, size // 2), F32),
        ],
        flops=5_000_000_000,
        limit=20,
    )
    fix_x = lax.ppermute(xcorn, "col", col_cross)
    fix_d = lax.ppermute(dcorn, "col", col_inner)
    to_inner, to_cross = call(send_kernel, [(OVL, 640), (OVL, 640)], [nblock, sblock, fix_x, fix_d])
    grad_inner = lax.ppermute(to_inner, "row", row_inner)
    grad_cross = lax.ppermute(to_cross, "row", row_cross)
    edge_x = lax.ppermute(xedge, "col", col_cross)
    edge_d = lax.ppermute(dedge, "col", col_inner)
    (weight,) = call(
        light_kernel,
        [(cells, cells)],
        [offs, corner_x, corner_d, halo_inner, halo_cross, probe_field],
        smem=(0,),
        scratch=[pltpu.VMEM((6, size + 2 * OVL, LANES), F32), pltpu.VMEM((cells, 384), F32)],
        flops=10_000_000_000,
    )
    (updated,) = call(
        final_kernel,
        [(2, cells, cells)],
        [object_slab, own, weight, edge_x, edge_d, grad_inner, grad_cross],
        hbm_out=True,
    )
    return updated


def solution(mesh):
    return jax.shard_map(
        local,
        mesh=mesh,
        in_specs=(
            P(None, "row", "col"),
            P(),
            P("row", "col", None, None),
            P("row", "col", None, None, None),
        ),
        out_specs=P(None, "row", "col"),
        check_vma=False,
    )
```

```python
import functools
import math

import jax
import jax.numpy as jnp
import ml_dtypes
import numpy as np
from jax import lax
from jax.experimental import pallas as pl
from jax.experimental.pallas import tpu as pltpu
from jax.sharding import PartitionSpec as P

OVL = 128
HALF = 64
LANES = 128

EPSILON = 0.01
PHOTON_SCALE = 0.01
STEP_SIZE = 0.5
REGULAR = 1.0

F32 = jnp.float32
BF16 = jnp.bfloat16


def call(kernel, out_shapes, args, smem=(), hbm_out=False, dtype=F32, scratch=(), flops=0, limit=16):
    specs = [
        pl.BlockSpec(memory_space=pltpu.SMEM if i in smem else pltpu.VMEM) for i in range(len(args))
    ]
    args = [
        x if i in smem else pltpu.with_memory_space_constraint(x, pltpu.VMEM)
        for i, x in enumerate(args)
    ]
    return pl.pallas_call(
        kernel,
        out_shape=[
            jax.ShapeDtypeStruct(s, F32) if hbm_out else pltpu.VMEM(s, dtype) for s in out_shapes
        ],
        in_specs=specs,
        out_specs=[pl.BlockSpec(memory_space=pltpu.VMEM) for _ in out_shapes],
        scratch_shapes=list(scratch),
        compiler_params=pltpu.CompilerParams(vmem_limit_bytes=limit * 1024 * 1024),
        cost_estimate=pl.CostEstimate(flops=flops, bytes_accessed=0, transcendentals=0)
        if flops
        else None,
    )(*args)


@functools.lru_cache(maxsize=None)
def tables(length):
    quarter = length // 4
    n = np.arange(quarter)[:, None]
    k = np.arange(quarter)[None, :]
    blocks = []
    for p in range(4):
        angle = 2.0 * np.pi * ((n * (4 * k + p)) % length) / length
        c = np.cos(angle) / math.sqrt(length)
        s = np.sin(angle) / math.sqrt(length)
        blocks.append(np.block([[c, -s], [s, c]]))
    blocks += [b.T for b in blocks]
    full = np.stack(blocks)
    high = full.astype(np.float32).astype(ml_dtypes.bfloat16)
    low = (full - high.astype(np.float64)).astype(np.float32).astype(ml_dtypes.bfloat16)
    return high, low


def split(x):
    high = x.astype(BF16)
    return high, (x - high.astype(F32)).astype(BF16)


def dot(a, b):
    return lax.dot_general(a, b, (((1,), (0,)), ((), ())), preferred_element_type=F32)


def mix_forward(x):
    (x0r, x0i), (x1r, x1i), (x2r, x2i), (x3r, x3i) = x
    ar, ai, br, bi = x0r + x2r, x0i + x2i, x0r - x2r, x0i - x2i
    cr, ci, dr, di = x1r + x3r, x1i + x3i, x1r - x3r, x1i - x3i
    return [(ar + cr, ai + ci), (br + di, bi - dr), (ar - cr, ai - ci), (br - di, bi + dr)]


def mix_inverse(x):
    (x0r, x0i), (x1r, x1i), (x2r, x2i), (x3r, x3i) = x
    ar, ai, br, bi = x0r + x2r, x0i + x2i, x0r - x2r, x0i - x2i
    cr, ci, dr, di = x1r + x3r, x1i + x3i, x1r - x3r, x1i - x3i
    return [(ar + cr, ai + ci), (br - di, bi + dr), (ar - cr, ai - ci), (br + di, bi - dr)]


def lane_iota(shape):
    return lax.broadcasted_iota(jnp.int32, shape, len(shape) - 1)


def row_iota(shape):
    return lax.broadcasted_iota(jnp.int32, shape, len(shape) - 2)


def turn(x):
    return pltpu.roll(x, HALF, len(x.shape) - 1)


def odd(axis):
    return lax.axis_index(axis) % 2 == 1


def row_kernel(offs, obj, inner, cross, held, numbers, sems):
    rows, cols = obj.shape[1:]
    far = odd("row")
    bases = jnp.where(far, 0, rows - OVL), jnp.where(far, rows - OVL, 0)
    copies = [pltpu.make_async_copy(offs, numbers, sems.at[2])]
    for t, base in enumerate(bases):
        part = obj.at[:, pl.ds(pl.multiple_of(base, 8), OVL), :]
        copies.append(pltpu.make_async_copy(part, held.at[t], sems.at[t]))
    for copy in (copies[1], copies[0], copies[2]):
        copy.start()
    copies[0].wait()
    lane = lane_iota((8, LANES))
    first, second = numbers[0, 0, 0, 0], numbers[0, 0, 0, 1]
    info = jnp.where(lane == 0, first, jnp.where(lane == 1, second, 1)).astype(F32)
    for t, out in enumerate((inner, cross)):
        out[5 * OVL : 5 * OVL + 8, :] = info
        copies[1 + t].wait()
        for c in range(2):
            for k in range(2):
                at = (2 * c + k) * OVL
                out[at : at + OVL, :] = held[t, c, :, 128 * k : 128 * k + 128]
            out[4 * OVL : 5 * OVL, c * HALF : c * HALF + HALF] = held[t, c, :, 256:cols]


def side_kernel(obj, xside, dside):
    cols = obj.shape[2]
    right = odd("col")
    for c in range(2):
        west = turn(obj[c, :, 0:128])
        east = obj[c, :, cols - OVL : cols]
        xside[c] = jnp.where(right, east, west)
        dside[c] = jnp.where(right, west, east)


def corner_kernel(offs, inner, cross, xside, dside):
    right = odd("col")
    lane = lane_iota((OVL, LANES))
    for part, halo in enumerate((inner, cross)):
        for c in range(2):
            west = turn(halo[2 * c * OVL : 2 * c * OVL + OVL, :])
            tail = halo[4 * OVL : 5 * OVL, :]
            middle = turn(halo[(2 * c + 1) * OVL : (2 * c + 2) * OVL, :])
            east = jnp.where(lane < HALF, middle, turn(tail) if c == 0 else tail)
            rows = slice((2 * part + c) * OVL, (2 * part + c) * OVL + OVL)
            xside[rows, :] = jnp.where(right, east, west)
            dside[rows, :] = jnp.where(right, west, east)
    lane = lane_iota((8, LANES))
    info = jnp.where(lane == 0, offs[0], jnp.where(lane == 1, offs[1], 1)).astype(F32)
    for out in (xside, dside):
        out[4 * OVL : 4 * OVL + 8, :] = inner[5 * OVL : 5 * OVL + 8, :]
        out[4 * OVL + 8 : 4 * OVL + 16, :] = cross[5 * OVL : 5 * OVL + 8, :]
        out[4 * OVL + 16 : 4 * OVL + 24, :] = info


def ready_kernel(offs, probe, counts, rolled, measured, wide):
    size = probe.shape[-1]
    quarter = size // 4
    u = offs[0]
    v = offs[1]
    for c in range(2):
        for t in range(4):
            cols = slice(t * quarter, (t + 1) * quarter)
            wide[c, t, 0:HALF, :] = probe[c, size - HALF : size, cols]
            wide[c, t, HALF : HALF + size, :] = probe[c, :, cols]
        for base in range(0, size, HALF):
            rows = pl.ds(HALF - u + base, HALF)
            piece = jnp.concatenate([wide[c, t, rows, :] for t in range(4)], axis=1)
            rolled[c, base : base + HALF, :] = pltpu.roll(piece, v, 1)
    r = row_iota((size, size))
    k = lane_iota((size, size))
    order = jnp.where(r == 4 * (k % quarter) + k // quarter, 1.0, 0.0).astype(BF16)
    for t in range(4):
        wide[0, t, 0:size, :] = counts[:, t * quarter : (t + 1) * quarter].astype(F32)
    for p in range(4):
        rows = jnp.concatenate([wide[0, t, pl.ds(p, quarter, stride=4), :] for t in range(4)], axis=1)
        high = jnp.floor(rows * (1.0 / 256.0))
        low = rows - 256.0 * high
        moved = 256.0 * dot(high.astype(BF16), order) + dot(low.astype(BF16), order)
        measured[p * quarter : (p + 1) * quarter, :] = jnp.sqrt(moved * PHOTON_SCALE)


def keep(hi, lo, at, x):
    hi[at], lo[at] = split(x)


STEP = 32


def enter(tiles, rolled, rows, hi, lo, at):
    quarter = rolled.shape[-1] // 4
    exits = []
    for q in range(4):
        cols = slice(q * quarter, (q + 1) * quarter)
        ar, ai = rolled[0, rows, cols], rolled[1, rows, cols]
        exits.append((ar * tiles[0][q] - ai * tiles[1][q], ar * tiles[1][q] + ai * tiles[0][q]))
    for p, (yr, yi) in enumerate(mix_forward(exits)):
        keep(hi, lo, (p, at, slice(0, quarter)), yr)
        keep(hi, lo, (p, at, slice(quarter, 2 * quarter)), yi)


def leave(z, at, rolled, rows, v, right):
    quarter = rolled.shape[-1] // 4
    quads = [(z[p, at, 0:quarter], z[p, at, quarter : 2 * quarter]) for p in range(4)]
    grads = ([], [])
    for q, (br, bi) in enumerate(mix_inverse(quads)):
        cols = slice(q * quarter, (q + 1) * quarter)
        ar, ai = rolled[0, rows, cols], rolled[1, rows, cols]
        grads[0].append(ar * br + ai * bi)
        grads[1].append(ar * bi - ai * br)
    lane = lane_iota((STEP, LANES))
    for g in grads:
        wout = turn(jnp.where(lane >= v, g[0], 0.0))
        eout = turn(jnp.where(lane < HALF, jnp.where(lane < v, g[0], 0.0), g[3]))
        yield g[1:], jnp.where(right, eout, wout), jnp.where(right, wout, eout)


def right_product(hi, lo, rows, p, high, low, k):
    a = hi[p, rows, :]
    return dot(a, high[k]) + dot(lo[p, rows, :], high[k]) + dot(a, low[k])


def left_product(hi, lo, at, high, low, k):
    a = hi[at]
    return dot(high[k], a) + dot(high[k], lo[at]) + dot(low[k], a)


def fore_kernel(offs, obj, xside, dside, rolled, high, low, z, hi, lo):
    cells = obj.shape[1]
    v = offs[1]
    right = odd("col")
    lane = lane_iota((STEP, LANES))
    for top in range(0, cells, cells // 2):
        for base in range(top, top + cells // 2, STEP):
            rows = slice(base, base + STEP)
            tiles = []
            for c in range(2):
                last = obj[c, rows, 256:cells]
                last = jnp.concatenate([last, last], axis=1)
                x, d = xside[c, rows, :], dside[c, rows, :]
                w, e = jnp.where(right, d, x), jnp.where(right, x, d)
                tiles.append(
                    [
                        jnp.where(lane < v, e, w),
                        obj[c, rows, 0:128],
                        obj[c, rows, 128:256],
                        jnp.where(lane < HALF, last, e),
                    ]
                )
            enter(tiles, rolled, slice(base + OVL, base + OVL + STEP), hi, lo, rows)
        rows = slice(top, top + cells // 2)
        for p in range(4):
            z[p, rows, :] = right_product(hi, lo, rows, p, high, low, p)


def main_kernel(
    offs, inner, cross, xcorner, dcorner, rolled, measured, zown, high, low,
    own_hi, own_lo, nblock, sblock, xcorn, dcorn, ah, al, bh, bl, zh, tf,
):
    size = rolled.shape[-1]
    quarter = size // 4
    cells = zown.shape[1]
    u = offs[0]
    v = offs[1]
    right = odd("col")
    far = odd("row")
    lane = lane_iota((STEP, LANES))

    def pieces(c, part, base):
        def take(first, second, at, again):
            a, b = first[at : at + STEP, :], second[again : again + STEP, :]
            return jnp.where(far, a, b) if part == 0 else jnp.where(far, b, a)

        tiles = [take(inner, cross, t * OVL + base, t * OVL + base) for t in (2 * c, 2 * c + 1, 4)]
        last = turn(tiles[2]) if c == 1 else tiles[2]
        x = take(xcorner, xcorner, c * OVL + base, (2 + c) * OVL + base)
        d = take(dcorner, dcorner, c * OVL + base, (2 + c) * OVL + base)
        w, e = jnp.where(right, d, x), jnp.where(right, x, d)
        return [jnp.where(lane < v, e, w), tiles[0], tiles[1], jnp.where(lane < HALF, last, e)]

    def patch(c, slot):
        if slot >= OVL:
            return pieces(c, 1, slot - OVL - cells)
        above = pieces(c, 0, slot)
        if slot >= HALF:
            return above
        row = row_iota((STEP, LANES)) + slot
        return [jnp.where(row < u, y, x) for x, y in zip(above, pieces(c, 1, slot + HALF))]

    block = 2 * quarter
    re, im = slice(0, quarter), slice(quarter, 2 * quarter)
    count = size - cells
    slots = [b if b < OVL else b + cells for b in range(0, count, STEP)]

    for base, slot in zip(range(0, count, STEP), slots):
        rows = slice(slot, slot + STEP)
        enter([patch(c, slot) for c in range(2)], rolled, rows, ah, al, slice(base, base + STEP))
    for p in range(4):
        zh[p] = right_product(ah, al, slice(0, count), p, high, low, p)

    def place(slot, halo, own):
        if slot < OVL:
            return halo, slice(slot, slot + STEP)
        if slot < OVL + cells:
            return own, slice(slot - OVL, slot - OVL + STEP)
        return halo, slice(slot - cells, slot - cells + STEP)

    for half in range(2):
        pair = (2 * half, 2 * half + 1)
        for t, p in enumerate(pair):
            cols = slice(t * quarter, (t + 1) * quarter)
            for r in range(0, quarter, STEP):
                quads = []
                for q in range(4):
                    z, rows = place(q * quarter + r, zh, zown)
                    quads.append((z[p, rows, re], z[p, rows, im]))
                for k, (yr, yi) in enumerate(mix_forward(quads)):
                    keep(bh, bl, (half, k, slice(r, r + STEP), cols), yr)
                    keep(bh, bl, (half, k, slice(quarter + r, quarter + r + STEP), cols), yi)
        for k in range(4):
            z = left_product(bh, bl, (half, k), high, low, 4 + k)
            zr, zi = z[re], z[im]
            m = measured[k * quarter : (k + 1) * quarter, half * block : (half + 1) * block]
            factor = 1.0 - m * lax.rsqrt(zr * zr + zi * zi + EPSILON)
            keep(bh, bl, (half, k, re), factor * zr)
            keep(bh, bl, (half, k, im), factor * zi)
        for k in range(4):
            tf[half, k] = left_product(bh, bl, (half, k), high, low, k)
        for t, p in enumerate(pair):
            cols = slice(t * quarter, (t + 1) * quarter)
            for r in range(0, quarter, STEP):
                again = slice(quarter + r, quarter + r + STEP)
                quads = [(tf[half, k, r : r + STEP, cols], tf[half, k, again, cols]) for k in range(4)]
                for q, (yr, yi) in enumerate(mix_inverse(quads)):
                    hi, rows = place(q * quarter + r, ah, own_hi)
                    lo, rows = place(q * quarter + r, al, own_lo)
                    keep(hi, lo, (p, rows, re), yr)
                    keep(hi, lo, (p, rows, im), yi)

    for p in range(4):
        zh[p] = right_product(ah, al, slice(0, count), p, high, low, 4 + p)
    for base, slot in zip(range(0, count, STEP), slots):
        at, rows = slice(base, base + STEP), slice(slot, slot + STEP)
        row = row_iota((STEP, LANES)) + slot
        sends = []
        if slot < OVL:
            sends.append((0, slot, row >= u if slot < HALF else None))
        if slot < HALF:
            sends.append((1, slot + HALF, row < u))
        if slot >= OVL:
            sends.append((1, slot - OVL - cells, None))
        for c, (g, xout, dout) in enumerate(leave(zh, at, rolled, rows, v, right)):
            for part, o, mask in sends:
                to = slice(o, o + STEP)
                put = (lambda x: x) if mask is None else (lambda x: jnp.where(mask, x, 0.0))
                block = (nblock, sblock)[part]
                for t in range(3):
                    block[c, to, 128 * t : 128 * t + 128] = put(g[t])
                xcorn[part, c, to, :] = put(xout)
                dcorn[part, c, to, :] = put(dout)


def after_kernel(offs, hi, lo, rolled, high, low, own, xedge, dedge, z):
    cells = own.shape[1]
    v = offs[1]
    right = odd("col")
    for top in range(0, cells, cells // 2):
        rows = slice(top, top + cells // 2)
        for p in range(4):
            z[p, rows, :] = right_product(hi, lo, rows, p, high, low, 4 + p)
        for base in range(top, top + cells // 2, STEP):
            at, rows = slice(base, base + STEP), slice(base + OVL, base + OVL + STEP)
            for c, (g, xout, dout) in enumerate(leave(z, at, rolled, rows, v, right)):
                own[c, at, 0:128] = g[0]
                own[c, at, 128:256] = g[1]
                own[c, at, 256:cells] = g[2][:, : cells - 256]
                xedge[c, at, :] = xout
                dedge[c, at, :] = dout


def send_kernel(nblock, sblock, xcorn, dcorn, inner, cross):
    right = odd("col")
    far = odd("row")
    first = lane_iota((OVL, LANES)) < HALF
    tiles = []
    for part, block in enumerate((nblock, sblock)):
        last, out = [], []
        for c in range(2):
            x, d = xcorn[part, c], dcorn[part, c]
            fw, fe = jnp.where(right, d, x), jnp.where(right, x, d)
            out.append(block[c, :, 0:128] + fw)
            out.append(block[c, :, 128:256] + jnp.where(first, 0.0, fe))
            last.append(block[c, :, 256:384] + fe)
        out.append(jnp.where(first, last[0], turn(last[1])))
        tiles.append(out)
    for t, (n, s) in enumerate(zip(*tiles)):
        inner[t * OVL : t * OVL + OVL, :] = jnp.where(far, n, s)
        cross[t * OVL : t * OVL + OVL, :] = jnp.where(far, s, n)


def light_kernel(
    offs, xcorner, dcorner, inner, cross, probe, weight, pad, acc
):
    size = probe.shape[-1]
    cells = weight.shape[0]
    far = odd("row")
    pad[...] = jnp.zeros(pad.shape, F32)
    for t in range(4):
        cols = slice(t * LANES, (t + 1) * LANES)
        x = probe[0, :, cols]
        y = probe[1, :, cols]
        pad[1 + t, OVL : OVL + size, :] = x * x + y * y
    acc[...] = jnp.zeros(acc.shape, F32)
    first = lane_iota((HALF, LANES)) < HALF
    right = odd("col")
    unit = row_iota((8, LANES)) == 0
    lane = lane_iota((8, LANES))
    for di in (0, -1, 1):
        for dj in (0, -1, 1):
            if di == 0 and dj == 0:
                u, v, there = offs[0], offs[1], 1.0
            else:

                def take(first, second, at, again):
                    a, b = first[at : at + 8, :], second[again : again + 8, :]
                    return jnp.where(far, a, b) if di < 0 else jnp.where(far, b, a)

                if dj == 0:
                    tile = take(inner, cross, 5 * OVL, 5 * OVL)
                else:
                    if di == 0:
                        x, d = [ref[4 * OVL + 16 : 4 * OVL + 24, :] for ref in (xcorner, dcorner)]
                    else:
                        x, d = [take(ref, ref, 4 * OVL, 4 * OVL + 8) for ref in (xcorner, dcorner)]
                    tile = jnp.where(right, d, x) if dj < 0 else jnp.where(right, x, d)
                u, v, there = [jnp.sum(jnp.where(unit & (lane == i), tile, 0.0)) for i in range(3)]
                u, v = u.astype(jnp.int32), v.astype(jnp.int32)
            start, count, put = {
                0: (2 * OVL - u, cells, 0),
                1: (OVL - u, OVL, cells - OVL),
                -1: (size + HALF - u, OVL, 0),
            }[di]
            seen = there
            for r in range(0, count, HALF):
                rows = pl.ds(start + r, HALF)
                to = slice(put + r, put + r + HALF)
                lo, hi, shift = {0: (1, 5, 384 + v), -1: (4, 6, lax.rem(192 + v, 256)), 1: (0, 2, 128 + v)}[dj]
                x = pltpu.roll(jnp.concatenate([pad[t, rows, :] for t in range(lo, hi)], axis=1), shift, 1)
                if dj == 0:
                    x = x[:, 0:384]
                    acc[to, :] += x * seen
                    continue
                if dj == -1:
                    x = x[:, 0:128]
                    acc[to, 0:128] += x * seen
                    continue
                x = turn(x[:, 0:128]) * seen
                acc[to, 128:256] += jnp.where(first, 0.0, x)
                acc[to, 256:384] += x
    for r in range(0, cells, HALF):
        rows = slice(r, r + HALF)
        weight[rows, :] = STEP_SIZE / (acc[rows, 0:cells] + REGULAR)


def final_kernel(obj, own, weight, xedge, dedge, inner, cross, updated):
    cells = obj.shape[1]
    right = odd("col")
    far = odd("row")
    first = lane_iota((HALF, LANES)) < HALF
    for r in range(0, cells, HALF):
        rows = slice(r, r + HALF)
        for c in range(2):
            x, d = xedge[c, rows, :], dedge[c, rows, :]
            fw, fe = jnp.where(right, d, x), jnp.where(right, x, d)
            g = [
                own[c, rows, 0:128] + fw,
                own[c, rows, 128:256] + jnp.where(first, 0.0, fe),
                own[c, rows, 256:cells] + fe[:, : cells - 256],
            ]
            adds = []
            if r < OVL:
                adds.append((0, r))
            if r >= cells - OVL:
                adds.append((1, r - cells + OVL))
            for part, o in adds:

                def take(tile, cols=slice(0, LANES)):
                    src = slice(tile * OVL + o, tile * OVL + o + HALF)
                    a, b = inner[src, cols], cross[src, cols]
                    return jnp.where(far, a, b) if part == 0 else jnp.where(far, b, a)

                g[0] = g[0] + take(2 * c)
                g[1] = g[1] + take(2 * c + 1)
                g[2] = g[2] + take(4, slice(c * HALF, c * HALF + HALF))
            for t, x in enumerate(g):
                cols = slice(128 * t, min(128 * t + 128, cells))
                updated[c, rows, cols] = obj[c, rows, cols] - x * weight[rows, cols]


def swaps(axis):
    count = lax.axis_size(axis)
    return [
        [pair for i in range(first, count - 1, 2) for pair in ((i, i + 1), (i + 1, i))]
        for first in (1, 0)
    ]


def local(object_slab, probe_field, offsets, counts):
    cells = object_slab.shape[1]
    size = probe_field.shape[-1]
    row_cross, row_inner = swaps("row")
    col_cross, col_inner = swaps("col")
    offs = offsets.reshape(2)
    table_high, table_low = tables(size)
    high, low = jnp.asarray(table_high), jnp.asarray(table_low)

    to_inner, to_cross = pl.pallas_call(
        row_kernel,
        name="rows",
        out_shape=[pltpu.VMEM((5 * OVL + 8, LANES), F32) for _ in range(2)],
        in_specs=[pl.BlockSpec(memory_space=pltpu.HBM) for _ in range(2)],
        out_specs=[pl.BlockSpec(memory_space=pltpu.VMEM) for _ in range(2)],
        scratch_shapes=[
            pltpu.VMEM((2, 2, OVL, cells), F32),
            pltpu.SMEM((1, 1, 1, 2), jnp.int32),
            pltpu.SemaphoreType.DMA((3,)),
        ],
        compiler_params=pltpu.CompilerParams(vmem_limit_bytes=8 * 1024 * 1024),
    )(*[pltpu.with_memory_space_constraint(x, pltpu.HBM) for x in (offsets, object_slab)])
    halo_inner = lax.ppermute(to_inner, "row", row_inner)
    halo_cross = lax.ppermute(to_cross, "row", row_cross)
    xside, dside = call(
        side_kernel, [(2, cells, OVL), (2, cells, OVL)], [object_slab], flops=5_000_000_000
    )
    side_x = lax.ppermute(xside, "col", col_cross)
    side_d = lax.ppermute(dside, "col", col_inner)

    rolled, measured = call(
        ready_kernel,
        [(2, size, size), (size, size)],
        [offs, probe_field, counts.reshape(size, size)],
        smem=(0,),
        scratch=[pltpu.VMEM((2, 4, size + HALF, LANES), F32)],
        flops=5_000_000_000,
    )
    half, count = size // 2, size - cells
    (zown,) = call(
        fore_kernel,
        [(4, cells, half)],
        [offs, object_slab, side_x, side_d, rolled, high, low],
        smem=(0,),
        scratch=[pltpu.VMEM((4, cells, half), BF16) for _ in range(2)],
        flops=2_000_000_000,
    )
    xcorner, dcorner = call(
        corner_kernel, [(4 * OVL + 24, OVL)] * 2, [offs, halo_inner, halo_cross], smem=(0,)
    )
    corner_x = lax.ppermute(xcorner, "col", col_cross)
    corner_d = lax.ppermute(dcorner, "col", col_inner)
    shapes = [
        ((4, cells, half), BF16),
        ((4, cells, half), BF16),
        ((2, OVL, 384), F32),
        ((2, OVL, 384), F32),
        ((2, 2, OVL, OVL), F32),
        ((2, 2, OVL, OVL), F32),
    ]
    operands = [halo_inner, halo_cross, corner_x, corner_d, rolled, measured, zown, high, low]
    own_hi, own_lo, nblock, sblock, xcorn, dcorn = pl.pallas_call(
        main_kernel,
        name="main",
        out_shape=[pltpu.VMEM(s, d) for s, d in shapes],
        in_specs=[pl.BlockSpec(memory_space=pltpu.SMEM)]
        + [pl.BlockSpec(memory_space=pltpu.VMEM) for _ in operands],
        out_specs=[pl.BlockSpec(memory_space=pltpu.VMEM) for _ in shapes],
        scratch_shapes=[
            pltpu.VMEM((4, count, half), BF16),
            pltpu.VMEM((4, count, half), BF16),
            pltpu.VMEM((2, 4, half, half), BF16),
            pltpu.VMEM((2, 4, half, half), BF16),
            pltpu.VMEM((4, count, half), F32),
            pltpu.VMEM((2, 4, half, half), F32),
        ],
        compiler_params=pltpu.CompilerParams(vmem_limit_bytes=20 * 1024 * 1024),
        cost_estimate=pl.CostEstimate(flops=5_000_000_000, bytes_accessed=0, transcendentals=0),
    )(offs, *[pltpu.with_memory_space_constraint(x, pltpu.VMEM) for x in operands])
    fix_x = lax.ppermute(xcorn, "col", col_cross)
    fix_d = lax.ppermute(dcorn, "col", col_inner)
    own, xedge, dedge = call(
        after_kernel,
        [(2, cells, cells), (2, cells, OVL), (2, cells, OVL)],
        [offs, own_hi, own_lo, rolled, high, low],
        smem=(0,),
        scratch=[pltpu.VMEM((4, cells, half), F32)],
        flops=2_000_000_000,
    )
    to_inner, to_cross = call(send_kernel, [(5 * OVL, LANES)] * 2, [nblock, sblock, fix_x, fix_d])
    grad_inner = lax.ppermute(to_inner, "row", row_inner)
    grad_cross = lax.ppermute(to_cross, "row", row_cross)
    edge_x = lax.ppermute(xedge, "col", col_cross)
    edge_d = lax.ppermute(dedge, "col", col_inner)
    (weight,) = call(
        light_kernel,
        [(cells, cells)],
        [offs, corner_x, corner_d, halo_inner, halo_cross, probe_field],
        smem=(0,),
        scratch=[pltpu.VMEM((6, size + 2 * OVL, LANES), F32), pltpu.VMEM((cells, 384), F32)],
        flops=10_000_000_000,
    )
    (updated,) = call(
        final_kernel,
        [(2, cells, cells)],
        [object_slab, own, weight, edge_x, edge_d, grad_inner, grad_cross],
        hbm_out=True,
    )
    return updated


def solution(mesh):
    return jax.shard_map(
        local,
        mesh=mesh,
        in_specs=(
            P(None, "row", "col"),
            P(),
            P("row", "col", None, None),
            P("row", "col", None, None, None),
        ),
        out_specs=P(None, "row", "col"),
        check_vma=False,
    )
```

```python
import functools
import math

import jax
import jax.numpy as jnp
import ml_dtypes
import numpy as np
from jax import lax
from jax.experimental import pallas as pl
from jax.experimental.pallas import tpu as pltpu
from jax.sharding import PartitionSpec as P

OVL = 128
HALF = 64
KEPT = 192
LANES = 128

EPSILON = 0.01
PHOTON_SCALE = 0.01
STEP_SIZE = 0.5
REGULAR = 1.0

F32 = jnp.float32
BF16 = jnp.bfloat16


def call(kernel, out_shapes, args, hbm_out=False, scratch=(), flops=0, limit=16):
    specs = [pl.BlockSpec(memory_space=pltpu.VMEM) for _ in args]
    args = [pltpu.with_memory_space_constraint(x, pltpu.VMEM) for x in args]
    return pl.pallas_call(
        kernel,
        out_shape=[
            jax.ShapeDtypeStruct(s, F32) if hbm_out else pltpu.VMEM(s, F32) for s in out_shapes
        ],
        in_specs=specs,
        out_specs=[pl.BlockSpec(memory_space=pltpu.VMEM) for _ in out_shapes],
        scratch_shapes=list(scratch),
        compiler_params=pltpu.CompilerParams(vmem_limit_bytes=limit * 1024 * 1024),
        cost_estimate=pl.CostEstimate(flops=flops, bytes_accessed=0, transcendentals=0)
        if flops
        else None,
    )(*args)


@functools.lru_cache(maxsize=None)
def tables(length):
    quarter = length // 4
    n = np.arange(quarter)[:, None]
    k = np.arange(quarter)[None, :]
    blocks = []
    for p in range(4):
        angle = 2.0 * np.pi * ((n * (4 * k + p)) % length) / length
        c = np.cos(angle) / math.sqrt(length)
        s = np.sin(angle) / math.sqrt(length)
        blocks.append(np.block([[c, -s], [s, c]]))
    blocks += [b.T for b in blocks]
    full = np.stack(blocks)
    high = full.astype(np.float32).astype(ml_dtypes.bfloat16)
    low = (full - high.astype(np.float64)).astype(np.float32).astype(ml_dtypes.bfloat16)
    return high, low


def split(x):
    high = x.astype(BF16)
    return high, (x - high.astype(F32)).astype(BF16)


def dot(a, b):
    return lax.dot_general(a, b, (((1,), (0,)), ((), ())), preferred_element_type=F32)


def mix_forward(x):
    (x0r, x0i), (x1r, x1i), (x2r, x2i), (x3r, x3i) = x
    ar, ai, br, bi = x0r + x2r, x0i + x2i, x0r - x2r, x0i - x2i
    cr, ci, dr, di = x1r + x3r, x1i + x3i, x1r - x3r, x1i - x3i
    return [(ar + cr, ai + ci), (br + di, bi - dr), (ar - cr, ai - ci), (br - di, bi + dr)]


def mix_inverse(x):
    (x0r, x0i), (x1r, x1i), (x2r, x2i), (x3r, x3i) = x
    ar, ai, br, bi = x0r + x2r, x0i + x2i, x0r - x2r, x0i - x2i
    cr, ci, dr, di = x1r + x3r, x1i + x3i, x1r - x3r, x1i - x3i
    return [(ar + cr, ai + ci), (br - di, bi + dr), (ar - cr, ai - ci), (br + di, bi - dr)]


def lane_iota(shape):
    return lax.broadcasted_iota(jnp.int32, shape, len(shape) - 1)


def row_iota(shape):
    return lax.broadcasted_iota(jnp.int32, shape, len(shape) - 2)


def turn(x):
    return pltpu.roll(x, HALF, len(x.shape) - 1)


def odd(axis):
    return lax.axis_index(axis) % 2 == 1


def paired(axis, x, first):
    place, count = lax.axis_index(axis), lax.axis_size(axis)
    if first == 0 and count % 2 == 0:
        return x
    if first == 0:
        return jnp.where(place < count - 1, x, 0.0)
    alone = place == 0 if count % 2 else (place == 0) | (place == count - 1)
    return jnp.where(alone, 0.0, x)


def offsets_tile(u, v):
    row = row_iota((8, LANES))
    return jnp.where(row == 0, u, jnp.where(row == 1, v, 1)).astype(F32)


def number(tile, i):
    picked = (lane_iota(tile.shape) == 0) & (row_iota(tile.shape) == i)
    return jnp.sum(jnp.where(picked, tile, 0.0))


def row_kernel(offs, obj, inner, cross, mine, held, numbers, sems):
    rows, cols = obj.shape[1:]
    far = odd("row")
    bases = jnp.where(far, 0, rows - OVL), jnp.where(far, rows - OVL, 0)
    copies = [pltpu.make_async_copy(offs, numbers, sems.at[2])]
    for t, base in enumerate(bases):
        part = obj.at[:, pl.ds(pl.multiple_of(base, 8), OVL), :]
        copies.append(pltpu.make_async_copy(part, held.at[t], sems.at[t]))
    for copy in (copies[1], copies[0], copies[2]):
        copy.start()
    copies[0].wait()
    info = offsets_tile(numbers[0, 0, 0, 0], numbers[0, 0, 0, 1])
    mine[...] = info
    for t, out in enumerate((inner, cross)):
        out[5 * OVL : 5 * OVL + 8, :] = paired("row", info, t)
        copies[1 + t].wait()
        for c in range(2):
            for k in range(2):
                at = (2 * c + k) * OVL
                out[at : at + OVL, :] = paired("row", held[t, c, :, 128 * k : 128 * k + 128], t)
            tail = paired("row", held[t, c, :, 256:cols], t)
            out[4 * OVL : 5 * OVL, c * HALF : c * HALF + HALF] = tail


def side_kernel(mine, obj, xside, dside):
    cells, cols = obj.shape[1:]
    right = odd("col")
    info = mine[...]
    for c in range(2):
        rows = slice(c * cells, c * cells + cells)
        west = turn(obj[c, :, 0:128])
        east = obj[c, :, cols - OVL : cols]
        xside[rows, :] = paired("col", jnp.where(right, east, west), 1)
        dside[rows, :] = paired("col", jnp.where(right, west, east), 0)
    xside[2 * cells : 2 * cells + 8, :] = paired("col", info, 1)
    dside[2 * cells : 2 * cells + 8, :] = paired("col", info, 0)


def corner_kernel(first, mine, inner, cross, side, out):
    far = odd("row")
    to_right = odd("col") if first else ~odd("col")
    cells = (side.shape[0] - 8) // 2
    border = side[2 * cells : 2 * cells + 1, :]
    lane = lane_iota((HALF, LANES))
    row = row_iota((HALF, LANES)).astype(F32)

    def end(part, c, base):
        def take(tile):
            at = slice(tile * OVL + base, tile * OVL + base + HALF)
            a, b = inner[at, :], cross[at, :]
            return jnp.where(far, a, b) if part == 0 else jnp.where(far, b, a)

        tail = take(4)
        east = jnp.where(lane < HALF, turn(take(2 * c + 1)), turn(tail) if c == 0 else tail)
        return paired("col", jnp.where(to_right, east, turn(take(2 * c))), first)

    for c in range(2):
        base = c * KEPT
        out[base : base + HALF, :] = jnp.where(row < border, end(1, c, HALF), end(0, c, 0))
        out[base + HALF : base + OVL, :] = end(0, c, HALF)
        out[base + OVL : base + KEPT, :] = end(1, c, 0)
    rows = 2 * KEPT
    out[rows : rows + 8, :] = paired("col", inner[5 * OVL : 5 * OVL + 8, :], first)
    out[rows + 8 : rows + 16, :] = paired("col", cross[5 * OVL : 5 * OVL + 8, :], first)
    out[rows + 16 : rows + 24, :] = paired("col", mine[...], first)


def ready_kernel(mine, probe, counts, rolled, measured, wide):
    size = probe.shape[-1]
    quarter = size // 4
    u, v = [number(mine[...], i).astype(jnp.int32) for i in range(2)]
    for c in range(2):
        for t in range(4):
            cols = slice(t * quarter, (t + 1) * quarter)
            wide[c, t, 0:HALF, :] = probe[c, size - HALF : size, cols]
            wide[c, t, HALF : HALF + size, :] = probe[c, :, cols]
        for base in range(0, size, HALF):
            rows = pl.ds(HALF - u + base, HALF)
            piece = jnp.concatenate([wide[c, t, rows, :] for t in range(4)], axis=1)
            rolled[c, base : base + HALF, :] = pltpu.roll(piece, v, 1)
    r = row_iota((size, size))
    k = lane_iota((size, size))
    order = jnp.where(r == 4 * (k % quarter) + k // quarter, 1.0, 0.0).astype(BF16)
    for t in range(4):
        wide[0, t, 0:size, :] = counts[:, t * quarter : (t + 1) * quarter].astype(F32)
    for p in range(4):
        rows = jnp.concatenate([wide[0, t, pl.ds(p, quarter, stride=4), :] for t in range(4)], axis=1)
        high = jnp.floor(rows * (1.0 / 256.0))
        low = rows - 256.0 * high
        moved = 256.0 * dot(high.astype(BF16), order) + dot(low.astype(BF16), order)
        measured[p * quarter : (p + 1) * quarter, :] = jnp.sqrt(moved * PHOTON_SCALE)


def keep(hi, lo, at, x):
    hi[at], lo[at] = split(x)


STEP = 32


def enter(tiles, rolled, rows, hi, lo, at):
    quarter = rolled.shape[-1] // 4
    exits = []
    for q in range(4):
        cols = slice(q * quarter, (q + 1) * quarter)
        ar, ai = rolled[0, rows, cols], rolled[1, rows, cols]
        exits.append((ar * tiles[0][q] - ai * tiles[1][q], ar * tiles[1][q] + ai * tiles[0][q]))
    for p, (yr, yi) in enumerate(mix_forward(exits)):
        keep(hi, lo, (p, at, slice(0, quarter)), yr)
        keep(hi, lo, (p, at, slice(quarter, 2 * quarter)), yi)


def leave(z, at, rolled, rows, v, right):
    quarter = rolled.shape[-1] // 4
    quads = [(z[p, at, 0:quarter], z[p, at, quarter : 2 * quarter]) for p in range(4)]
    grads = ([], [])
    for q, (br, bi) in enumerate(mix_inverse(quads)):
        cols = slice(q * quarter, (q + 1) * quarter)
        ar, ai = rolled[0, rows, cols], rolled[1, rows, cols]
        grads[0].append(ar * br + ai * bi)
        grads[1].append(ar * bi - ai * br)
    lane = lane_iota((STEP, LANES))
    early = lane.astype(F32) < v
    for g in grads:
        wout = turn(jnp.where(early, 0.0, g[0]))
        eout = turn(jnp.where(lane < HALF, jnp.where(early, g[0], 0.0), g[3]))
        xout = paired("col", jnp.where(right, eout, wout), 1)
        yield g[1:], xout, paired("col", jnp.where(right, wout, eout), 0)


def right_product(hi, lo, rows, p, high, low, k):
    a = hi[p, rows, :]
    return dot(a, high[k]) + dot(lo[p, rows, :], high[k]) + dot(a, low[k])


def left_product(hi, lo, at, high, low, k):
    a = hi[at]
    return dot(high[k], a) + dot(high[k], lo[at]) + dot(low[k], a)


def fore_kernel(mine, obj, xside, dside, rolled, high, low, z, hi, lo):
    cells = obj.shape[1]
    v = mine[1:2, :]
    right = odd("col")
    lane = lane_iota((STEP, LANES))
    early = lane.astype(F32) < v
    for top in range(0, cells, cells // 2):
        for base in range(top, top + cells // 2, STEP):
            rows = slice(base, base + STEP)
            tiles = []
            for c in range(2):
                last = obj[c, rows, 256:cells]
                last = jnp.concatenate([last, last], axis=1)
                at = slice(c * cells + base, c * cells + base + STEP)
                x, d = xside[at, :], dside[at, :]
                w, e = jnp.where(right, d, x), jnp.where(right, x, d)
                tiles.append(
                    [
                        jnp.where(early, e, w),
                        obj[c, rows, 0:128],
                        obj[c, rows, 128:256],
                        jnp.where(lane < HALF, last, e),
                    ]
                )
            enter(tiles, rolled, slice(base + OVL, base + OVL + STEP), hi, lo, rows)
        rows = slice(top, top + cells // 2)
        for p in range(4):
            z[p, rows, :] = right_product(hi, lo, rows, p, high, low, p)


def main_kernel(
    mine, inner, cross, xcorner, dcorner, rolled, measured, zown, high, low,
    own_hi, own_lo, nblock, sblock, xcorn, dcorn, ah, al, bh, bl, zh, tf,
):
    size = rolled.shape[-1]
    quarter = size // 4
    cells = zown.shape[1]
    u = mine[0:1, :]
    v = mine[1:2, :]
    right = odd("col")
    far = odd("row")
    lane = lane_iota((STEP, LANES))
    early = lane.astype(F32) < v
    step_row = row_iota((STEP, LANES)).astype(F32)

    def patch(c, slot, base):
        def halo(part, start):
            tiles = []
            for t in (2 * c, 2 * c + 1, 4):
                at = slice(t * OVL + start, t * OVL + start + STEP)
                a, b = inner[at, :], cross[at, :]
                tiles.append(jnp.where(far, a, b) if part == 0 else jnp.where(far, b, a))
            return tiles

        if slot >= OVL:
            tiles = halo(1, slot - OVL - cells)
        else:
            tiles = halo(0, slot)
        if slot < HALF:
            row = step_row + slot
            tiles = [jnp.where(row < u, b, a) for a, b in zip(tiles, halo(1, slot + HALF))]
        last = turn(tiles[2]) if c == 1 else tiles[2]
        at = slice(c * KEPT + base, c * KEPT + base + STEP)
        x, d = xcorner[at, :], dcorner[at, :]
        w, e = jnp.where(right, d, x), jnp.where(right, x, d)
        return [jnp.where(early, e, w), tiles[0], tiles[1], jnp.where(lane < HALF, last, e)]

    block = 2 * quarter
    re, im = slice(0, quarter), slice(quarter, 2 * quarter)
    count = size - cells
    slots = [b if b < OVL else b + cells for b in range(0, count, STEP)]

    for base, slot in zip(range(0, count, STEP), slots):
        rows = slice(slot, slot + STEP)
        enter([patch(c, slot, base) for c in range(2)], rolled, rows, ah, al, slice(base, base + STEP))
    for p in range(4):
        zh[p] = right_product(ah, al, slice(0, count), p, high, low, p)

    def place(slot, halo, own):
        if slot < OVL:
            return halo, slice(slot, slot + STEP)
        if slot < OVL + cells:
            return own, slice(slot - OVL, slot - OVL + STEP)
        return halo, slice(slot - cells, slot - cells + STEP)

    for half in range(2):
        pair = (2 * half, 2 * half + 1)
        for t, p in enumerate(pair):
            cols = slice(t * quarter, (t + 1) * quarter)
            for r in range(0, quarter, STEP):
                quads = []
                for q in range(4):
                    z, rows = place(q * quarter + r, zh, zown)
                    quads.append((z[p, rows, re], z[p, rows, im]))
                for k, (yr, yi) in enumerate(mix_forward(quads)):
                    keep(bh, bl, (half, k, slice(r, r + STEP), cols), yr)
                    keep(bh, bl, (half, k, slice(quarter + r, quarter + r + STEP), cols), yi)
        for k in range(4):
            z = left_product(bh, bl, (half, k), high, low, 4 + k)
            zr, zi = z[re], z[im]
            m = measured[k * quarter : (k + 1) * quarter, half * block : (half + 1) * block]
            factor = 1.0 - m * lax.rsqrt(zr * zr + zi * zi + EPSILON)
            keep(bh, bl, (half, k, re), factor * zr)
            keep(bh, bl, (half, k, im), factor * zi)
        for k in range(4):
            tf[half, k] = left_product(bh, bl, (half, k), high, low, k)
        for t, p in enumerate(pair):
            cols = slice(t * quarter, (t + 1) * quarter)
            for r in range(0, quarter, STEP):
                again = slice(quarter + r, quarter + r + STEP)
                quads = [(tf[half, k, r : r + STEP, cols], tf[half, k, again, cols]) for k in range(4)]
                for q, (yr, yi) in enumerate(mix_inverse(quads)):
                    hi, rows = place(q * quarter + r, ah, own_hi)
                    lo, rows = place(q * quarter + r, al, own_lo)
                    keep(hi, lo, (p, rows, re), yr)
                    keep(hi, lo, (p, rows, im), yi)

    for p in range(4):
        zh[p] = right_product(ah, al, slice(0, count), p, high, low, 4 + p)
    for base, slot in zip(range(0, count, STEP), slots):
        at, rows = slice(base, base + STEP), slice(slot, slot + STEP)
        row = step_row + slot
        sends = []
        if slot < OVL:
            sends.append((0, slot, row >= u if slot < HALF else None))
        if slot < HALF:
            sends.append((1, slot + HALF, row < u))
        if slot >= OVL:
            sends.append((1, slot - OVL - cells, None))
        for c, (g, xout, dout) in enumerate(leave(zh, at, rolled, rows, v, right)):
            xcorn[c, at, :] = xout
            dcorn[c, at, :] = dout
            for part, o, mask in sends:
                to = slice(o, o + STEP)
                put = (lambda x: x) if mask is None else (lambda x: jnp.where(mask, x, 0.0))
                block = (nblock, sblock)[part]
                for t in range(3):
                    block[c, to, 128 * t : 128 * t + 128] = put(g[t])


def after_kernel(mine, hi, lo, rolled, high, low, own, xedge, dedge, z):
    cells = own.shape[1]
    v = mine[1:2, :]
    right = odd("col")
    for top in range(0, cells, cells // 2):
        rows = slice(top, top + cells // 2)
        for p in range(4):
            z[p, rows, :] = right_product(hi, lo, rows, p, high, low, 4 + p)
        for base in range(top, top + cells // 2, STEP):
            at, rows = slice(base, base + STEP), slice(base + OVL, base + OVL + STEP)
            for c, (g, xout, dout) in enumerate(leave(z, at, rolled, rows, v, right)):
                own[c, at, 0:128] = g[0]
                own[c, at, 128:256] = g[1]
                own[c, at, 256:cells] = g[2][:, : cells - 256]
                xedge[c, at, :] = xout
                dedge[c, at, :] = dout


def send_kernel(nblock, sblock, xcorn, dcorn, xcorner, dcorner, inner, cross):
    right = odd("col")
    far = odd("row")
    first = lane_iota((HALF, LANES)) < HALF
    row = row_iota((HALF, LANES)).astype(F32)
    at = 2 * KEPT + 16
    borders = [ref[at : at + 1, :] for ref in (xcorner, dcorner)]

    def corner(ref, border, c, part, base):
        if part == 1 and base == 0:
            return ref[c, OVL:KEPT, :]
        if part == 0 and base == HALF:
            return ref[c, HALF:OVL, :]
        mixed = ref[c, 0:HALF, :]
        return jnp.where((row < border) == (part == 1), mixed, 0.0)

    for base in (0, HALF):
        rows = slice(base, base + HALF)
        tiles = []
        for part, block in enumerate((nblock, sblock)):
            last, out = [], []
            for c in range(2):
                x, d = [corner(*pair, c, part, base) for pair in zip((xcorn, dcorn), borders)]
                fw, fe = jnp.where(right, d, x), jnp.where(right, x, d)
                out.append(block[c, rows, 0:128] + fw)
                out.append(block[c, rows, 128:256] + jnp.where(first, 0.0, fe))
                last.append(block[c, rows, 256:384] + fe)
            out.append(jnp.where(first, last[0], turn(last[1])))
            tiles.append(out)
        for t, (n, s) in enumerate(zip(*tiles)):
            to = slice(t * OVL + base, t * OVL + base + HALF)
            inner[to, :] = paired("row", jnp.where(far, n, s), 0)
            cross[to, :] = paired("row", jnp.where(far, s, n), 1)


def light_kernel(
    mine, xcorner, dcorner, inner, cross, probe, weight, pad, acc
):
    size = probe.shape[-1]
    cells = weight.shape[0]
    far = odd("row")
    pad[...] = jnp.zeros(pad.shape, F32)
    for t in range(4):
        cols = slice(t * LANES, (t + 1) * LANES)
        x = probe[0, :, cols]
        y = probe[1, :, cols]
        pad[1 + t, OVL : OVL + size, :] = x * x + y * y
    acc[...] = jnp.zeros(acc.shape, F32)
    first = lane_iota((HALF, LANES)) < HALF
    right = odd("col")
    for di in (0, -1, 1):
        for dj in (0, -1, 1):

            def take(first, second, at, again):
                a, b = first[at : at + 8, :], second[again : again + 8, :]
                return jnp.where(far, a, b) if di < 0 else jnp.where(far, b, a)

            if di == 0 and dj == 0:
                tile = mine[...]
            elif dj == 0:
                tile = take(inner, cross, 5 * OVL, 5 * OVL)
            else:
                if di == 0:
                    x, d = [ref[2 * KEPT + 16 : 2 * KEPT + 24, :] for ref in (xcorner, dcorner)]
                else:
                    x, d = [take(ref, ref, 2 * KEPT, 2 * KEPT + 8) for ref in (xcorner, dcorner)]
                tile = jnp.where(right, d, x) if dj < 0 else jnp.where(right, x, d)
            u, v, there = [number(tile, i) for i in range(3)]
            u, v = u.astype(jnp.int32), v.astype(jnp.int32)
            start, count, put = {
                0: (2 * OVL - u, cells, 0),
                1: (OVL - u, OVL, cells - OVL),
                -1: (size + HALF - u, OVL, 0),
            }[di]
            seen = there
            for r in range(0, count, HALF):
                rows = pl.ds(start + r, HALF)
                to = slice(put + r, put + r + HALF)
                lo, hi, shift = {0: (1, 5, 384 + v), -1: (4, 6, lax.rem(192 + v, 256)), 1: (0, 2, 128 + v)}[dj]
                x = pltpu.roll(jnp.concatenate([pad[t, rows, :] for t in range(lo, hi)], axis=1), shift, 1)
                if dj == 0:
                    x = x[:, 0:384]
                    acc[to, :] += x * seen
                    continue
                if dj == -1:
                    x = x[:, 0:128]
                    acc[to, 0:128] += x * seen
                    continue
                x = turn(x[:, 0:128]) * seen
                acc[to, 128:256] += jnp.where(first, 0.0, x)
                acc[to, 256:384] += x
    for r in range(0, cells, HALF):
        rows = slice(r, r + HALF)
        weight[rows, :] = STEP_SIZE / (acc[rows, 0:cells] + REGULAR)


def final_kernel(obj, own, weight, xedge, dedge, inner, cross, updated):
    cells = obj.shape[1]
    right = odd("col")
    far = odd("row")
    first = lane_iota((HALF, LANES)) < HALF
    for r in range(0, cells, HALF):
        rows = slice(r, r + HALF)
        for c in range(2):
            x, d = xedge[c, rows, :], dedge[c, rows, :]
            fw, fe = jnp.where(right, d, x), jnp.where(right, x, d)
            g = [
                own[c, rows, 0:128] + fw,
                own[c, rows, 128:256] + jnp.where(first, 0.0, fe),
                own[c, rows, 256:cells] + fe[:, : cells - 256],
            ]
            adds = []
            if r < OVL:
                adds.append((0, r))
            if r >= cells - OVL:
                adds.append((1, r - cells + OVL))
            for part, o in adds:

                def take(tile, cols=slice(0, LANES)):
                    src = slice(tile * OVL + o, tile * OVL + o + HALF)
                    a, b = inner[src, cols], cross[src, cols]
                    return jnp.where(far, a, b) if part == 0 else jnp.where(far, b, a)

                g[0] = g[0] + take(2 * c)
                g[1] = g[1] + take(2 * c + 1)
                g[2] = g[2] + take(4, slice(c * HALF, c * HALF + HALF))
            for t, x in enumerate(g):
                cols = slice(128 * t, min(128 * t + 128, cells))
                updated[c, rows, cols] = obj[c, rows, cols] - x * weight[rows, cols]


def swap(count, first):
    partner = list(range(count))
    for i in range(first, count - 1, 2):
        partner[i], partner[i + 1] = i + 1, i
    return partner


def routes():
    rows, cols = lax.axis_size("row"), lax.axis_size("col")
    odd_row, even_row = swap(rows, 1), swap(rows, 0)
    odd_col, even_col = swap(cols, 1), swap(cols, 0)

    def pairs(partner):
        grid = [(r, c, *partner(r, c)) for r in range(rows) for c in range(cols)]
        return [(r * cols + c, to_r * cols + to_c) for r, c, to_r, to_c in grid]

    return (
        pairs(lambda r, c: (odd_row[r], c if odd_row[r] != r else even_col[c])),
        pairs(lambda r, c: (even_row[r], c)),
        pairs(lambda r, c: (r, odd_col[c])),
        pairs(lambda r, c: (r, even_col[c])),
        pairs(lambda r, c: (r if odd_col[c] != c else even_row[r], odd_col[c])),
    )


def permute(x, pairs):
    return lax.ppermute(x, ("row", "col"), pairs)


def local(object_slab, probe_field, offsets, counts):
    cells = object_slab.shape[1]
    size = probe_field.shape[-1]
    row_cross, row_inner, col_cross, col_inner, col_full = routes()
    table_high, table_low = tables(size)
    high, low = jnp.asarray(table_high), jnp.asarray(table_low)

    to_inner, to_cross, mine = pl.pallas_call(
        row_kernel,
        name="rows",
        out_shape=[pltpu.VMEM((n, LANES), F32) for n in (5 * OVL + 8, 5 * OVL + 8, 8)],
        in_specs=[pl.BlockSpec(memory_space=pltpu.HBM) for _ in range(2)],
        out_specs=[pl.BlockSpec(memory_space=pltpu.VMEM) for _ in range(3)],
        scratch_shapes=[
            pltpu.VMEM((2, 2, OVL, cells), F32),
            pltpu.SMEM((1, 1, 1, 2), jnp.int32),
            pltpu.SemaphoreType.DMA((3,)),
        ],
        compiler_params=pltpu.CompilerParams(vmem_limit_bytes=8 * 1024 * 1024),
        cost_estimate=pl.CostEstimate(flops=5_000_000_000, bytes_accessed=0, transcendentals=0),
    )(*[pltpu.with_memory_space_constraint(x, pltpu.HBM) for x in (offsets, object_slab)])
    halo_inner = permute(to_inner, row_inner)
    halo_cross = permute(to_cross, row_cross)
    xside, dside = call(side_kernel, [(2 * cells + 8, OVL)] * 2, [mine, object_slab], flops=5_000_000_000)
    side_x = permute(xside, col_cross)
    side_d = permute(dside, col_inner)

    rolled, measured = call(
        ready_kernel,
        [(2, size, size), (size, size)],
        [mine, probe_field, counts.reshape(size, size)],
        scratch=[pltpu.VMEM((2, 4, size + HALF, LANES), F32)],
        flops=5_000_000_000,
    )
    half, count = size // 2, size - cells
    (zown,) = call(
        fore_kernel,
        [(4, cells, half)],
        [mine, object_slab, side_x, side_d, rolled, high, low],
        scratch=[pltpu.VMEM((4, cells, half), BF16) for _ in range(2)],
        flops=2_000_000_000,
    )
    ends = []
    for first, side in ((1, side_x), (0, side_d)):
        kernel = functools.partial(corner_kernel, first)
        operands = [mine, halo_inner, halo_cross, side]
        ends += call(kernel, [(2 * KEPT + 24, OVL)], operands)
    corner_x = permute(ends[0], col_full)
    corner_d = permute(ends[1], col_inner)
    shapes = [
        ((4, cells, half), BF16),
        ((4, cells, half), BF16),
        ((2, OVL, 384), F32),
        ((2, OVL, 384), F32),
        ((2, count, OVL), F32),
        ((2, count, OVL), F32),
    ]
    operands = [mine, halo_inner, halo_cross, corner_x, corner_d, rolled, measured, zown, high, low]
    own_hi, own_lo, nblock, sblock, xcorn, dcorn = pl.pallas_call(
        main_kernel,
        name="main",
        out_shape=[pltpu.VMEM(s, d) for s, d in shapes],
        in_specs=[pl.BlockSpec(memory_space=pltpu.VMEM) for _ in operands],
        out_specs=[pl.BlockSpec(memory_space=pltpu.VMEM) for _ in shapes],
        scratch_shapes=[
            pltpu.VMEM((4, count, half), BF16),
            pltpu.VMEM((4, count, half), BF16),
            pltpu.VMEM((2, 4, half, half), BF16),
            pltpu.VMEM((2, 4, half, half), BF16),
            pltpu.VMEM((4, count, half), F32),
            pltpu.VMEM((2, 4, half, half), F32),
        ],
        compiler_params=pltpu.CompilerParams(vmem_limit_bytes=20 * 1024 * 1024),
        cost_estimate=pl.CostEstimate(flops=5_000_000_000, bytes_accessed=0, transcendentals=0),
    )(*[pltpu.with_memory_space_constraint(x, pltpu.VMEM) for x in operands])
    fix_x = permute(xcorn, col_full)
    fix_d = permute(dcorn, col_inner)
    own, xedge, dedge = call(
        after_kernel,
        [(2, cells, cells), (2, cells, OVL), (2, cells, OVL)],
        [mine, own_hi, own_lo, rolled, high, low],
        scratch=[pltpu.VMEM((4, cells, half), F32)],
        flops=2_000_000_000,
    )
    to_inner, to_cross = call(send_kernel, [(5 * OVL, LANES)] * 2, [nblock, sblock, fix_x, fix_d, corner_x, corner_d])
    grad_inner = permute(to_inner, row_inner)
    grad_cross = permute(to_cross, row_cross)
    edge_x = permute(xedge, col_cross)
    edge_d = permute(dedge, col_inner)
    (weight,) = call(
        light_kernel,
        [(cells, cells)],
        [mine, corner_x, corner_d, halo_inner, halo_cross, probe_field],
        scratch=[pltpu.VMEM((6, size + 2 * OVL, LANES), F32), pltpu.VMEM((cells, 384), F32)],
        flops=10_000_000_000,
    )
    (updated,) = call(
        final_kernel,
        [(2, cells, cells)],
        [object_slab, own, weight, edge_x, edge_d, grad_inner, grad_cross],
        hbm_out=True,
    )
    return updated


def solution(mesh):
    return jax.shard_map(
        local,
        mesh=mesh,
        in_specs=(
            P(None, "row", "col"),
            P(),
            P("row", "col", None, None),
            P("row", "col", None, None, None),
        ),
        out_specs=P(None, "row", "col"),
        check_vma=False,
    )
```

```python
import functools
import math

import jax
import jax.numpy as jnp
import ml_dtypes
import numpy as np
from jax import lax
from jax.experimental import pallas as pl
from jax.experimental.pallas import tpu as pltpu
from jax.sharding import PartitionSpec as P

OVL = 128
HALF = 64
KEPT = 192
LANES = 128

EPSILON = 0.01
PHOTON_SCALE = 0.01
STEP_SIZE = 0.5
REGULAR = 1.0

F32 = jnp.float32
BF16 = jnp.bfloat16


def call(kernel, out_shapes, args, hbm_out=False, scratch=(), flops=0, limit=16):
    specs = [pl.BlockSpec(memory_space=pltpu.VMEM) for _ in args]
    args = [pltpu.with_memory_space_constraint(x, pltpu.VMEM) for x in args]
    return pl.pallas_call(
        kernel,
        out_shape=[
            jax.ShapeDtypeStruct(s, F32) if hbm_out else pltpu.VMEM(s, F32) for s in out_shapes
        ],
        in_specs=specs,
        out_specs=[
            pl.BlockSpec(memory_space=pltpu.HBM if hbm_out else pltpu.VMEM) for _ in out_shapes
        ],
        scratch_shapes=list(scratch),
        compiler_params=pltpu.CompilerParams(vmem_limit_bytes=limit * 1024 * 1024),
        cost_estimate=pl.CostEstimate(flops=flops, bytes_accessed=0, transcendentals=0)
        if flops
        else None,
    )(*args)


@functools.lru_cache(maxsize=None)
def tables(length):
    quarter = length // 4
    n = np.arange(quarter)[:, None]
    k = np.arange(quarter)[None, :]
    blocks = []
    for p in range(4):
        angle = 2.0 * np.pi * ((n * (4 * k + p)) % length) / length
        c = np.cos(angle) / math.sqrt(length)
        s = np.sin(angle) / math.sqrt(length)
        blocks.append(np.block([[c, -s], [s, c]]))
    blocks += [b.T for b in blocks]
    full = np.stack(blocks)
    high = full.astype(np.float32).astype(ml_dtypes.bfloat16)
    low = (full - high.astype(np.float64)).astype(np.float32).astype(ml_dtypes.bfloat16)
    return high, low


def split(x):
    high = x.astype(BF16)
    return high, (x - high.astype(F32)).astype(BF16)


def dot(a, b):
    return lax.dot_general(a, b, (((1,), (0,)), ((), ())), preferred_element_type=F32)


def mix_forward(x):
    (x0r, x0i), (x1r, x1i), (x2r, x2i), (x3r, x3i) = x
    ar, ai, br, bi = x0r + x2r, x0i + x2i, x0r - x2r, x0i - x2i
    cr, ci, dr, di = x1r + x3r, x1i + x3i, x1r - x3r, x1i - x3i
    return [(ar + cr, ai + ci), (br + di, bi - dr), (ar - cr, ai - ci), (br - di, bi + dr)]


def mix_inverse(x):
    (x0r, x0i), (x1r, x1i), (x2r, x2i), (x3r, x3i) = x
    ar, ai, br, bi = x0r + x2r, x0i + x2i, x0r - x2r, x0i - x2i
    cr, ci, dr, di = x1r + x3r, x1i + x3i, x1r - x3r, x1i - x3i
    return [(ar + cr, ai + ci), (br - di, bi + dr), (ar - cr, ai - ci), (br + di, bi - dr)]


def lane_iota(shape):
    return lax.broadcasted_iota(jnp.int32, shape, len(shape) - 1)


def row_iota(shape):
    return lax.broadcasted_iota(jnp.int32, shape, len(shape) - 2)


def turn(x):
    return pltpu.roll(x, HALF, len(x.shape) - 1)


def odd(axis):
    return lax.axis_index(axis) % 2 == 1


def paired(axis, x, first):
    place, count = lax.axis_index(axis), lax.axis_size(axis)
    if first == 0 and count % 2 == 0:
        return x
    if first == 0:
        return jnp.where(place < count - 1, x, 0.0)
    alone = place == 0 if count % 2 else (place == 0) | (place == count - 1)
    return jnp.where(alone, 0.0, x)


def offsets_tile(u, v):
    row = row_iota((8, LANES))
    return jnp.where(row == 0, u, jnp.where(row == 1, v, 1)).astype(F32)


def number(tile, i):
    picked = (lane_iota(tile.shape) == 0) & (row_iota(tile.shape) == i)
    return jnp.sum(jnp.where(picked, tile, 0.0))


def row_kernel(first, source, obj, *refs):
    rows, cols = obj.shape[1:]
    upward = odd("row") if first == 0 else ~odd("row")
    base = pl.multiple_of(jnp.where(upward, 0, rows - OVL), 8)
    out, *mine, held, numbers, sems = refs
    copies = [pltpu.make_async_copy(obj.at[:, pl.ds(base, OVL), :], held, sems.at[0])]
    copies[0].start()
    if first == 0:
        copies.append(pltpu.make_async_copy(source, numbers, sems.at[1]))
        copies[1].start()
        copies[1].wait()
        info = offsets_tile(numbers[0, 0, 0, 0], numbers[0, 0, 0, 1])
        mine[0][...] = info
    else:
        info = source[...]
    out[5 * OVL : 5 * OVL + 8, :] = paired("row", info, first)
    copies[0].wait()
    for c in range(2):
        for k in range(2):
            at = (2 * c + k) * OVL
            out[at : at + OVL, :] = paired("row", held[c, :, 128 * k : 128 * k + 128], first)
        tail = paired("row", held[c, :, 256:cols], first)
        out[4 * OVL : 5 * OVL, c * HALF : c * HALF + HALF] = tail


def side_kernel(mine, obj, xside, dside):
    cells, cols = obj.shape[1:]
    right = odd("col")
    info = mine[...]
    for c in range(2):
        rows = slice(c * cells, c * cells + cells)
        west = turn(obj[c, :, 0:128])
        east = obj[c, :, cols - OVL : cols]
        xside[rows, :] = paired("col", jnp.where(right, east, west), 1)
        dside[rows, :] = paired("col", jnp.where(right, west, east), 0)
    xside[2 * cells : 2 * cells + 8, :] = paired("col", info, 1)
    dside[2 * cells : 2 * cells + 8, :] = paired("col", info, 0)


def corner_kernel(first, mine, inner, cross, side, out):
    far = odd("row")
    to_right = odd("col") if first else ~odd("col")
    cells = (side.shape[0] - 8) // 2
    border = side[2 * cells : 2 * cells + 1, :]
    lane = lane_iota((HALF, LANES))
    row = row_iota((HALF, LANES)).astype(F32)

    def end(part, c, base):
        def take(tile):
            at = slice(tile * OVL + base, tile * OVL + base + HALF)
            a, b = inner[at, :], cross[at, :]
            return jnp.where(far, a, b) if part == 0 else jnp.where(far, b, a)

        tail = take(4)
        east = jnp.where(lane < HALF, turn(take(2 * c + 1)), turn(tail) if c == 0 else tail)
        return paired("col", jnp.where(to_right, east, turn(take(2 * c))), first)

    for c in range(2):
        base = c * KEPT
        out[base : base + HALF, :] = jnp.where(row < border, end(1, c, HALF), end(0, c, 0))
        out[base + HALF : base + OVL, :] = end(0, c, HALF)
        out[base + OVL : base + KEPT, :] = end(1, c, 0)
    rows = 2 * KEPT
    out[rows : rows + 8, :] = paired("col", inner[5 * OVL : 5 * OVL + 8, :], first)
    out[rows + 8 : rows + 16, :] = paired("col", cross[5 * OVL : 5 * OVL + 8, :], first)
    out[rows + 16 : rows + 24, :] = paired("col", mine[...], first)


def ready_kernel(mine, probe, counts, rolled, measured, wide):
    size = probe.shape[-1]
    quarter = size // 4
    u, v = [number(mine[...], i).astype(jnp.int32) for i in range(2)]
    for c in range(2):
        for t in range(4):
            cols = slice(t * quarter, (t + 1) * quarter)
            wide[c, t, 0:HALF, :] = probe[c, size - HALF : size, cols]
            wide[c, t, HALF : HALF + size, :] = probe[c, :, cols]
        for base in range(0, size, HALF):
            rows = pl.ds(HALF - u + base, HALF)
            piece = jnp.concatenate([wide[c, t, rows, :] for t in range(4)], axis=1)
            rolled[c, base : base + HALF, :] = pltpu.roll(piece, v, 1)
    r = row_iota((size, size))
    k = lane_iota((size, size))
    order = jnp.where(r == 4 * (k % quarter) + k // quarter, 1.0, 0.0).astype(BF16)
    for t in range(4):
        wide[0, t, 0:size, :] = counts[:, t * quarter : (t + 1) * quarter].astype(F32)
    for p in range(4):
        rows = jnp.concatenate([wide[0, t, pl.ds(p, quarter, stride=4), :] for t in range(4)], axis=1)
        high = jnp.floor(rows * (1.0 / 256.0))
        low = rows - 256.0 * high
        moved = 256.0 * dot(high.astype(BF16), order) + dot(low.astype(BF16), order)
        measured[p * quarter : (p + 1) * quarter, :] = jnp.sqrt(moved * PHOTON_SCALE)


def keep(hi, lo, at, x):
    hi[at], lo[at] = split(x)


STEP = 32


def enter(tiles, rolled, rows, hi, lo, at):
    quarter = rolled.shape[-1] // 4
    exits = []
    for q in range(4):
        cols = slice(q * quarter, (q + 1) * quarter)
        ar, ai = rolled[0, rows, cols], rolled[1, rows, cols]
        exits.append((ar * tiles[0][q] - ai * tiles[1][q], ar * tiles[1][q] + ai * tiles[0][q]))
    for p, (yr, yi) in enumerate(mix_forward(exits)):
        keep(hi, lo, (p, at, slice(0, quarter)), yr)
        keep(hi, lo, (p, at, slice(quarter, 2 * quarter)), yi)


def leave(z, at, rolled, rows, v, right):
    quarter = rolled.shape[-1] // 4
    quads = [(z[p, at, 0:quarter], z[p, at, quarter : 2 * quarter]) for p in range(4)]
    grads = ([], [])
    for q, (br, bi) in enumerate(mix_inverse(quads)):
        cols = slice(q * quarter, (q + 1) * quarter)
        ar, ai = rolled[0, rows, cols], rolled[1, rows, cols]
        grads[0].append(ar * br + ai * bi)
        grads[1].append(ar * bi - ai * br)
    lane = lane_iota((STEP, LANES))
    early = lane.astype(F32) < v
    for g in grads:
        wout = turn(jnp.where(early, 0.0, g[0]))
        eout = turn(jnp.where(lane < HALF, jnp.where(early, g[0], 0.0), g[3]))
        xout = paired("col", jnp.where(right, eout, wout), 1)
        yield g[1:], xout, paired("col", jnp.where(right, wout, eout), 0)


def right_product(hi, lo, rows, p, high, low, k):
    a = hi[p, rows, :]
    return dot(a, high[k]) + dot(lo[p, rows, :], high[k]) + dot(a, low[k])


def left_product(hi, lo, at, high, low, k):
    a = hi[at]
    return dot(high[k], a) + dot(high[k], lo[at]) + dot(low[k], a)


def fore_kernel(mine, obj, xside, dside, rolled, high, low, z, hi, lo):
    cells = obj.shape[1]
    v = mine[1:2, :]
    right = odd("col")
    lane = lane_iota((STEP, LANES))
    early = lane.astype(F32) < v
    for top in range(0, cells, cells // 2):
        for base in range(top, top + cells // 2, STEP):
            rows = slice(base, base + STEP)
            tiles = []
            for c in range(2):
                last = obj[c, rows, 256:cells]
                last = jnp.concatenate([last, last], axis=1)
                at = slice(c * cells + base, c * cells + base + STEP)
                x, d = xside[at, :], dside[at, :]
                w, e = jnp.where(right, d, x), jnp.where(right, x, d)
                tiles.append(
                    [
                        jnp.where(early, e, w),
                        obj[c, rows, 0:128],
                        obj[c, rows, 128:256],
                        jnp.where(lane < HALF, last, e),
                    ]
                )
            enter(tiles, rolled, slice(base + OVL, base + OVL + STEP), hi, lo, rows)
        rows = slice(top, top + cells // 2)
        for p in range(4):
            z[p, rows, :] = right_product(hi, lo, rows, p, high, low, p)


def main_kernel(
    mine, inner, cross, xcorner, dcorner, rolled, measured, zown, high, low,
    own_hi, own_lo, zback, xcorn, dcorn, ah, al, bh, bl, zh, tf,
):
    size = rolled.shape[-1]
    quarter = size // 4
    cells = zown.shape[1]
    u = mine[0:1, :]
    v = mine[1:2, :]
    right = odd("col")
    far = odd("row")
    lane = lane_iota((STEP, LANES))
    early = lane.astype(F32) < v
    step_row = row_iota((STEP, LANES)).astype(F32)

    def patch(c, slot, base):
        def halo(part, start):
            tiles = []
            for t in (2 * c, 2 * c + 1, 4):
                at = slice(t * OVL + start, t * OVL + start + STEP)
                a, b = inner[at, :], cross[at, :]
                tiles.append(jnp.where(far, a, b) if part == 0 else jnp.where(far, b, a))
            return tiles

        if slot >= OVL:
            tiles = halo(1, slot - OVL - cells)
        else:
            tiles = halo(0, slot)
        if slot < HALF:
            row = step_row + slot
            tiles = [jnp.where(row < u, b, a) for a, b in zip(tiles, halo(1, slot + HALF))]
        last = turn(tiles[2]) if c == 1 else tiles[2]
        at = slice(c * KEPT + base, c * KEPT + base + STEP)
        x, d = xcorner[at, :], dcorner[at, :]
        w, e = jnp.where(right, d, x), jnp.where(right, x, d)
        return [jnp.where(early, e, w), tiles[0], tiles[1], jnp.where(lane < HALF, last, e)]

    block = 2 * quarter
    re, im = slice(0, quarter), slice(quarter, 2 * quarter)
    count = size - cells
    slots = [b if b < OVL else b + cells for b in range(0, count, STEP)]

    for base, slot in zip(range(0, count, STEP), slots):
        rows = slice(slot, slot + STEP)
        enter([patch(c, slot, base) for c in range(2)], rolled, rows, ah, al, slice(base, base + STEP))
    for p in range(4):
        zh[p] = right_product(ah, al, slice(0, count), p, high, low, p)

    def place(slot, halo, own):
        if slot < OVL:
            return halo, slice(slot, slot + STEP)
        if slot < OVL + cells:
            return own, slice(slot - OVL, slot - OVL + STEP)
        return halo, slice(slot - cells, slot - cells + STEP)

    for half in range(2):
        pair = (2 * half, 2 * half + 1)
        for t, p in enumerate(pair):
            cols = slice(t * quarter, (t + 1) * quarter)
            for r in range(0, quarter, STEP):
                quads = []
                for q in range(4):
                    z, rows = place(q * quarter + r, zh, zown)
                    quads.append((z[p, rows, re], z[p, rows, im]))
                for k, (yr, yi) in enumerate(mix_forward(quads)):
                    keep(bh, bl, (half, k, slice(r, r + STEP), cols), yr)
                    keep(bh, bl, (half, k, slice(quarter + r, quarter + r + STEP), cols), yi)
    for half in range(2):
        for k in range(4):
            z = left_product(bh, bl, (half, k), high, low, 4 + k)
            zr, zi = z[re], z[im]
            m = measured[k * quarter : (k + 1) * quarter, half * block : (half + 1) * block]
            factor = 1.0 - m * lax.rsqrt(zr * zr + zi * zi + EPSILON)
            keep(bh, bl, (half, k, re), factor * zr)
            keep(bh, bl, (half, k, im), factor * zi)
    for half in range(2):
        for k in range(4):
            tf[half, k] = left_product(bh, bl, (half, k), high, low, k)
    for half in range(2):
        pair = (2 * half, 2 * half + 1)
        for t, p in enumerate(pair):
            cols = slice(t * quarter, (t + 1) * quarter)
            for r in range(0, quarter, STEP):
                again = slice(quarter + r, quarter + r + STEP)
                quads = [(tf[half, k, r : r + STEP, cols], tf[half, k, again, cols]) for k in range(4)]
                for q, (yr, yi) in enumerate(mix_inverse(quads)):
                    hi, rows = place(q * quarter + r, ah, own_hi)
                    lo, rows = place(q * quarter + r, al, own_lo)
                    keep(hi, lo, (p, rows, re), yr)
                    keep(hi, lo, (p, rows, im), yi)

    for p in range(4):
        zback[p] = right_product(ah, al, slice(0, count), p, high, low, 4 + p)
    for base, slot in zip(range(0, count, STEP), slots):
        at, rows = slice(base, base + STEP), slice(slot, slot + STEP)
        for c, (_, xout, dout) in enumerate(leave(zback, at, rolled, rows, v, right)):
            xcorn[c, at, :] = xout
            dcorn[c, at, :] = dout


def after_kernel(mine, hi, lo, zback, rolled, high, low, own, xedge, dedge, nblock, sblock, z):
    cells = own.shape[1]
    v = mine[1:2, :]
    right = odd("col")
    for top in range(0, cells, cells // 2):
        rows = slice(top, top + cells // 2)
        for p in range(4):
            z[p, rows, :] = right_product(hi, lo, rows, p, high, low, 4 + p)
        for base in range(top, top + cells // 2, STEP):
            at, rows = slice(base, base + STEP), slice(base + OVL, base + OVL + STEP)
            for c, (g, xout, dout) in enumerate(leave(z, at, rolled, rows, v, right)):
                own[c, at, 0:128] = g[0]
                own[c, at, 128:256] = g[1]
                own[c, at, 256:cells] = g[2][:, : cells - 256]
                xedge[c, at, :] = xout
                dedge[c, at, :] = dout
    u = mine[0:1, :]
    for base in range(0, zback.shape[1], STEP):
        slot = base if base < OVL else base + cells
        row = row_iota((STEP, LANES)).astype(F32) + slot
        sends = []
        if slot < OVL:
            sends.append((nblock, slot, row >= u if slot < HALF else None))
        if slot < HALF:
            sends.append((sblock, slot + HALF, row < u))
        if slot >= OVL:
            sends.append((sblock, slot - OVL - cells, None))
        at, rows = slice(base, base + STEP), slice(slot, slot + STEP)
        for c, (g, _, _) in enumerate(leave(zback, at, rolled, rows, v, right)):
            for block, o, mask in sends:
                for t, x in enumerate(g):
                    put = x if mask is None else jnp.where(mask, x, 0.0)
                    block[c, o : o + STEP, 128 * t : 128 * t + 128] = put


def send_kernel(nblock, sblock, xcorn, dcorn, xcorner, dcorner, inner, cross):
    right = odd("col")
    far = odd("row")
    first = lane_iota((HALF, LANES)) < HALF
    row = row_iota((HALF, LANES)).astype(F32)
    at = 2 * KEPT + 16
    borders = [ref[at : at + 1, :] for ref in (xcorner, dcorner)]

    def corner(ref, border, c, part, base):
        if part == 1 and base == 0:
            return ref[c, OVL:KEPT, :]
        if part == 0 and base == HALF:
            return ref[c, HALF:OVL, :]
        mixed = ref[c, 0:HALF, :]
        return jnp.where((row < border) == (part == 1), mixed, 0.0)

    for base in (0, HALF):
        rows = slice(base, base + HALF)
        tiles = []
        for part, block in enumerate((nblock, sblock)):
            last, out = [], []
            for c in range(2):
                x, d = [corner(*pair, c, part, base) for pair in zip((xcorn, dcorn), borders)]
                fw, fe = jnp.where(right, d, x), jnp.where(right, x, d)
                out.append(block[c, rows, 0:128] + fw)
                out.append(block[c, rows, 128:256] + jnp.where(first, 0.0, fe))
                last.append(block[c, rows, 256:384] + fe)
            out.append(jnp.where(first, last[0], turn(last[1])))
            tiles.append(out)
        for t, (n, s) in enumerate(zip(*tiles)):
            to = slice(t * OVL + base, t * OVL + base + HALF)
            inner[to, :] = paired("row", jnp.where(far, n, s), 0)
            cross[to, :] = paired("row", jnp.where(far, s, n), 1)


def light_kernel(
    mine, xcorner, dcorner, inner, cross, probe, weight, pad, acc
):
    size = probe.shape[-1]
    cells = weight.shape[0]
    far = odd("row")
    pad[...] = jnp.zeros(pad.shape, F32)
    for t in range(4):
        cols = slice(t * LANES, (t + 1) * LANES)
        x = probe[0, :, cols]
        y = probe[1, :, cols]
        pad[1 + t, OVL : OVL + size, :] = x * x + y * y
    acc[...] = jnp.zeros(acc.shape, F32)
    first = lane_iota((HALF, LANES)) < HALF
    right = odd("col")
    for di in (0, -1, 1):
        for dj in (0, -1, 1):

            def take(first, second, at, again):
                a, b = first[at : at + 8, :], second[again : again + 8, :]
                return jnp.where(far, a, b) if di < 0 else jnp.where(far, b, a)

            if di == 0 and dj == 0:
                tile = mine[...]
            elif dj == 0:
                tile = take(inner, cross, 5 * OVL, 5 * OVL)
            else:
                if di == 0:
                    x, d = [ref[2 * KEPT + 16 : 2 * KEPT + 24, :] for ref in (xcorner, dcorner)]
                else:
                    x, d = [take(ref, ref, 2 * KEPT, 2 * KEPT + 8) for ref in (xcorner, dcorner)]
                tile = jnp.where(right, d, x) if dj < 0 else jnp.where(right, x, d)
            u, v, there = [number(tile, i) for i in range(3)]
            u, v = u.astype(jnp.int32), v.astype(jnp.int32)
            start, count, put = {
                0: (2 * OVL - u, cells, 0),
                1: (OVL - u, OVL, cells - OVL),
                -1: (size + HALF - u, OVL, 0),
            }[di]
            seen = there
            for r in range(0, count, HALF):
                rows = pl.ds(start + r, HALF)
                to = slice(put + r, put + r + HALF)
                lo, hi, shift = {0: (1, 5, 384 + v), -1: (4, 6, lax.rem(192 + v, 256)), 1: (0, 2, 128 + v)}[dj]
                x = pltpu.roll(jnp.concatenate([pad[t, rows, :] for t in range(lo, hi)], axis=1), shift, 1)
                if dj == 0:
                    x = x[:, 0:384]
                    acc[to, :] += x * seen
                    continue
                if dj == -1:
                    x = x[:, 0:128]
                    acc[to, 0:128] += x * seen
                    continue
                x = turn(x[:, 0:128]) * seen
                acc[to, 128:256] += jnp.where(first, 0.0, x)
                acc[to, 256:384] += x
    for r in range(0, cells, HALF):
        rows = slice(r, r + HALF)
        weight[rows, :] = STEP_SIZE / (acc[rows, 0:cells] + REGULAR)


def final_kernel(obj, own, weight, xedge, dedge, inner, cross, updated, held, sems):
    cells = obj.shape[1]
    right = odd("col")
    far = odd("row")
    first = lane_iota((HALF, LANES)) < HALF
    copies = []
    for r in range(0, cells, HALF):
        rows = slice(r, r + HALF)
        for c in range(2):
            x, d = xedge[c, rows, :], dedge[c, rows, :]
            fw, fe = jnp.where(right, d, x), jnp.where(right, x, d)
            g = [
                own[c, rows, 0:128] + fw,
                own[c, rows, 128:256] + jnp.where(first, 0.0, fe),
                own[c, rows, 256:cells] + fe[:, : cells - 256],
            ]
            adds = []
            if r < OVL:
                adds.append((0, r))
            if r >= cells - OVL:
                adds.append((1, r - cells + OVL))
            for part, o in adds:

                def take(tile, cols=slice(0, LANES)):
                    src = slice(tile * OVL + o, tile * OVL + o + HALF)
                    a, b = inner[src, cols], cross[src, cols]
                    return jnp.where(far, a, b) if part == 0 else jnp.where(far, b, a)

                g[0] = g[0] + take(2 * c)
                g[1] = g[1] + take(2 * c + 1)
                g[2] = g[2] + take(4, slice(c * HALF, c * HALF + HALF))
            for t, x in enumerate(g):
                cols = slice(128 * t, min(128 * t + 128, cells))
                held[c, rows, cols] = obj[c, rows, cols] - x * weight[rows, cols]
        part = (slice(None), rows, slice(None))
        copies.append(pltpu.make_async_copy(held.at[part], updated.at[part], sems.at[r // HALF]))
        copies[-1].start()
    for copy in copies:
        copy.wait()


def swap(count, first):
    partner = list(range(count))
    for i in range(first, count - 1, 2):
        partner[i], partner[i + 1] = i + 1, i
    return partner


def routes():
    rows, cols = lax.axis_size("row"), lax.axis_size("col")
    odd_row, even_row = swap(rows, 1), swap(rows, 0)
    odd_col, even_col = swap(cols, 1), swap(cols, 0)

    def pairs(partner):
        grid = [(r, c, *partner(r, c)) for r in range(rows) for c in range(cols)]
        return [(r * cols + c, to_r * cols + to_c) for r, c, to_r, to_c in grid]

    return (
        pairs(lambda r, c: (odd_row[r], c if odd_row[r] != r else even_col[c])),
        pairs(lambda r, c: (even_row[r], c)),
        pairs(lambda r, c: (r, odd_col[c])),
        pairs(lambda r, c: (r, even_col[c])),
        pairs(lambda r, c: (r if odd_col[c] != c else even_row[r], odd_col[c])),
    )


def permute(x, pairs):
    return lax.ppermute(x, ("row", "col"), pairs)


def local(object_slab, probe_field, offsets, counts):
    cells = object_slab.shape[1]
    size = probe_field.shape[-1]
    row_cross, row_inner, col_cross, col_inner, col_full = routes()
    table_high, table_low = tables(size)
    high, low = jnp.asarray(table_high), jnp.asarray(table_low)

    def rows_for(first, source, space):
        shapes = [(5 * OVL + 8, LANES)] + [(8, LANES)] * (first == 0)
        step = pl.pallas_call(
            functools.partial(row_kernel, first),
            out_shape=[pltpu.VMEM(n, F32) for n in shapes],
            in_specs=[pl.BlockSpec(memory_space=space), pl.BlockSpec(memory_space=pltpu.HBM)],
            out_specs=[pl.BlockSpec(memory_space=pltpu.VMEM) for _ in shapes],
            scratch_shapes=[
                pltpu.VMEM((2, OVL, cells), F32),
                pltpu.SMEM((1, 1, 1, 2), jnp.int32),
                pltpu.SemaphoreType.DMA((2,)),
            ],
            compiler_params=pltpu.CompilerParams(vmem_limit_bytes=8 * 1024 * 1024),
            cost_estimate=pl.CostEstimate(flops=2_500_000_000, bytes_accessed=0, transcendentals=0),
        )
        return step(
            pltpu.with_memory_space_constraint(source, space),
            pltpu.with_memory_space_constraint(object_slab, pltpu.HBM),
        )

    to_inner, mine = rows_for(0, offsets, pltpu.HBM)
    halo_inner = permute(to_inner, row_inner)
    (to_cross,) = rows_for(1, mine, pltpu.VMEM)
    halo_cross = permute(to_cross, row_cross)
    xside, dside = call(side_kernel, [(2 * cells + 8, OVL)] * 2, [mine, object_slab], flops=5_000_000_000)
    side_x = permute(xside, col_cross)
    side_d = permute(dside, col_inner)

    rolled, measured = call(
        ready_kernel,
        [(2, size, size), (size, size)],
        [mine, probe_field, counts.reshape(size, size)],
        scratch=[pltpu.VMEM((2, 4, size + HALF, LANES), F32)],
        flops=5_000_000_000,
    )
    half, count = size // 2, size - cells
    (zown,) = call(
        fore_kernel,
        [(4, cells, half)],
        [mine, object_slab, side_x, side_d, rolled, high, low],
        scratch=[pltpu.VMEM((4, cells, half), BF16) for _ in range(2)],
        flops=2_000_000_000,
    )
    ends = []
    for first, side in ((1, side_x), (0, side_d)):
        kernel = functools.partial(corner_kernel, first)
        operands = [mine, halo_inner, halo_cross, side]
        ends += call(kernel, [(2 * KEPT + 24, OVL)], operands)
    corner_x = permute(ends[0], col_full)
    corner_d = permute(ends[1], col_inner)
    shapes = [
        ((4, cells, half), BF16),
        ((4, cells, half), BF16),
        ((4, count, half), F32),
        ((2, count, OVL), F32),
        ((2, count, OVL), F32),
    ]
    operands = [mine, halo_inner, halo_cross, corner_x, corner_d, rolled, measured, zown, high, low]
    own_hi, own_lo, zback, xcorn, dcorn = pl.pallas_call(
        main_kernel,
        name="main",
        out_shape=[pltpu.VMEM(s, d) for s, d in shapes],
        in_specs=[pl.BlockSpec(memory_space=pltpu.VMEM) for _ in operands],
        out_specs=[pl.BlockSpec(memory_space=pltpu.VMEM) for _ in shapes],
        scratch_shapes=[
            pltpu.VMEM((4, count, half), BF16),
            pltpu.VMEM((4, count, half), BF16),
            pltpu.VMEM((2, 4, half, half), BF16),
            pltpu.VMEM((2, 4, half, half), BF16),
            pltpu.VMEM((4, count, half), F32),
            pltpu.VMEM((2, 4, half, half), F32),
        ],
        compiler_params=pltpu.CompilerParams(vmem_limit_bytes=20 * 1024 * 1024),
        cost_estimate=pl.CostEstimate(flops=5_000_000_000, bytes_accessed=0, transcendentals=0),
    )(*[pltpu.with_memory_space_constraint(x, pltpu.VMEM) for x in operands])
    fix_x = permute(xcorn, col_full)
    fix_d = permute(dcorn, col_inner)
    own, xedge, dedge, nblock, sblock = call(
        after_kernel,
        [(2, cells, cells)] + [(2, cells, OVL)] * 2 + [(2, OVL, 384)] * 2,
        [mine, own_hi, own_lo, zback, rolled, high, low],
        scratch=[pltpu.VMEM((4, cells, half), F32)],
        flops=2_000_000_000,
    )
    to_inner, to_cross = call(send_kernel, [(5 * OVL, LANES)] * 2, [nblock, sblock, fix_x, fix_d, corner_x, corner_d])
    grad_inner = permute(to_inner, row_inner)
    grad_cross = permute(to_cross, row_cross)
    edge_x = permute(xedge, col_cross)
    edge_d = permute(dedge, col_inner)
    (weight,) = call(
        light_kernel,
        [(cells, cells)],
        [mine, corner_x, corner_d, halo_inner, halo_cross, probe_field],
        scratch=[pltpu.VMEM((6, size + 2 * OVL, LANES), F32), pltpu.VMEM((cells, 384), F32)],
        flops=10_000_000_000,
    )
    (updated,) = call(
        final_kernel,
        [(2, cells, cells)],
        [object_slab, own, weight, edge_x, edge_d, grad_inner, grad_cross],
        hbm_out=True,
        scratch=[
            pltpu.VMEM((2, cells, cells), F32),
            pltpu.SemaphoreType.DMA((cells // HALF,)),
        ],
    )
    return updated


def solution(mesh):
    return jax.shard_map(
        local,
        mesh=mesh,
        in_specs=(
            P(None, "row", "col"),
            P(),
            P("row", "col", None, None),
            P("row", "col", None, None, None),
        ),
        out_specs=P(None, "row", "col"),
        check_vma=False,
    )
```

```python
import functools
import math

import jax
import jax.numpy as jnp
import ml_dtypes
import numpy as np
from jax import lax
from jax.experimental import pallas as pl
from jax.experimental.pallas import tpu as pltpu
from jax.sharding import PartitionSpec as P

OVL = 128
HALF = 64
KEPT = 192
LANES = 128

EPSILON = 0.01
PHOTON_SCALE = 0.01
STEP_SIZE = 0.5
REGULAR = 1.0

F32 = jnp.float32
BF16 = jnp.bfloat16


def call(kernel, out_shapes, args, hbm_out=False, scratch=(), flops=0, limit=16):
    specs = [pl.BlockSpec(memory_space=pltpu.VMEM) for _ in args]
    args = [pltpu.with_memory_space_constraint(x, pltpu.VMEM) for x in args]
    return pl.pallas_call(
        kernel,
        out_shape=[
            jax.ShapeDtypeStruct(s, F32) if hbm_out else pltpu.VMEM(s, F32) for s in out_shapes
        ],
        in_specs=specs,
        out_specs=[
            pl.BlockSpec(memory_space=pltpu.HBM if hbm_out else pltpu.VMEM) for _ in out_shapes
        ],
        scratch_shapes=list(scratch),
        compiler_params=pltpu.CompilerParams(vmem_limit_bytes=limit * 1024 * 1024),
        cost_estimate=pl.CostEstimate(flops=flops, bytes_accessed=0, transcendentals=0)
        if flops
        else None,
    )(*args)


@functools.lru_cache(maxsize=None)
def tables(length):
    quarter = length // 4
    n = np.arange(quarter)[:, None]
    k = np.arange(quarter)[None, :]
    blocks = []
    for p in range(4):
        angle = 2.0 * np.pi * ((n * (4 * k + p)) % length) / length
        c = np.cos(angle) / math.sqrt(length)
        s = np.sin(angle) / math.sqrt(length)
        blocks.append(np.block([[c, -s], [s, c]]))
    blocks += [b.T for b in blocks]
    full = np.stack(blocks)
    high = full.astype(np.float32).astype(ml_dtypes.bfloat16)
    low = (full - high.astype(np.float64)).astype(np.float32).astype(ml_dtypes.bfloat16)
    return high, low


def split(x):
    high = x.astype(BF16)
    return high, (x - high.astype(F32)).astype(BF16)


def dot(a, b):
    return lax.dot_general(a, b, (((1,), (0,)), ((), ())), preferred_element_type=F32)


def mix_forward(x):
    (x0r, x0i), (x1r, x1i), (x2r, x2i), (x3r, x3i) = x
    ar, ai, br, bi = x0r + x2r, x0i + x2i, x0r - x2r, x0i - x2i
    cr, ci, dr, di = x1r + x3r, x1i + x3i, x1r - x3r, x1i - x3i
    return [(ar + cr, ai + ci), (br + di, bi - dr), (ar - cr, ai - ci), (br - di, bi + dr)]


def mix_inverse(x):
    (x0r, x0i), (x1r, x1i), (x2r, x2i), (x3r, x3i) = x
    ar, ai, br, bi = x0r + x2r, x0i + x2i, x0r - x2r, x0i - x2i
    cr, ci, dr, di = x1r + x3r, x1i + x3i, x1r - x3r, x1i - x3i
    return [(ar + cr, ai + ci), (br - di, bi + dr), (ar - cr, ai - ci), (br + di, bi - dr)]


def lane_iota(shape):
    return lax.broadcasted_iota(jnp.int32, shape, len(shape) - 1)


def row_iota(shape):
    return lax.broadcasted_iota(jnp.int32, shape, len(shape) - 2)


def turn(x):
    return pltpu.roll(x, HALF, len(x.shape) - 1)


def odd(axis):
    return lax.axis_index(axis) % 2 == 1


def paired(axis, x, first):
    place, count = lax.axis_index(axis), lax.axis_size(axis)
    if first == 0 and count % 2 == 0:
        return x
    if first == 0:
        return jnp.where(place < count - 1, x, 0.0)
    alone = place == 0 if count % 2 else (place == 0) | (place == count - 1)
    return jnp.where(alone, 0.0, x)


def offsets_tile(u, v):
    row = row_iota((8, LANES))
    return jnp.where(row == 0, u, jnp.where(row == 1, v, 1)).astype(F32)


def number(tile, i):
    picked = (lane_iota(tile.shape) == 0) & (row_iota(tile.shape) == i)
    return jnp.sum(jnp.where(picked, tile, 0.0))


def row_kernel(first, source, obj, *refs):
    rows, cols = obj.shape[1:]
    upward = odd("row") if first == 0 else ~odd("row")
    base = pl.multiple_of(jnp.where(upward, 0, rows - OVL), 8)
    out, middle, *mine, held, numbers, sems = refs
    copies = [pltpu.make_async_copy(obj.at[:, pl.ds(base, OVL), :], held, sems.at[0])]
    copies[0].start()
    if first == 0:
        copies.append(pltpu.make_async_copy(source, numbers, sems.at[1]))
        copies[1].start()
        copies[1].wait()
        info = offsets_tile(numbers[0, 0, 0, 0], numbers[0, 0, 0, 1])
        mine[0][...] = info
    else:
        info = source[...]
    out[4 * OVL : 4 * OVL + 8, :] = paired("row", info, first)
    copies[0].wait()
    for c in range(2):
        at = 2 * c * OVL
        out[at : at + OVL, :] = paired("row", held[c, :, 0:OVL], first)
        out[at + OVL : at + 2 * OVL, :] = paired("row", held[c, :, cols - OVL : cols], first)
        middle[:, c * HALF : c * HALF + HALF] = paired("row", held[c, :, OVL : cols - OVL], first)


def side_kernel(mine, obj, xside, dside):
    cells, cols = obj.shape[1:]
    right = odd("col")
    info = mine[...]
    for c in range(2):
        rows = slice(c * cells, c * cells + cells)
        west = turn(obj[c, :, 0:128])
        east = obj[c, :, cols - OVL : cols]
        xside[rows, :] = paired("col", jnp.where(right, east, west), 1)
        dside[rows, :] = paired("col", jnp.where(right, west, east), 0)
    xside[2 * cells : 2 * cells + 8, :] = paired("col", info, 1)
    dside[2 * cells : 2 * cells + 8, :] = paired("col", info, 0)


def corner_kernel(first, mine, inner, cross, side, out):
    far = odd("row")
    to_right = odd("col") if first else ~odd("col")
    cells = (side.shape[0] - 8) // 2
    border = side[2 * cells : 2 * cells + 1, :]
    row = row_iota((HALF, LANES)).astype(F32)

    def end(part, c, base):
        def take(tile):
            at = slice(tile * OVL + base, tile * OVL + base + HALF)
            a, b = inner[at, :], cross[at, :]
            return jnp.where(far, a, b) if part == 0 else jnp.where(far, b, a)

        return paired("col", jnp.where(to_right, take(2 * c + 1), turn(take(2 * c))), first)

    for c in range(2):
        base = c * KEPT
        out[base : base + HALF, :] = jnp.where(row < border, end(1, c, HALF), end(0, c, 0))
        out[base + HALF : base + OVL, :] = end(0, c, HALF)
        out[base + OVL : base + KEPT, :] = end(1, c, 0)
    rows = 2 * KEPT
    out[rows : rows + 8, :] = paired("col", inner[4 * OVL : 4 * OVL + 8, :], first)
    out[rows + 8 : rows + 16, :] = paired("col", cross[4 * OVL : 4 * OVL + 8, :], first)
    out[rows + 16 : rows + 24, :] = paired("col", mine[...], first)


def ready_kernel(mine, probe, counts, rolled, measured, wide):
    size = probe.shape[-1]
    quarter = size // 4
    u, v = [number(mine[...], i).astype(jnp.int32) for i in range(2)]
    for c in range(2):
        for t in range(4):
            cols = slice(t * quarter, (t + 1) * quarter)
            wide[c, t, 0:HALF, :] = probe[c, size - HALF : size, cols]
            wide[c, t, HALF : HALF + size, :] = probe[c, :, cols]
        for base in range(0, size, HALF):
            rows = pl.ds(HALF - u + base, HALF)
            piece = jnp.concatenate([wide[c, t, rows, :] for t in range(4)], axis=1)
            rolled[c, base : base + HALF, :] = pltpu.roll(piece, v, 1)
    r = row_iota((size, size))
    k = lane_iota((size, size))
    order = jnp.where(r == 4 * (k % quarter) + k // quarter, 1.0, 0.0).astype(BF16)
    for t in range(4):
        wide[0, t, 0:size, :] = counts[:, t * quarter : (t + 1) * quarter].astype(F32)
    for p in range(4):
        rows = jnp.concatenate([wide[0, t, pl.ds(p, quarter, stride=4), :] for t in range(4)], axis=1)
        high = jnp.floor(rows * (1.0 / 256.0))
        low = rows - 256.0 * high
        moved = 256.0 * dot(high.astype(BF16), order) + dot(low.astype(BF16), order)
        measured[p * quarter : (p + 1) * quarter, :] = jnp.sqrt(moved * PHOTON_SCALE)


def keep(hi, lo, at, x):
    hi[at], lo[at] = split(x)


STEP = 32


def enter(tiles, rolled, rows, hi, lo, at):
    quarter = rolled.shape[-1] // 4
    exits = []
    for q in range(4):
        cols = slice(q * quarter, (q + 1) * quarter)
        ar, ai = rolled[0, rows, cols], rolled[1, rows, cols]
        exits.append((ar * tiles[0][q] - ai * tiles[1][q], ar * tiles[1][q] + ai * tiles[0][q]))
    for p, (yr, yi) in enumerate(mix_forward(exits)):
        keep(hi, lo, (p, at, slice(0, quarter)), yr)
        keep(hi, lo, (p, at, slice(quarter, 2 * quarter)), yi)


def leave(z, at, rolled, rows, v, right):
    quarter = rolled.shape[-1] // 4
    quads = [(z[p, at, 0:quarter], z[p, at, quarter : 2 * quarter]) for p in range(4)]
    grads = ([], [])
    for q, (br, bi) in enumerate(mix_inverse(quads)):
        cols = slice(q * quarter, (q + 1) * quarter)
        ar, ai = rolled[0, rows, cols], rolled[1, rows, cols]
        grads[0].append(ar * br + ai * bi)
        grads[1].append(ar * bi - ai * br)
    lane = lane_iota((STEP, LANES))
    early = lane.astype(F32) < v
    for g in grads:
        wout = turn(jnp.where(early, 0.0, g[0]))
        eout = turn(jnp.where(lane < HALF, jnp.where(early, g[0], 0.0), g[3]))
        xout = paired("col", jnp.where(right, eout, wout), 1)
        yield g[1:], xout, paired("col", jnp.where(right, wout, eout), 0)


def right_product(hi, lo, rows, p, high, low, k):
    a = hi[p, rows, :]
    return dot(a, high[k]) + dot(lo[p, rows, :], high[k]) + dot(a, low[k])


def left_product(hi, lo, at, high, low, k):
    a = hi[at]
    return dot(high[k], a) + dot(high[k], lo[at]) + dot(low[k], a)


def fore_kernel(mine, obj, xside, dside, rolled, high, low, z, hi, lo):
    cells = obj.shape[1]
    v = mine[1:2, :]
    right = odd("col")
    lane = lane_iota((STEP, LANES))
    early = lane.astype(F32) < v
    for top in range(0, cells, cells // 2):
        for base in range(top, top + cells // 2, STEP):
            rows = slice(base, base + STEP)
            tiles = []
            for c in range(2):
                last = obj[c, rows, 256:cells]
                last = jnp.concatenate([last, last], axis=1)
                at = slice(c * cells + base, c * cells + base + STEP)
                x, d = xside[at, :], dside[at, :]
                w, e = jnp.where(right, d, x), jnp.where(right, x, d)
                tiles.append(
                    [
                        jnp.where(early, e, w),
                        obj[c, rows, 0:128],
                        obj[c, rows, 128:256],
                        jnp.where(lane < HALF, last, e),
                    ]
                )
            enter(tiles, rolled, slice(base + OVL, base + OVL + STEP), hi, lo, rows)
        rows = slice(top, top + cells // 2)
        for p in range(4):
            z[p, rows, :] = right_product(hi, lo, rows, p, high, low, p)


def main_kernel(
    mine, inner, cross, minner, mcross, xcorner, dcorner, rolled, measured, zown, high, low,
    own_hi, own_lo, zback, xcorn, dcorn, ah, al, bh, bl, zh, tf,
):
    size = rolled.shape[-1]
    quarter = size // 4
    cells = zown.shape[1]
    u = mine[0:1, :]
    v = mine[1:2, :]
    right = odd("col")
    far = odd("row")
    lane = lane_iota((STEP, LANES))
    early = lane.astype(F32) < v
    step_row = row_iota((STEP, LANES)).astype(F32)

    def patch(c, slot, base):
        def halo(part, start):
            tiles = []
            for first, second, t in ((inner, cross, 2 * c), (minner, mcross, 0), (inner, cross, 2 * c + 1)):
                at = slice(t * OVL + start, t * OVL + start + STEP)
                a, b = first[at, :], second[at, :]
                tiles.append(jnp.where(far, a, b) if part == 0 else jnp.where(far, b, a))
            return tiles

        if slot >= OVL:
            tiles = halo(1, slot - OVL - cells)
        else:
            tiles = halo(0, slot)
        if slot < HALF:
            row = step_row + slot
            tiles = [jnp.where(row < u, b, a) for a, b in zip(tiles, halo(1, slot + HALF))]
        last = turn(tiles[2])
        middle = jnp.where(lane < HALF, turn(tiles[1]) if c == 1 else tiles[1], last)
        at = slice(c * KEPT + base, c * KEPT + base + STEP)
        x, d = xcorner[at, :], dcorner[at, :]
        w, e = jnp.where(right, d, x), jnp.where(right, x, d)
        return [jnp.where(early, e, w), tiles[0], middle, jnp.where(lane < HALF, last, e)]

    block = 2 * quarter
    re, im = slice(0, quarter), slice(quarter, 2 * quarter)
    count = size - cells
    slots = [b if b < OVL else b + cells for b in range(0, count, STEP)]

    for base, slot in zip(range(0, count, STEP), slots):
        rows = slice(slot, slot + STEP)
        enter([patch(c, slot, base) for c in range(2)], rolled, rows, ah, al, slice(base, base + STEP))
    for p in range(4):
        zh[p] = right_product(ah, al, slice(0, count), p, high, low, p)

    def place(slot, halo, own):
        if slot < OVL:
            return halo, slice(slot, slot + STEP)
        if slot < OVL + cells:
            return own, slice(slot - OVL, slot - OVL + STEP)
        return halo, slice(slot - cells, slot - cells + STEP)

    for half in range(2):
        pair = (2 * half, 2 * half + 1)
        for t, p in enumerate(pair):
            cols = slice(t * quarter, (t + 1) * quarter)
            for r in range(0, quarter, STEP):
                quads = []
                for q in range(4):
                    z, rows = place(q * quarter + r, zh, zown)
                    quads.append((z[p, rows, re], z[p, rows, im]))
                for k, (yr, yi) in enumerate(mix_forward(quads)):
                    keep(bh, bl, (half, k, slice(r, r + STEP), cols), yr)
                    keep(bh, bl, (half, k, slice(quarter + r, quarter + r + STEP), cols), yi)
    for half in range(2):
        for k in range(4):
            z = left_product(bh, bl, (half, k), high, low, 4 + k)
            zr, zi = z[re], z[im]
            m = measured[k * quarter : (k + 1) * quarter, half * block : (half + 1) * block]
            factor = 1.0 - m * lax.rsqrt(zr * zr + zi * zi + EPSILON)
            keep(bh, bl, (half, k, re), factor * zr)
            keep(bh, bl, (half, k, im), factor * zi)
    for half in range(2):
        for k in range(4):
            tf[half, k] = left_product(bh, bl, (half, k), high, low, k)
    for half in range(2):
        pair = (2 * half, 2 * half + 1)
        for t, p in enumerate(pair):
            cols = slice(t * quarter, (t + 1) * quarter)
            for r in range(0, quarter, STEP):
                again = slice(quarter + r, quarter + r + STEP)
                quads = [(tf[half, k, r : r + STEP, cols], tf[half, k, again, cols]) for k in range(4)]
                for q, (yr, yi) in enumerate(mix_inverse(quads)):
                    hi, rows = place(q * quarter + r, ah, own_hi)
                    lo, rows = place(q * quarter + r, al, own_lo)
                    keep(hi, lo, (p, rows, re), yr)
                    keep(hi, lo, (p, rows, im), yi)

    for p in range(4):
        zback[p] = right_product(ah, al, slice(0, count), p, high, low, 4 + p)
    for base, slot in zip(range(0, count, STEP), slots):
        at, rows = slice(base, base + STEP), slice(slot, slot + STEP)
        for c, (_, xout, dout) in enumerate(leave(zback, at, rolled, rows, v, right)):
            xcorn[c, at, :] = xout
            dcorn[c, at, :] = dout


def after_kernel(mine, hi, lo, rolled, high, low, own, xedge, dedge, z):
    cells = own.shape[1]
    v = mine[1:2, :]
    right = odd("col")
    for top in range(0, cells, cells // 2):
        rows = slice(top, top + cells // 2)
        for p in range(4):
            z[p, rows, :] = right_product(hi, lo, rows, p, high, low, 4 + p)
        for base in range(top, top + cells // 2, STEP):
            at, rows = slice(base, base + STEP), slice(base + OVL, base + OVL + STEP)
            for c, (g, xout, dout) in enumerate(leave(z, at, rolled, rows, v, right)):
                own[c, at, 0:128] = g[0]
                own[c, at, 128:256] = g[1]
                own[c, at, 256:cells] = g[2][:, : cells - 256]
                xedge[c, at, :] = xout
                dedge[c, at, :] = dout


def block_kernel(mine, zback, rolled, nblock, sblock, minner, mcross):
    cells = rolled.shape[-1] - zback.shape[1]
    v = mine[1:2, :]
    right = odd("col")
    u = mine[0:1, :]
    for base in range(0, zback.shape[1], STEP):
        slot = base if base < OVL else base + cells
        row = row_iota((STEP, LANES)).astype(F32) + slot
        sends = []
        if slot < OVL:
            sends.append((nblock, slot, row >= u if slot < HALF else None))
        if slot < HALF:
            sends.append((sblock, slot + HALF, row < u))
        if slot >= OVL:
            sends.append((sblock, slot - OVL - cells, None))
        at, rows = slice(base, base + STEP), slice(slot, slot + STEP)
        for c, (g, _, _) in enumerate(leave(zback, at, rolled, rows, v, right)):
            for block, o, mask in sends:
                for t, x in enumerate(g):
                    put = x if mask is None else jnp.where(mask, x, 0.0)
                    block[c, o : o + STEP, 128 * t : 128 * t + 128] = put
    far = odd("row")
    first = lane_iota((OVL, LANES)) < HALF
    n, s = [jnp.where(first, b[0, :, 128:256], turn(b[1, :, 128:256])) for b in (nblock, sblock)]
    minner[...] = paired("row", jnp.where(far, n, s), 0)
    mcross[...] = paired("row", jnp.where(far, s, n), 1)


def send_kernel(nblock, sblock, xcorn, dcorn, xcorner, dcorner, inner, cross):
    right = odd("col")
    far = odd("row")
    first = lane_iota((HALF, LANES)) < HALF
    row = row_iota((HALF, LANES)).astype(F32)
    at = 2 * KEPT + 16
    borders = [ref[at : at + 1, :] for ref in (xcorner, dcorner)]

    def corner(ref, border, c, part, base):
        if part == 1 and base == 0:
            return ref[c, OVL:KEPT, :]
        if part == 0 and base == HALF:
            return ref[c, HALF:OVL, :]
        mixed = ref[c, 0:HALF, :]
        return jnp.where((row < border) == (part == 1), mixed, 0.0)

    for base in (0, HALF):
        rows = slice(base, base + HALF)
        tiles = []
        for part, block in enumerate((nblock, sblock)):
            out = []
            for c in range(2):
                x, d = [corner(*pair, c, part, base) for pair in zip((xcorn, dcorn), borders)]
                fw, fe = jnp.where(right, d, x), jnp.where(right, x, d)
                out.append(block[c, rows, 0:128] + fw)
                end = jnp.where(first, block[c, rows, 256:384], block[c, rows, 128:256])
                out.append(turn(end + fe))
            tiles.append(out)
        for t, (n, s) in enumerate(zip(*tiles)):
            to = slice(t * OVL + base, t * OVL + base + HALF)
            inner[to, :] = paired("row", jnp.where(far, n, s), 0)
            cross[to, :] = paired("row", jnp.where(far, s, n), 1)


def light_kernel(
    mine, xcorner, dcorner, inner, cross, probe, weight, pad, acc
):
    size = probe.shape[-1]
    cells = weight.shape[0]
    far = odd("row")
    pad[...] = jnp.zeros(pad.shape, F32)
    for t in range(4):
        cols = slice(t * LANES, (t + 1) * LANES)
        x = probe[0, :, cols]
        y = probe[1, :, cols]
        pad[1 + t, OVL : OVL + size, :] = x * x + y * y
    acc[...] = jnp.zeros(acc.shape, F32)
    first = lane_iota((HALF, LANES)) < HALF
    right = odd("col")
    for di in (0, -1, 1):
        for dj in (0, -1, 1):

            def take(first, second, at, again):
                a, b = first[at : at + 8, :], second[again : again + 8, :]
                return jnp.where(far, a, b) if di < 0 else jnp.where(far, b, a)

            if di == 0 and dj == 0:
                tile = mine[...]
            elif dj == 0:
                tile = take(inner, cross, 4 * OVL, 4 * OVL)
            else:
                if di == 0:
                    x, d = [ref[2 * KEPT + 16 : 2 * KEPT + 24, :] for ref in (xcorner, dcorner)]
                else:
                    x, d = [take(ref, ref, 2 * KEPT, 2 * KEPT + 8) for ref in (xcorner, dcorner)]
                tile = jnp.where(right, d, x) if dj < 0 else jnp.where(right, x, d)
            u, v, there = [number(tile, i) for i in range(3)]
            u, v = u.astype(jnp.int32), v.astype(jnp.int32)
            start, count, put = {
                0: (2 * OVL - u, cells, 0),
                1: (OVL - u, OVL, cells - OVL),
                -1: (size + HALF - u, OVL, 0),
            }[di]
            seen = there
            for r in range(0, count, HALF):
                rows = pl.ds(start + r, HALF)
                to = slice(put + r, put + r + HALF)
                lo, hi, shift = {0: (1, 5, 384 + v), -1: (4, 6, lax.rem(192 + v, 256)), 1: (0, 2, 128 + v)}[dj]
                x = pltpu.roll(jnp.concatenate([pad[t, rows, :] for t in range(lo, hi)], axis=1), shift, 1)
                if dj == 0:
                    x = x[:, 0:384]
                    acc[to, :] += x * seen
                    continue
                if dj == -1:
                    x = x[:, 0:128]
                    acc[to, 0:128] += x * seen
                    continue
                x = turn(x[:, 0:128]) * seen
                acc[to, 128:256] += jnp.where(first, 0.0, x)
                acc[to, 256:384] += x
    for r in range(0, cells, HALF):
        rows = slice(r, r + HALF)
        weight[rows, :] = STEP_SIZE / (acc[rows, 0:cells] + REGULAR)


def final_kernel(
    obj, own, weight, xedge, dedge, inner, cross, minner, mcross, updated, held, sems
):
    cells = obj.shape[1]
    right = odd("col")
    far = odd("row")
    first = lane_iota((HALF, LANES)) < HALF
    copies = []
    for r in range(0, cells, HALF):
        rows = slice(r, r + HALF)
        for c in range(2):
            x, d = xedge[c, rows, :], dedge[c, rows, :]
            fw, fe = jnp.where(right, d, x), jnp.where(right, x, d)
            g = [
                own[c, rows, 0:128] + fw,
                own[c, rows, 128:256] + jnp.where(first, 0.0, fe),
                own[c, rows, 256:cells] + fe[:, : cells - 256],
            ]
            adds = []
            if r < OVL:
                adds.append((0, r))
            if r >= cells - OVL:
                adds.append((1, r - cells + OVL))
            for part, o in adds:

                def take(first, second, tile):
                    src = slice(tile * OVL + o, tile * OVL + o + HALF)
                    a, b = first[src, :], second[src, :]
                    return jnp.where(far, a, b) if part == 0 else jnp.where(far, b, a)

                end = turn(take(inner, cross, 2 * c + 1))
                middle = take(minner, mcross, 0)
                g[0] = g[0] + take(inner, cross, 2 * c)
                g[1] = g[1] + jnp.where(first, turn(middle) if c == 1 else middle, end)
                g[2] = g[2] + end[:, : cells - 256]
            for t, x in enumerate(g):
                cols = slice(128 * t, min(128 * t + 128, cells))
                held[c, rows, cols] = obj[c, rows, cols] - x * weight[rows, cols]
        part = (slice(None), rows, slice(None))
        copies.append(pltpu.make_async_copy(held.at[part], updated.at[part], sems.at[r // HALF]))
        copies[-1].start()
    for copy in copies:
        copy.wait()


def swap(count, first):
    partner = list(range(count))
    for i in range(first, count - 1, 2):
        partner[i], partner[i + 1] = i + 1, i
    return partner


def routes():
    rows, cols = lax.axis_size("row"), lax.axis_size("col")
    odd_row, even_row = swap(rows, 1), swap(rows, 0)
    odd_col, even_col = swap(cols, 1), swap(cols, 0)

    def pairs(partner):
        grid = [(r, c, *partner(r, c)) for r in range(rows) for c in range(cols)]
        return [(r * cols + c, to_r * cols + to_c) for r, c, to_r, to_c in grid]

    return (
        pairs(lambda r, c: (odd_row[r], c if odd_row[r] != r else even_col[c])),
        pairs(lambda r, c: (even_row[r], c)),
        pairs(lambda r, c: (r, odd_col[c])),
        pairs(lambda r, c: (r, even_col[c])),
        pairs(lambda r, c: (r if odd_col[c] != c else even_row[r], odd_col[c])),
    )


def permute(x, pairs):
    return lax.ppermute(x, ("row", "col"), pairs)


def local(object_slab, probe_field, offsets, counts):
    cells = object_slab.shape[1]
    size = probe_field.shape[-1]
    row_cross, row_inner, col_cross, col_inner, col_full = routes()
    table_high, table_low = tables(size)
    high, low = jnp.asarray(table_high), jnp.asarray(table_low)

    def rows_for(first, source, space):
        shapes = [(4 * OVL + 8, LANES), (OVL, LANES)] + [(8, LANES)] * (first == 0)
        step = pl.pallas_call(
            functools.partial(row_kernel, first),
            out_shape=[pltpu.VMEM(n, F32) for n in shapes],
            in_specs=[pl.BlockSpec(memory_space=space), pl.BlockSpec(memory_space=pltpu.HBM)],
            out_specs=[pl.BlockSpec(memory_space=pltpu.VMEM) for _ in shapes],
            scratch_shapes=[
                pltpu.VMEM((2, OVL, cells), F32),
                pltpu.SMEM((1, 1, 1, 2), jnp.int32),
                pltpu.SemaphoreType.DMA((2,)),
            ],
            compiler_params=pltpu.CompilerParams(vmem_limit_bytes=8 * 1024 * 1024),
            cost_estimate=pl.CostEstimate(flops=2_500_000_000, bytes_accessed=0, transcendentals=0),
        )
        return step(
            pltpu.with_memory_space_constraint(source, space),
            pltpu.with_memory_space_constraint(object_slab, pltpu.HBM),
        )

    to_inner, middle_inner, mine = rows_for(0, offsets, pltpu.HBM)
    halo_inner = permute(to_inner, row_inner)
    to_cross, middle_cross = rows_for(1, mine, pltpu.VMEM)
    halo_cross = permute(to_cross, row_cross)
    xside, dside = call(side_kernel, [(2 * cells + 8, OVL)] * 2, [mine, object_slab], flops=5_000_000_000)
    side_x = permute(xside, col_cross)
    side_d = permute(dside, col_inner)

    rolled, measured = call(
        ready_kernel,
        [(2, size, size), (size, size)],
        [mine, probe_field, counts.reshape(size, size)],
        scratch=[pltpu.VMEM((2, 4, size + HALF, LANES), F32)],
        flops=5_000_000_000,
    )
    half, count = size // 2, size - cells
    (zown,) = call(
        fore_kernel,
        [(4, cells, half)],
        [mine, object_slab, side_x, side_d, rolled, high, low],
        scratch=[pltpu.VMEM((4, cells, half), BF16) for _ in range(2)],
        flops=2_000_000_000,
    )
    halo_mi = permute(middle_inner, row_inner)
    halo_mc = permute(middle_cross, row_cross)
    ends = []
    for first, side in ((1, side_x), (0, side_d)):
        kernel = functools.partial(corner_kernel, first)
        operands = [mine, halo_inner, halo_cross, side]
        ends += call(kernel, [(2 * KEPT + 24, OVL)], operands)
    corner_x = permute(ends[0], col_full)
    corner_d = permute(ends[1], col_inner)
    shapes = [
        ((4, cells, half), BF16),
        ((4, cells, half), BF16),
        ((4, count, half), F32),
        ((2, count, OVL), F32),
        ((2, count, OVL), F32),
    ]
    operands = [mine, halo_inner, halo_cross, halo_mi, halo_mc, corner_x, corner_d]
    operands += [rolled, measured, zown, high, low]
    own_hi, own_lo, zback, xcorn, dcorn = pl.pallas_call(
        main_kernel,
        name="main",
        out_shape=[pltpu.VMEM(s, d) for s, d in shapes],
        in_specs=[pl.BlockSpec(memory_space=pltpu.VMEM) for _ in operands],
        out_specs=[pl.BlockSpec(memory_space=pltpu.VMEM) for _ in shapes],
        scratch_shapes=[
            pltpu.VMEM((4, count, half), BF16),
            pltpu.VMEM((4, count, half), BF16),
            pltpu.VMEM((2, 4, half, half), BF16),
            pltpu.VMEM((2, 4, half, half), BF16),
            pltpu.VMEM((4, count, half), F32),
            pltpu.VMEM((2, 4, half, half), F32),
        ],
        compiler_params=pltpu.CompilerParams(vmem_limit_bytes=20 * 1024 * 1024),
        cost_estimate=pl.CostEstimate(flops=5_000_000_000, bytes_accessed=0, transcendentals=0),
    )(*[pltpu.with_memory_space_constraint(x, pltpu.VMEM) for x in operands])
    fix_x = permute(xcorn, col_full)
    fix_d = permute(dcorn, col_inner)
    nblock, sblock, middle_inner, middle_cross = call(
        block_kernel, [(2, OVL, 384)] * 2 + [(OVL, LANES)] * 2, [mine, zback, rolled], flops=1_000_000_000
    )
    grad_mi = permute(middle_inner, row_inner)
    grad_mc = permute(middle_cross, row_cross)
    to_inner, to_cross = call(send_kernel, [(4 * OVL, LANES)] * 2, [nblock, sblock, fix_x, fix_d, corner_x, corner_d])
    grad_inner = permute(to_inner, row_inner)
    grad_cross = permute(to_cross, row_cross)
    own, xedge, dedge = call(
        after_kernel,
        [(2, cells, cells)] + [(2, cells, OVL)] * 2,
        [mine, own_hi, own_lo, rolled, high, low],
        scratch=[pltpu.VMEM((4, cells, half), F32)],
        flops=2_000_000_000,
    )
    edge_x = permute(xedge, col_cross)
    edge_d = permute(dedge, col_inner)
    (weight,) = call(
        light_kernel,
        [(cells, cells)],
        [mine, corner_x, corner_d, halo_inner, halo_cross, probe_field],
        scratch=[pltpu.VMEM((6, size + 2 * OVL, LANES), F32), pltpu.VMEM((cells, 384), F32)],
        flops=10_000_000_000,
    )
    (updated,) = call(
        final_kernel,
        [(2, cells, cells)],
        [object_slab, own, weight, edge_x, edge_d, grad_inner, grad_cross, grad_mi, grad_mc],
        hbm_out=True,
        scratch=[
            pltpu.VMEM((2, cells, cells), F32),
            pltpu.SemaphoreType.DMA((cells // HALF,)),
        ],
    )
    return updated


def solution(mesh):
    return jax.shard_map(
        local,
        mesh=mesh,
        in_specs=(
            P(None, "row", "col"),
            P(),
            P("row", "col", None, None),
            P("row", "col", None, None, None),
        ),
        out_specs=P(None, "row", "col"),
        check_vma=False,
    )
```

```python
import functools
import math

import jax
import jax.numpy as jnp
import ml_dtypes
import numpy as np
from jax import lax
from jax.experimental import pallas as pl
from jax.experimental.pallas import tpu as pltpu
from jax.sharding import PartitionSpec as P


OVL = 128
HALF = 64
KEPT = 192
LANES = 128

EPSILON = 0.01
PHOTON_SCALE = 0.01
STEP_SIZE = 0.5
REGULAR = 1.0

F32 = jnp.float32
BF16 = jnp.bfloat16


def call(kernel, out_shapes, args, hbm_out=False, scratch=(), flops=0, limit=16):
    specs = [pl.BlockSpec(memory_space=pltpu.VMEM) for _ in args]
    args = [pltpu.with_memory_space_constraint(x, pltpu.VMEM) for x in args]
    return pl.pallas_call(
        kernel,
        out_shape=[
            jax.ShapeDtypeStruct(s, F32) if hbm_out else pltpu.VMEM(s, F32) for s in out_shapes
        ],
        in_specs=specs,
        out_specs=[
            pl.BlockSpec(memory_space=pltpu.HBM if hbm_out else pltpu.VMEM) for _ in out_shapes
        ],
        scratch_shapes=list(scratch),
        compiler_params=pltpu.CompilerParams(vmem_limit_bytes=limit * 1024 * 1024),
        cost_estimate=pl.CostEstimate(flops=flops, bytes_accessed=0, transcendentals=0)
        if flops
        else None,
    )(*args)


@functools.lru_cache(maxsize=None)
def tables(length):
    quarter = length // 4
    n = np.arange(quarter)[:, None]
    k = np.arange(quarter)[None, :]
    blocks = []
    for p in range(4):
        angle = 2.0 * np.pi * ((n * (4 * k + p)) % length) / length
        c = np.cos(angle) / math.sqrt(length)
        s = np.sin(angle) / math.sqrt(length)
        blocks.append(np.block([[c, -s], [s, c]]))
    blocks += [b.T for b in blocks]
    full = np.stack(blocks)
    high = full.astype(np.float32).astype(ml_dtypes.bfloat16)
    low = (full - high.astype(np.float64)).astype(np.float32).astype(ml_dtypes.bfloat16)
    return high, low


def split(x):
    high = x.astype(BF16)
    return high, (x - high.astype(F32)).astype(BF16)


def dot(a, b):
    return lax.dot_general(a, b, (((1,), (0,)), ((), ())), preferred_element_type=F32)


def mix_forward(x):
    (x0r, x0i), (x1r, x1i), (x2r, x2i), (x3r, x3i) = x
    ar, ai, br, bi = x0r + x2r, x0i + x2i, x0r - x2r, x0i - x2i
    cr, ci, dr, di = x1r + x3r, x1i + x3i, x1r - x3r, x1i - x3i
    return [(ar + cr, ai + ci), (br + di, bi - dr), (ar - cr, ai - ci), (br - di, bi + dr)]


def mix_inverse(x):
    (x0r, x0i), (x1r, x1i), (x2r, x2i), (x3r, x3i) = x
    ar, ai, br, bi = x0r + x2r, x0i + x2i, x0r - x2r, x0i - x2i
    cr, ci, dr, di = x1r + x3r, x1i + x3i, x1r - x3r, x1i - x3i
    return [(ar + cr, ai + ci), (br - di, bi + dr), (ar - cr, ai - ci), (br + di, bi - dr)]


def lane_iota(shape):
    return lax.broadcasted_iota(jnp.int32, shape, len(shape) - 1)


def row_iota(shape):
    return lax.broadcasted_iota(jnp.int32, shape, len(shape) - 2)


def turn(x):
    return pltpu.roll(x, HALF, len(x.shape) - 1)


def odd(axis):
    return lax.axis_index(axis) % 2 == 1


def paired(axis, x, first):
    place, count = lax.axis_index(axis), lax.axis_size(axis)
    if first == 0 and count % 2 == 0:
        return x
    if first == 0:
        return jnp.where(place < count - 1, x, 0.0)
    alone = place == 0 if count % 2 else (place == 0) | (place == count - 1)
    return jnp.where(alone, 0.0, x)


def offsets_tile(u, v):
    row = row_iota((8, LANES))
    return jnp.where(row == 0, u, jnp.where(row == 1, v, 1)).astype(F32)


def number(tile, i):
    picked = (lane_iota(tile.shape) == 0) & (row_iota(tile.shape) == i)
    return jnp.sum(jnp.where(picked, tile, 0.0))


def row_kernel(first, source, obj, *refs):
    rows, cols = obj.shape[1:]
    upward = odd("row") if first == 0 else ~odd("row")
    base = pl.multiple_of(jnp.where(upward, 0, rows - OVL), 8)
    out, middle, *mine, held, numbers, sems = refs
    copies = [pltpu.make_async_copy(obj.at[:, pl.ds(base, OVL), :], held, sems.at[0])]
    copies[0].start()
    if first == 0:
        copies.append(pltpu.make_async_copy(source, numbers, sems.at[1]))
        copies[1].start()
        copies[1].wait()
        info = offsets_tile(numbers[0, 0, 0, 0], numbers[0, 0, 0, 1])
        mine[0][...] = info
    else:
        info = source[...]
    out[4 * OVL : 4 * OVL + 8, :] = paired("row", info, first)
    copies[0].wait()
    for c in range(2):
        at = 2 * c * OVL
        out[at : at + OVL, :] = paired("row", held[c, :, 0:OVL], first)
        out[at + OVL : at + 2 * OVL, :] = paired("row", held[c, :, cols - OVL : cols], first)
        middle[:, c * HALF : c * HALF + HALF] = paired("row", held[c, :, OVL : cols - OVL], first)


def side_kernel(mine, obj, xside, dside):
    cells, cols = obj.shape[1:]
    right = odd("col")
    info = mine[...]
    for c in range(2):
        rows = slice(c * cells, c * cells + cells)
        west = turn(obj[c, :, 0:128])
        east = obj[c, :, cols - OVL : cols]
        xside[rows, :] = paired("col", jnp.where(right, east, west), 1)
        dside[rows, :] = paired("col", jnp.where(right, west, east), 0)
    xside[2 * cells : 2 * cells + 8, :] = paired("col", info, 1)
    dside[2 * cells : 2 * cells + 8, :] = paired("col", info, 0)


def corner_kernel(first, mine, inner, cross, side, out):
    far = odd("row")
    to_right = odd("col") if first else ~odd("col")
    cells = (side.shape[0] - 8) // 2
    border = side[2 * cells : 2 * cells + 1, :]
    row = row_iota((HALF, LANES)).astype(F32)

    def end(part, c, base):
        def take(tile):
            at = slice(tile * OVL + base, tile * OVL + base + HALF)
            a, b = inner[at, :], cross[at, :]
            return jnp.where(far, a, b) if part == 0 else jnp.where(far, b, a)

        return paired("col", jnp.where(to_right, take(2 * c + 1), turn(take(2 * c))), first)

    for c in range(2):
        base = c * KEPT
        out[base : base + HALF, :] = jnp.where(row < border, end(1, c, HALF), end(0, c, 0))
        out[base + HALF : base + OVL, :] = end(0, c, HALF)
        out[base + OVL : base + KEPT, :] = end(1, c, 0)
    rows = 2 * KEPT
    out[rows : rows + 8, :] = paired("col", inner[4 * OVL : 4 * OVL + 8, :], first)
    out[rows + 8 : rows + 16, :] = paired("col", cross[4 * OVL : 4 * OVL + 8, :], first)
    out[rows + 16 : rows + 24, :] = paired("col", mine[...], first)


def ready_kernel(mine, probe, counts, rolled, measured, wide):
    size = probe.shape[-1]
    quarter = size // 4
    u, v = [number(mine[...], i).astype(jnp.int32) for i in range(2)]
    for c in range(2):
        for t in range(4):
            cols = slice(t * quarter, (t + 1) * quarter)
            wide[c, t, 0:HALF, :] = probe[c, size - HALF : size, cols]
            wide[c, t, HALF : HALF + size, :] = probe[c, :, cols]
        for base in range(0, size, HALF):
            rows = pl.ds(HALF - u + base, HALF)
            piece = jnp.concatenate([wide[c, t, rows, :] for t in range(4)], axis=1)
            rolled[c, base : base + HALF, :] = pltpu.roll(piece, v, 1)
    r = row_iota((size, size))
    k = lane_iota((size, size))
    order = jnp.where(r == 4 * (k % quarter) + k // quarter, 1.0, 0.0).astype(BF16)
    for t in range(4):
        wide[0, t, 0:size, :] = counts[:, t * quarter : (t + 1) * quarter].astype(F32)
    for p in range(4):
        rows = jnp.concatenate([wide[0, t, pl.ds(p, quarter, stride=4), :] for t in range(4)], axis=1)
        high = jnp.floor(rows * (1.0 / 256.0))
        low = rows - 256.0 * high
        moved = 256.0 * dot(high.astype(BF16), order) + dot(low.astype(BF16), order)
        measured[p * quarter : (p + 1) * quarter, :] = jnp.sqrt(moved * PHOTON_SCALE)


def keep(hi, lo, at, x):
    hi[at], lo[at] = split(x)


STEP = 32


def enter(tiles, rolled, rows, hi, lo, at):
    quarter = rolled.shape[-1] // 4
    exits = []
    for q in range(4):
        cols = slice(q * quarter, (q + 1) * quarter)
        ar, ai = rolled[0, rows, cols], rolled[1, rows, cols]
        exits.append((ar * tiles[0][q] - ai * tiles[1][q], ar * tiles[1][q] + ai * tiles[0][q]))
    for p, (yr, yi) in enumerate(mix_forward(exits)):
        keep(hi, lo, (p, at, slice(0, quarter)), yr)
        keep(hi, lo, (p, at, slice(quarter, 2 * quarter)), yi)


def leave(z, at, rolled, rows, v, right):
    quarter = rolled.shape[-1] // 4
    quads = [(z[p, at, 0:quarter], z[p, at, quarter : 2 * quarter]) for p in range(4)]
    grads = ([], [])
    for q, (br, bi) in enumerate(mix_inverse(quads)):
        cols = slice(q * quarter, (q + 1) * quarter)
        ar, ai = rolled[0, rows, cols], rolled[1, rows, cols]
        grads[0].append(ar * br + ai * bi)
        grads[1].append(ar * bi - ai * br)
    lane = lane_iota((STEP, LANES))
    early = lane.astype(F32) < v
    for g in grads:
        wout = turn(jnp.where(early, 0.0, g[0]))
        eout = turn(jnp.where(lane < HALF, jnp.where(early, g[0], 0.0), g[3]))
        xout = paired("col", jnp.where(right, eout, wout), 1)
        yield g[1:], xout, paired("col", jnp.where(right, wout, eout), 0)


def right_product(hi, lo, rows, p, high, low, k):
    a = hi[p, rows, :]
    return dot(a, high[k]) + dot(lo[p, rows, :], high[k]) + dot(a, low[k])


def left_product(hi, lo, at, high, low, k):
    a = hi[at]
    return dot(high[k], a) + dot(high[k], lo[at]) + dot(low[k], a)


def fore_kernel(mine, obj, xside, dside, rolled, high, low, z, hi, lo):
    cells = obj.shape[1]
    v = mine[1:2, :]
    right = odd("col")
    lane = lane_iota((STEP, LANES))
    early = lane.astype(F32) < v
    for top in range(0, cells, cells // 2):
        for base in range(top, top + cells // 2, STEP):
            rows = slice(base, base + STEP)
            tiles = []
            for c in range(2):
                last = obj[c, rows, 256:cells]
                last = jnp.concatenate([last, last], axis=1)
                at = slice(c * cells + base, c * cells + base + STEP)
                x, d = xside[at, :], dside[at, :]
                w, e = jnp.where(right, d, x), jnp.where(right, x, d)
                tiles.append(
                    [
                        jnp.where(early, e, w),
                        obj[c, rows, 0:128],
                        obj[c, rows, 128:256],
                        jnp.where(lane < HALF, last, e),
                    ]
                )
            enter(tiles, rolled, slice(base + OVL, base + OVL + STEP), hi, lo, rows)
        rows = slice(top, top + cells // 2)
        for p in range(4):
            z[p, rows, :] = right_product(hi, lo, rows, p, high, low, p)


def main_kernel(
    mine, inner, cross, minner, mcross, xcorner, dcorner, rolled, measured, zown, high, low,
    own_hi, own_lo, zback, xcorn, dcorn, ah, al, bh, bl, zh, tf,
):
    size = rolled.shape[-1]
    quarter = size // 4
    cells = zown.shape[1]
    u = mine[0:1, :]
    v = mine[1:2, :]
    right = odd("col")
    far = odd("row")
    lane = lane_iota((STEP, LANES))
    early = lane.astype(F32) < v
    step_row = row_iota((STEP, LANES)).astype(F32)

    def patch(c, slot, base):
        def halo(part, start):
            tiles = []
            for first, second, t in ((inner, cross, 2 * c), (minner, mcross, 0), (inner, cross, 2 * c + 1)):
                at = slice(t * OVL + start, t * OVL + start + STEP)
                a, b = first[at, :], second[at, :]
                tiles.append(jnp.where(far, a, b) if part == 0 else jnp.where(far, b, a))
            return tiles

        if slot >= OVL:
            tiles = halo(1, slot - OVL - cells)
        else:
            tiles = halo(0, slot)
        if slot < HALF:
            row = step_row + slot
            tiles = [jnp.where(row < u, b, a) for a, b in zip(tiles, halo(1, slot + HALF))]
        last = turn(tiles[2])
        middle = jnp.where(lane < HALF, turn(tiles[1]) if c == 1 else tiles[1], last)
        at = slice(c * KEPT + base, c * KEPT + base + STEP)
        x, d = xcorner[at, :], dcorner[at, :]
        w, e = jnp.where(right, d, x), jnp.where(right, x, d)
        return [jnp.where(early, e, w), tiles[0], middle, jnp.where(lane < HALF, last, e)]

    block = 2 * quarter
    re, im = slice(0, quarter), slice(quarter, 2 * quarter)
    count = size - cells
    slots = [b if b < OVL else b + cells for b in range(0, count, STEP)]

    for base, slot in zip(range(0, count, STEP), slots):
        rows = slice(slot, slot + STEP)
        enter([patch(c, slot, base) for c in range(2)], rolled, rows, ah, al, slice(base, base + STEP))
    for p in range(4):
        zh[p] = right_product(ah, al, slice(0, count), p, high, low, p)

    def place(slot, halo, own):
        if slot < OVL:
            return halo, slice(slot, slot + STEP)
        if slot < OVL + cells:
            return own, slice(slot - OVL, slot - OVL + STEP)
        return halo, slice(slot - cells, slot - cells + STEP)

    for half in range(2):
        pair = (2 * half, 2 * half + 1)
        for t, p in enumerate(pair):
            cols = slice(t * quarter, (t + 1) * quarter)
            for r in range(0, quarter, STEP):
                quads = []
                for q in range(4):
                    z, rows = place(q * quarter + r, zh, zown)
                    quads.append((z[p, rows, re], z[p, rows, im]))
                for k, (yr, yi) in enumerate(mix_forward(quads)):
                    keep(bh, bl, (half, k, slice(r, r + STEP), cols), yr)
                    keep(bh, bl, (half, k, slice(quarter + r, quarter + r + STEP), cols), yi)
    for half in range(2):
        for k in range(4):
            z = left_product(bh, bl, (half, k), high, low, 4 + k)
            zr, zi = z[re], z[im]
            m = measured[k * quarter : (k + 1) * quarter, half * block : (half + 1) * block]
            factor = 1.0 - m * lax.rsqrt(zr * zr + zi * zi + EPSILON)
            keep(bh, bl, (half, k, re), factor * zr)
            keep(bh, bl, (half, k, im), factor * zi)
    for half in range(2):
        for k in range(4):
            tf[half, k] = left_product(bh, bl, (half, k), high, low, k)
    for half in range(2):
        pair = (2 * half, 2 * half + 1)
        for t, p in enumerate(pair):
            cols = slice(t * quarter, (t + 1) * quarter)
            for r in range(0, quarter, STEP):
                again = slice(quarter + r, quarter + r + STEP)
                quads = [(tf[half, k, r : r + STEP, cols], tf[half, k, again, cols]) for k in range(4)]
                for q, (yr, yi) in enumerate(mix_inverse(quads)):
                    hi, rows = place(q * quarter + r, ah, own_hi)
                    lo, rows = place(q * quarter + r, al, own_lo)
                    keep(hi, lo, (p, rows, re), yr)
                    keep(hi, lo, (p, rows, im), yi)

    for p in range(4):
        zback[p] = right_product(ah, al, slice(0, count), p, high, low, 4 + p)
    for base, slot in zip(range(0, count, STEP), slots):
        at, rows = slice(base, base + STEP), slice(slot, slot + STEP)
        for c, (_, xout, dout) in enumerate(leave(zback, at, rolled, rows, v, right)):
            xcorn[c, at, :] = xout
            dcorn[c, at, :] = dout


def after_kernel(mine, hi, lo, rolled, high, low, own, xedge, dedge, z):
    cells = own.shape[1]
    v = mine[1:2, :]
    right = odd("col")
    for top in range(0, cells, cells // 2):
        rows = slice(top, top + cells // 2)
        for p in range(4):
            z[p, rows, :] = right_product(hi, lo, rows, p, high, low, 4 + p)
        for base in range(top, top + cells // 2, STEP):
            at, rows = slice(base, base + STEP), slice(base + OVL, base + OVL + STEP)
            for c, (g, xout, dout) in enumerate(leave(z, at, rolled, rows, v, right)):
                own[c, at, 0:128] = g[0]
                own[c, at, 128:256] = g[1]
                own[c, at, 256:cells] = g[2][:, : cells - 256]
                xedge[c, at, :] = xout
                dedge[c, at, :] = dout


def block_kernel(mine, zback, rolled, nblock, sblock, minner, mcross):
    cells = rolled.shape[-1] - zback.shape[1]
    v = mine[1:2, :]
    right = odd("col")
    u = mine[0:1, :]
    for base in range(0, zback.shape[1], STEP):
        slot = base if base < OVL else base + cells
        row = row_iota((STEP, LANES)).astype(F32) + slot
        sends = []
        if slot < OVL:
            sends.append((nblock, slot, row >= u if slot < HALF else None))
        if slot < HALF:
            sends.append((sblock, slot + HALF, row < u))
        if slot >= OVL:
            sends.append((sblock, slot - OVL - cells, None))
        at, rows = slice(base, base + STEP), slice(slot, slot + STEP)
        for c, (g, _, _) in enumerate(leave(zback, at, rolled, rows, v, right)):
            for block, o, mask in sends:
                for t, x in enumerate(g):
                    put = x if mask is None else jnp.where(mask, x, 0.0)
                    block[c, o : o + STEP, 128 * t : 128 * t + 128] = put
    far = odd("row")
    first = lane_iota((OVL, LANES)) < HALF
    n, s = [jnp.where(first, b[0, :, 128:256], turn(b[1, :, 128:256])) for b in (nblock, sblock)]
    minner[...] = paired("row", jnp.where(far, n, s), 0)
    mcross[...] = paired("row", jnp.where(far, s, n), 1)


def send_kernel(nblock, sblock, xcorn, dcorn, xcorner, dcorner, inner, cross):
    right = odd("col")
    far = odd("row")
    first = lane_iota((HALF, LANES)) < HALF
    row = row_iota((HALF, LANES)).astype(F32)
    at = 2 * KEPT + 16
    borders = [ref[at : at + 1, :] for ref in (xcorner, dcorner)]

    def corner(ref, border, c, part, base):
        if part == 1 and base == 0:
            return ref[c, OVL:KEPT, :]
        if part == 0 and base == HALF:
            return ref[c, HALF:OVL, :]
        mixed = ref[c, 0:HALF, :]
        return jnp.where((row < border) == (part == 1), mixed, 0.0)

    for base in (0, HALF):
        rows = slice(base, base + HALF)
        tiles = []
        for part, block in enumerate((nblock, sblock)):
            out = []
            for c in range(2):
                x, d = [corner(*pair, c, part, base) for pair in zip((xcorn, dcorn), borders)]
                fw, fe = jnp.where(right, d, x), jnp.where(right, x, d)
                out.append(block[c, rows, 0:128] + fw)
                end = jnp.where(first, block[c, rows, 256:384], block[c, rows, 128:256])
                out.append(turn(end + fe))
            tiles.append(out)
        for t, (n, s) in enumerate(zip(*tiles)):
            to = slice(t * OVL + base, t * OVL + base + HALF)
            inner[to, :] = paired("row", jnp.where(far, n, s), 0)
            cross[to, :] = paired("row", jnp.where(far, s, n), 1)


def light_kernel(
    mine, xcorner, dcorner, inner, cross, probe, weight, pad, acc
):
    size = probe.shape[-1]
    cells = weight.shape[0]
    far = odd("row")
    pad[...] = jnp.zeros(pad.shape, F32)
    for t in range(4):
        cols = slice(t * LANES, (t + 1) * LANES)
        x = probe[0, :, cols]
        y = probe[1, :, cols]
        pad[1 + t, OVL : OVL + size, :] = x * x + y * y
    acc[...] = jnp.zeros(acc.shape, F32)
    first = lane_iota((HALF, LANES)) < HALF
    right = odd("col")
    for di in (0, -1, 1):
        for dj in (0, -1, 1):

            def take(first, second, at, again):
                a, b = first[at : at + 8, :], second[again : again + 8, :]
                return jnp.where(far, a, b) if di < 0 else jnp.where(far, b, a)

            if di == 0 and dj == 0:
                tile = mine[...]
            elif dj == 0:
                tile = take(inner, cross, 4 * OVL, 4 * OVL)
            else:
                if di == 0:
                    x, d = [ref[2 * KEPT + 16 : 2 * KEPT + 24, :] for ref in (xcorner, dcorner)]
                else:
                    x, d = [take(ref, ref, 2 * KEPT, 2 * KEPT + 8) for ref in (xcorner, dcorner)]
                tile = jnp.where(right, d, x) if dj < 0 else jnp.where(right, x, d)
            u, v, there = [number(tile, i) for i in range(3)]
            u, v = u.astype(jnp.int32), v.astype(jnp.int32)
            start, count, put = {
                0: (2 * OVL - u, cells, 0),
                1: (OVL - u, OVL, cells - OVL),
                -1: (size + HALF - u, OVL, 0),
            }[di]
            seen = there
            for r in range(0, count, HALF):
                rows = pl.ds(start + r, HALF)
                to = slice(put + r, put + r + HALF)
                lo, hi, shift = {0: (1, 5, 384 + v), -1: (4, 6, lax.rem(192 + v, 256)), 1: (0, 2, 128 + v)}[dj]
                x = pltpu.roll(jnp.concatenate([pad[t, rows, :] for t in range(lo, hi)], axis=1), shift, 1)
                if dj == 0:
                    x = x[:, 0:384]
                    acc[to, :] += x * seen
                    continue
                if dj == -1:
                    x = x[:, 0:128]
                    acc[to, 0:128] += x * seen
                    continue
                x = turn(x[:, 0:128]) * seen
                acc[to, 128:256] += jnp.where(first, 0.0, x)
                acc[to, 256:384] += x
    for r in range(0, cells, HALF):
        rows = slice(r, r + HALF)
        weight[rows, :] = STEP_SIZE / (acc[rows, 0:cells] + REGULAR)


def final_kernel(
    obj, own, weight, xedge, dedge, inner, cross, minner, mcross, updated, held, sems
):
    cells = obj.shape[1]
    right = odd("col")
    far = odd("row")
    first = lane_iota((HALF, LANES)) < HALF
    copies = []
    for r in range(0, cells, HALF):
        rows = slice(r, r + HALF)
        for c in range(2):
            x, d = xedge[c, rows, :], dedge[c, rows, :]
            fw, fe = jnp.where(right, d, x), jnp.where(right, x, d)
            g = [
                own[c, rows, 0:128] + fw,
                own[c, rows, 128:256] + jnp.where(first, 0.0, fe),
                own[c, rows, 256:cells] + fe[:, : cells - 256],
            ]
            adds = []
            if r < OVL:
                adds.append((0, r))
            if r >= cells - OVL:
                adds.append((1, r - cells + OVL))
            for part, o in adds:

                def take(first, second, tile):
                    src = slice(tile * OVL + o, tile * OVL + o + HALF)
                    a, b = first[src, :], second[src, :]
                    return jnp.where(far, a, b) if part == 0 else jnp.where(far, b, a)

                end = turn(take(inner, cross, 2 * c + 1))
                middle = take(minner, mcross, 0)
                g[0] = g[0] + take(inner, cross, 2 * c)
                g[1] = g[1] + jnp.where(first, turn(middle) if c == 1 else middle, end)
                g[2] = g[2] + end[:, : cells - 256]
            for t, x in enumerate(g):
                cols = slice(128 * t, min(128 * t + 128, cells))
                held[c, rows, cols] = obj[c, rows, cols] - x * weight[rows, cols]
        part = (slice(None), rows, slice(None))
        copies.append(pltpu.make_async_copy(held.at[part], updated.at[part], sems.at[r // HALF]))
        copies[-1].start()
    for copy in copies:
        copy.wait()


def swap(count, first, gap=1):
    partner = list(range(count))
    for i in range(first, count - gap):
        if (i - first) // gap % 2 == 0:
            partner[i], partner[i + gap] = i + gap, i
    return partner


def routes():
    rows, cols = lax.axis_size("row"), lax.axis_size("col")
    odd_row, even_row, far_row = swap(rows, 1), swap(rows, 0), swap(rows, 0, 2)
    odd_col, even_col = swap(cols, 1), swap(cols, 0)

    def pairs(partner):
        grid = [(r, c, *partner(r, c)) for r in range(rows) for c in range(cols)]
        return [(r * cols + c, to_r * cols + to_c) for r, c, to_r, to_c in grid]

    return (
        pairs(lambda r, c: (odd_row[r], c if odd_row[r] != r else even_col[c])),
        pairs(lambda r, c: (even_row[r], c)),
        pairs(lambda r, c: (r, odd_col[c])),
        pairs(lambda r, c: (r, even_col[c])),
        pairs(lambda r, c: (r if odd_col[c] != c else far_row[r], odd_col[c])),
    )


def permute(x, pairs):
    return lax.ppermute(x, ("row", "col"), pairs)


def local(object_slab, probe_field, offsets, counts):
    cells = object_slab.shape[1]
    size = probe_field.shape[-1]
    row_cross, row_inner, col_cross, col_inner, col_full = routes()
    table_high, table_low = tables(size)
    high, low = jnp.asarray(table_high), jnp.asarray(table_low)

    def rows_for(first, source, space):
        shapes = [(4 * OVL + 8, LANES), (OVL, LANES)] + [(8, LANES)] * (first == 0)
        step = pl.pallas_call(
            functools.partial(row_kernel, first),
            out_shape=[pltpu.VMEM(n, F32) for n in shapes],
            in_specs=[pl.BlockSpec(memory_space=space), pl.BlockSpec(memory_space=pltpu.HBM)],
            out_specs=[pl.BlockSpec(memory_space=pltpu.VMEM) for _ in shapes],
            scratch_shapes=[
                pltpu.VMEM((2, OVL, cells), F32),
                pltpu.SMEM((1, 1, 1, 2), jnp.int32),
                pltpu.SemaphoreType.DMA((2,)),
            ],
            compiler_params=pltpu.CompilerParams(vmem_limit_bytes=8 * 1024 * 1024),
            cost_estimate=pl.CostEstimate(flops=2_500_000_000, bytes_accessed=0, transcendentals=0),
        )
        return step(
            pltpu.with_memory_space_constraint(source, space),
            pltpu.with_memory_space_constraint(object_slab, pltpu.HBM),
        )

    to_inner, middle_inner, mine = rows_for(0, offsets, pltpu.HBM)
    halo_inner = permute(to_inner, row_inner)
    to_cross, middle_cross = rows_for(1, mine, pltpu.VMEM)
    halo_cross = permute(to_cross, row_cross)
    xside, dside = call(side_kernel, [(2 * cells + 8, OVL)] * 2, [mine, object_slab], flops=5_000_000_000)
    side_x = permute(xside, col_cross)
    side_d = permute(dside, col_inner)

    rolled, measured = call(
        ready_kernel,
        [(2, size, size), (size, size)],
        [mine, probe_field, counts.reshape(size, size)],
        scratch=[pltpu.VMEM((2, 4, size + HALF, LANES), F32)],
        flops=5_000_000_000,
    )
    half, count = size // 2, size - cells
    (zown,) = call(
        fore_kernel,
        [(4, cells, half)],
        [mine, object_slab, side_x, side_d, rolled, high, low],
        scratch=[pltpu.VMEM((4, cells, half), BF16) for _ in range(2)],
        flops=2_000_000_000,
    )
    halo_mi = permute(middle_inner, row_inner)
    halo_mc = permute(middle_cross, row_cross)
    ends = []
    for first, side in ((1, side_x), (0, side_d)):
        kernel = functools.partial(corner_kernel, first)
        operands = [mine, halo_inner, halo_cross, side]
        ends += call(kernel, [(2 * KEPT + 24, OVL)], operands)
    corner_x = permute(ends[0], col_full)
    corner_d = permute(ends[1], col_inner)
    shapes = [
        ((4, cells, half), BF16),
        ((4, cells, half), BF16),
        ((4, count, half), F32),
        ((2, count, OVL), F32),
        ((2, count, OVL), F32),
    ]
    operands = [mine, halo_inner, halo_cross, halo_mi, halo_mc, corner_x, corner_d]
    operands += [rolled, measured, zown, high, low]
    own_hi, own_lo, zback, xcorn, dcorn = pl.pallas_call(
        main_kernel,
        name="main",
        out_shape=[pltpu.VMEM(s, d) for s, d in shapes],
        in_specs=[pl.BlockSpec(memory_space=pltpu.VMEM) for _ in operands],
        out_specs=[pl.BlockSpec(memory_space=pltpu.VMEM) for _ in shapes],
        scratch_shapes=[
            pltpu.VMEM((4, count, half), BF16),
            pltpu.VMEM((4, count, half), BF16),
            pltpu.VMEM((2, 4, half, half), BF16),
            pltpu.VMEM((2, 4, half, half), BF16),
            pltpu.VMEM((4, count, half), F32),
            pltpu.VMEM((2, 4, half, half), F32),
        ],
        compiler_params=pltpu.CompilerParams(vmem_limit_bytes=20 * 1024 * 1024),
        cost_estimate=pl.CostEstimate(flops=5_000_000_000, bytes_accessed=0, transcendentals=0),
    )(*[pltpu.with_memory_space_constraint(x, pltpu.VMEM) for x in operands])
    fix_x = permute(xcorn, col_full)
    fix_d = permute(dcorn, col_inner)
    nblock, sblock, middle_inner, middle_cross = call(
        block_kernel, [(2, OVL, 384)] * 2 + [(OVL, LANES)] * 2, [mine, zback, rolled], flops=1_000_000_000
    )
    grad_mi = permute(middle_inner, row_inner)
    grad_mc = permute(middle_cross, row_cross)
    to_inner, to_cross = call(send_kernel, [(4 * OVL, LANES)] * 2, [nblock, sblock, fix_x, fix_d, corner_x, corner_d])
    grad_inner = permute(to_inner, row_inner)
    grad_cross = permute(to_cross, row_cross)
    own, xedge, dedge = call(
        after_kernel,
        [(2, cells, cells)] + [(2, cells, OVL)] * 2,
        [mine, own_hi, own_lo, rolled, high, low],
        scratch=[pltpu.VMEM((4, cells, half), F32)],
        flops=2_000_000_000,
    )
    edge_x = permute(xedge, col_cross)
    edge_d = permute(dedge, col_inner)
    (weight,) = call(
        light_kernel,
        [(cells, cells)],
        [mine, corner_x, corner_d, halo_inner, halo_cross, probe_field],
        scratch=[pltpu.VMEM((6, size + 2 * OVL, LANES), F32), pltpu.VMEM((cells, 384), F32)],
        flops=10_000_000_000,
    )
    (updated,) = call(
        final_kernel,
        [(2, cells, cells)],
        [object_slab, own, weight, edge_x, edge_d, grad_inner, grad_cross, grad_mi, grad_mc],
        hbm_out=True,
        scratch=[
            pltpu.VMEM((2, cells, cells), F32),
            pltpu.SemaphoreType.DMA((cells // HALF,)),
        ],
    )
    return updated


def solution(mesh):
    return jax.shard_map(
        local,
        mesh=mesh,
        in_specs=(
            P(None, "row", "col"),
            P(),
            P("row", "col", None, None),
            P("row", "col", None, None, None),
        ),
        out_specs=P(None, "row", "col"),
        check_vma=False,
    )
```
